16 devices in a mesh: stage: 2 (over z), expert: 8 (over y, x, core).
Axes of the slice: x: 2, y: 2, z: 2, core: 2. Of those that a mesh axis runs over, the one named last changes fastest.
Arguments:
- w_gate: bfloat16 [2, 8, 2048, 1024], P('stage', 'expert')
- w_up: bfloat16 [2, 8, 2048, 1024], P('stage', 'expert')
- w_down: bfloat16 [2, 8, 1024, 2048], P('stage', 'expert')
- hot_units: int32 [1], replicated
- slot_map: int32 [16, 2], replicated
Outputs:
- output 1: bfloat16 [2, 48, 2048, 1024], P(None, ('stage', 'expert'))
- output 2: bfloat16 [2, 48, 512, 2048], P(None, ('stage', 'expert'))
All inputs are finite; a program needn't handle non-finite values.
Results may differ from the reference program's by a relative error of at most 0.001.
Values are sent between devices in bfloat16 or wider.
A program may use at most 1 GiB of HBM per device.

```python
import jax
import jax.numpy as jnp

LAYERS = 2
EXPERTS = 8
D_MODEL = 2048
FF_EXPERT = 1024
DEVICES_FLAT = 16
HOT_UNITS = 1
EXTRA_SLOTS = 2

SPLIT_COUNT = max(DEVICES_FLAT // EXPERTS, 1)
UNITS_DEV = max(EXPERTS // DEVICES_FLAT, 1)
FF_DEV = FF_EXPERT // SPLIT_COUNT
UNIT_COUNT = EXPERTS * SPLIT_COUNT
SLOTS_DEV = UNITS_DEV + EXTRA_SLOTS
REPLICAS = 3 * DEVICES_FLAT // 2


def setup_inputs(seed: int = 0) -> dict:
    base_key = jax.random.key(seed)
    key_gate, key_up, key_down, key_hot, key_slot = jax.random.split(base_key, 5)
    gate_shape = (LAYERS, EXPERTS, D_MODEL, FF_EXPERT)
    down_shape = (LAYERS, EXPERTS, FF_EXPERT, D_MODEL)
    w_gate = (jax.random.normal(key_gate, gate_shape, jnp.float32) * D_MODEL ** -0.5).astype(jnp.bfloat16)
    w_up = (jax.random.normal(key_up, gate_shape, jnp.float32) * D_MODEL ** -0.5).astype(jnp.bfloat16)
    w_down = (jax.random.normal(key_down, down_shape, jnp.float32) * FF_EXPERT ** -0.5).astype(jnp.bfloat16)
    hot_units = jax.random.permutation(key_hot, UNIT_COUNT)[:HOT_UNITS].astype(jnp.int32)
    slot_order = jax.random.permutation(key_slot, DEVICES_FLAT * EXTRA_SLOTS)
    slot_map = jnp.where(slot_order < REPLICAS, slot_order % HOT_UNITS, -1).astype(jnp.int32).reshape(DEVICES_FLAT, EXTRA_SLOTS)
    return {'w_gate': w_gate, 'w_up': w_up, 'w_down': w_down, 'hot_units': hot_units, 'slot_map': slot_map}


def reference(w_gate, w_up, w_down, hot_units, slot_map):
    gate_parts = w_gate.reshape(LAYERS, EXPERTS, D_MODEL, SPLIT_COUNT, FF_DEV)
    up_parts = w_up.reshape(LAYERS, EXPERTS, D_MODEL, SPLIT_COUNT, FF_DEV)
    fused_units = jnp.concatenate([gate_parts, up_parts], axis=-1).transpose(0, 1, 3, 2, 4).reshape(LAYERS, UNIT_COUNT, D_MODEL, 2 * FF_DEV)
    down_units = w_down.reshape(LAYERS, UNIT_COUNT, FF_DEV, D_MODEL)
    slot_used = slot_map >= 0
    extra_ids = jnp.where(slot_used, hot_units[jnp.maximum(slot_map, 0)], 0).reshape(-1)
    keep_mask = slot_used.reshape(1, DEVICES_FLAT, EXTRA_SLOTS, 1, 1)
    fused_extra = jnp.where(keep_mask, jnp.take(fused_units, extra_ids, axis=1).reshape(LAYERS, DEVICES_FLAT, EXTRA_SLOTS, D_MODEL, 2 * FF_DEV), 0)
    down_extra = jnp.where(keep_mask, jnp.take(down_units, extra_ids, axis=1).reshape(LAYERS, DEVICES_FLAT, EXTRA_SLOTS, FF_DEV, D_MODEL), 0)
    fused_home = fused_units.reshape(LAYERS, DEVICES_FLAT, UNITS_DEV, D_MODEL, 2 * FF_DEV)
    down_home = down_units.reshape(LAYERS, DEVICES_FLAT, UNITS_DEV, FF_DEV, D_MODEL)
    w13 = jnp.concatenate([fused_home, fused_extra], axis=2).reshape(LAYERS, DEVICES_FLAT * SLOTS_DEV, D_MODEL, 2 * FF_DEV)
    w_down_out = jnp.concatenate([down_home, down_extra], axis=2).reshape(LAYERS, DEVICES_FLAT * SLOTS_DEV, FF_DEV, D_MODEL)
    return w13, w_down_out
```

```python
import functools

import jax
import jax.numpy as jnp
from jax import lax
from jax.experimental import pallas as pl
from jax.experimental.pallas import tpu as pltpu
from jax.sharding import PartitionSpec as P

MESH = pl.DeviceIdType.MESH
ANY = pl.BlockSpec(memory_space=pl.ANY)
BF16 = jnp.bfloat16

PARENT = (
    (None, 0, 3, 1, 5, 1, 7, 5),
    (None, 3, 0, 2, 6, 7, 2, 3),
    (None, 5, 6, 7, 0, 4, 4, 6),
)
DEPTH = (
    (0, 1, 3, 2, 3, 2, 4, 3),
    (0, 3, 1, 2, 3, 4, 2, 3),
    (0, 3, 3, 4, 1, 2, 2, 3),
)
CHILDREN = tuple(tuple(tuple(v for v in range(1, 8) if par[v] == r) for r in range(8)) for par in PARENT)
N = 16


def coords():
    z = lax.axis_index("stage")
    j = lax.axis_index("expert")
    return z, j // 4, (j // 2) % 2, j % 2


def dev(z, y, x, q):
    return (z, y * 4 + x * 2 + q)


def flip(v, bit):
    return 1 - v if bit else v


def table(index, values):
    out = jnp.int32(values[0])
    for i, v in enumerate(values[1:], 1):
        if v != values[0]:
            out = jnp.where(index == i, jnp.int32(v), out)
    return out


def home_kernel(gate, up, down, home13, homed, vg, vd, load_sem, send_sem, recv_sem):
    s, a, b, c = coords()

    def source(k, p):
        if p == 2:
            return down.at[0, 0, pl.ds(k * 512, 512), :], vd.at[k]
        return (gate, up)[p].at[0, 0, :, pl.ds(k * 512, 512)], vg.at[k, p]

    def dest(layer, p):
        return homed.at[layer] if p == 2 else home13.at[layer, :, pl.ds(p * 512, 512)]

    loads = {}
    for p in range(3):
        for k in range(2):
            loads[k, p] = pltpu.make_async_copy(*source(k, p), load_sem.at[k, p])
            loads[k, p].start()
    stay = [(s == a) & (a == b) & (b == c) & (c == k) for k in range(2)]

    def send(k, p):
        return pltpu.make_async_remote_copy(
            src_ref=source(k, p)[1],
            dst_ref=dest(s, p),
            send_sem=send_sem.at[k, p],
            recv_sem=recv_sem.at[s, p],
            device_id=dev(a, b, c, k),
            device_id_type=MESH,
        )

    for p in range(3):
        for k in range(2):
            loads[k, p].wait()

            @pl.when(stay[k])
            def _():
                pltpu.make_async_copy(source(k, p)[1], dest(s, p), recv_sem.at[s, p]).start()

            @pl.when(jnp.logical_not(stay[k]))
            def _():
                send(k, p).start()

    for p in range(3):
        for k in range(2):

            @pl.when(jnp.logical_not(stay[k]))
            def _():
                send(k, p).wait_send()

    for layer in range(2):
        for p in range(3):
            pltpu.make_async_copy(dest(layer, p), dest(layer, p), recv_sem.at[layer, p]).wait()


def hot_kernel(unit, gate, up, down, hot13, hotd, vg, vd, load_sem, recv_sem, send_sem, side_send, side_recv, out_sem):
    e, k = unit // 2, unit % 2
    ra, rb, rc = e // 4, (e // 2) % 2, e % 2
    z, y, x, q = coords()

    def source(p):
        return down.at[0, 0, pl.ds(k * 512, 512), :] if p == 2 else (gate, up)[p].at[0, 0, :, pl.ds(k * 512, 512)]

    def held(s, p, i=None):
        if p == 2:
            return vd.at[s] if i is None else vd.at[s, pl.ds(i * (512 // N), 512 // N), :]
        return vg.at[s, p] if i is None else vg.at[s, p, pl.ds(i * (2048 // N), 2048 // N), :]

    def final(s, p, i=None):
        if p == 2:
            return hotd.at[s] if i is None else hotd.at[s, pl.ds(i * (512 // N), 512 // N), :]
        cols = pl.ds(p * 512, 512)
        return hot13.at[s, :, cols] if i is None else hot13.at[s, pl.ds(i * (2048 // N), 2048 // N), cols]

    state = []
    for s in range(2):
        fz, fy, fx = flip(z, s), flip(y, ra), flip(x, rb)
        rel = fz * 4 + fy * 2 + fx
        relay = q == jnp.where(rel == 0, rc, s)
        state.append((rel, relay, fz, fy, fx))

    for s in range(2):
        rel, relay = state[s][:2]

        @pl.when(relay & (rel == 0))
        def _():
            for p in range(3):
                pltpu.make_async_copy(source(p), held(s, p), load_sem.at[p]).start()
            for p in range(3):
                pltpu.make_async_copy(source(p), held(s, p), load_sem.at[p]).wait()

    def step(t, carry):
        for s in range(2):
            rel, relay, fz, fy, fx = state[s]
            for p in range(3):
                i = t - table(rel, DEPTH[p])

                @pl.when(relay & (i >= 0) & (i < N))
                def _():
                    @pl.when(rel != 0)
                    def _():
                        pltpu.make_async_copy(held(s, p, i), held(s, p, i), recv_sem.at[s, p, i]).wait()

                    for m in range(2):
                        nodes = [r for r in range(8) if len(CHILDREN[p][r]) > m]
                        if not nodes:
                            continue
                        child = table(rel, [CHILDREN[p][r][m] if r in nodes else -1 for r in range(8)])

                        @pl.when(child >= 0)
                        def _():
                            to = dev(flip(child // 4, s), flip((child // 2) % 2, ra), flip(child % 2, rb), s)
                            pltpu.make_async_remote_copy(
                                src_ref=held(s, p, i),
                                dst_ref=held(s, p, i),
                                send_sem=send_sem.at[s, p, m],
                                recv_sem=recv_sem.at[s, p, i],
                                device_id=to,
                                device_id_type=MESH,
                            ).start()

                    pltpu.make_async_remote_copy(
                        src_ref=held(s, p, i),
                        dst_ref=final(s, p, i),
                        send_sem=side_send.at[s, p],
                        recv_sem=side_recv.at[s, p],
                        device_id=dev(z, y, x, 1 - q),
                        device_id_type=MESH,
                    ).start()
                    pltpu.make_async_copy(held(s, p, i), final(s, p, i), out_sem.at[s, p]).start()

        return carry

    lax.fori_loop(0, N + max(map(max, DEPTH)), step, 0)

    for s in range(2):
        rel, relay = state[s][:2]
        for p in range(3):

            @pl.when(relay)
            def _():
                for m in range(2):
                    nodes = [r for r in range(8) if len(CHILDREN[p][r]) > m]
                    if not nodes:
                        continue

                    @pl.when(table(rel, [1 if r in nodes else 0 for r in range(8)]) == 1)
                    def _():
                        pltpu.make_async_copy(held(s, p), held(s, p), send_sem.at[s, p, m]).wait()

                pltpu.make_async_copy(held(s, p), held(s, p), side_send.at[s, p]).wait()
                pltpu.make_async_copy(held(s, p), final(s, p), out_sem.at[s, p]).wait()

            @pl.when(jnp.logical_not(relay))
            def _():
                pltpu.make_async_copy(final(s, p), final(s, p), side_recv.at[s, p]).wait()


def place_kernel(slots, home13, homed, hot13, hotd, out13, outd, va, vb, zero, in_sem, out_sem):
    me = lax.axis_index("stage") * 8 + lax.axis_index("expert")
    vah, vaH = va
    vbh, vbH = vb
    zero[...] = jnp.zeros_like(zero)
    pairs = []
    for g in range(4):
        layer, r = g // 2, g % 2
        rows = pl.ds(r * 1024, 1024)
        pairs.append((home13.at[layer, rows], vah.at[layer, rows], lambda t, layer=layer, rows=rows: out13.at[layer, t, rows], False, 0))
        pairs.append((hot13.at[layer, rows], vaH.at[layer, rows], lambda t, layer=layer, rows=rows: out13.at[layer, t, rows], True, 0))
    for layer in range(2):
        pairs.append((homed.at[layer], vbh.at[layer], lambda t, layer=layer: outd.at[layer, t], False, 1))
        pairs.append((hotd.at[layer], vbH.at[layer], lambda t, layer=layer: outd.at[layer, t], True, 1))
    for n, (src, mid, out, hot, kind) in enumerate(pairs):
        pltpu.make_async_copy(src, mid, in_sem.at[n]).start()
    for n, (src, mid, out, hot, kind) in enumerate(pairs):
        pltpu.make_async_copy(src, mid, in_sem.at[n]).wait()
        if not hot:
            pltpu.make_async_copy(mid, out(0), out_sem).start()
            continue
        for t in (1, 2):
            filled = slots[me, t - 1] >= 0

            @pl.when(filled)
            def _():
                pltpu.make_async_copy(mid, out(t), out_sem).start()

            @pl.when(jnp.logical_not(filled))
            def _():
                if kind == 0:
                    pltpu.make_async_copy(zero, out(t), out_sem).start()
                else:
                    for h in range(2):
                        pltpu.make_async_copy(zero.at[pl.ds(0, 512)], out(t).at[:, pl.ds(h * 1024, 1024)], out_sem).start()
    for n, (src, mid, out, hot, kind) in enumerate(pairs):
        for t in (1, 2) if hot else (0,):
            pltpu.make_async_copy(mid, out(t), out_sem).wait()


def solution(mesh):
    DMA = pltpu.SemaphoreType.DMA

    def local(gate, up, down, hot_units, slot_map):
        units13 = jax.ShapeDtypeStruct((2, 2048, 1024), BF16)
        unitsd = jax.ShapeDtypeStruct((2, 512, 2048), BF16)
        params = pltpu.CompilerParams(has_side_effects=True, vmem_limit_bytes=48 << 20)
        home13, homed = pl.pallas_call(
            home_kernel,
            out_shape=(units13, unitsd),
            in_specs=[ANY] * 3,
            out_specs=(ANY, ANY),
            scratch_shapes=[
                pltpu.VMEM((2, 2, 2048, 512), BF16),
                pltpu.VMEM((2, 512, 2048), BF16),
                DMA((2, 3)),
                DMA((2, 3)),
                DMA((2, 3)),
            ],
            compiler_params=params,
            name="home",
        )(gate, up, down)

        def hot(unit):
            return pl.pallas_call(
                functools.partial(hot_kernel, unit),
                out_shape=(units13, unitsd),
                in_specs=[ANY] * 3,
                out_specs=(ANY, ANY),
                scratch_shapes=[
                    pltpu.VMEM((2, 2, 2048, 512), BF16),
                    pltpu.VMEM((2, 512, 2048), BF16),
                    DMA((3,)),
                    DMA((2, 3, N)),
                    DMA((2, 3, 2)),
                    DMA((2, 3)),
                    DMA((2, 3)),
                    DMA((2, 3)),
                ],
                compiler_params=params,
                name=f"hot{unit}",
            )

        hot13, hotd = lax.switch(hot_units[0], [hot(u) for u in range(16)], gate, up, down)
        return pl.pallas_call(
            place_kernel,
            out_shape=(
                jax.ShapeDtypeStruct((2, 3, 2048, 1024), BF16),
                jax.ShapeDtypeStruct((2, 3, 512, 2048), BF16),
            ),
            in_specs=[pl.BlockSpec(memory_space=pltpu.SMEM)] + [ANY] * 4,
            out_specs=(ANY, ANY),
            scratch_shapes=[
                [pltpu.VMEM((2, 2048, 1024), BF16)] * 2,
                [pltpu.VMEM((2, 512, 2048), BF16)] * 2,
                pltpu.VMEM((1024, 1024), BF16),
                DMA((12,)),
                DMA,
            ],
            compiler_params=pltpu.CompilerParams(vmem_limit_bytes=48 << 20),
            name="place",
        )(slot_map, home13, homed, hot13, hotd)

    spec = P("stage", "expert")
    out = P(None, ("stage", "expert"))
    return jax.shard_map(local, mesh=mesh, in_specs=(spec, spec, spec, P(), P()), out_specs=(out, out), check_vma=False)
```

```python
import functools

import jax
import jax.numpy as jnp
from jax import lax
from jax.experimental import pallas as pl
from jax.experimental.pallas import tpu as pltpu
from jax.sharding import PartitionSpec as P

MESH = pl.DeviceIdType.MESH
ANY = pl.BlockSpec(memory_space=pl.ANY)
BF16 = jnp.bfloat16

PARENT = (
    (None, 0, 3, 1, 5, 1, 7, 5),
    (None, 3, 0, 2, 6, 7, 2, 3),
    (None, 5, 6, 7, 0, 4, 4, 6),
)
DEPTH = (
    (0, 1, 3, 2, 3, 2, 4, 3),
    (0, 3, 1, 2, 3, 4, 2, 3),
    (0, 3, 3, 4, 1, 2, 2, 3),
)
CHILDREN = tuple(tuple(tuple(v for v in range(1, 8) if par[v] == r) for r in range(8)) for par in PARENT)
DEEPEST = max(map(max, DEPTH))
N = 16
WINDOW = 3


def coords():
    z = lax.axis_index("stage")
    j = lax.axis_index("expert")
    return z, j // 4, (j // 2) % 2, j % 2


def dev(z, y, x, q):
    return (z, y * 4 + x * 2 + q)


def flip(v, bit):
    return 1 - v if bit else v


def table(index, values):
    out = jnp.int32(values[0])
    for i, v in enumerate(values[1:], 1):
        if v != values[0]:
            out = jnp.where(index == i, jnp.int32(v), out)
    return out


def move_kernel(unit, gate, up, down, home13, homed, hot13, hotd, vg, vd, load_sem, recv_sem, send_sem, side_send, side_recv, out_sem, home_send, home_recv):
    e, half = unit // 2, unit % 2
    ra, rb, rc = e // 4, (e // 2) % 2, e % 2
    z, y, x, q = coords()

    def source(k, p, i=None):
        if p == 2:
            return down.at[0, 0, pl.ds(k * 512, 512), :] if i is None else down.at[0, 0, pl.ds(k * 512 + i * (512 // N), 512 // N), :]
        cols = pl.ds(k * 512, 512)
        return (gate, up)[p].at[0, 0, :, cols] if i is None else (gate, up)[p].at[0, 0, pl.ds(i * (2048 // N), 2048 // N), cols]

    def held(s, p, i=None):
        if p == 2:
            return vd.at[s] if i is None else vd.at[s, pl.ds(i * (512 // N), 512 // N), :]
        return vg.at[s, p] if i is None else vg.at[s, p, pl.ds(i * (2048 // N), 2048 // N), :]

    def place(out13, outd, s, p, i=None):
        if p == 2:
            return outd.at[s] if i is None else outd.at[s, pl.ds(i * (512 // N), 512 // N), :]
        cols = pl.ds(p * 512, 512)
        return out13.at[s, :, cols] if i is None else out13.at[s, pl.ds(i * (2048 // N), 2048 // N), cols]

    final = functools.partial(place, hot13, hotd)
    home = functools.partial(place, home13, homed)

    state = []
    for s in range(2):
        fz, fy, fx = flip(z, s), flip(y, ra), flip(x, rb)
        rel = fz * 4 + fy * 2 + fx
        relay = q == jnp.where(rel == 0, rc, s)
        state.append((rel, relay, fz, fy, fx))

    for s in range(2):
        rel, relay = state[s][:2]

        @pl.when(relay & (rel == 0))
        def _():
            for p in range(3):
                pltpu.make_async_copy(source(half, p), held(s, p), load_sem.at[p]).start()
            for p in range(3):
                pltpu.make_async_copy(source(half, p), held(s, p), load_sem.at[p]).wait()

    def hot_wave(t):
        for s in range(2):
            rel, relay, fz, fy, fx = state[s]
            for p in range(3):
                i = t - table(rel, DEPTH[p])

                @pl.when(relay & (i >= 0) & (i < N))
                def _():
                    @pl.when(rel != 0)
                    def _():
                        pltpu.make_async_copy(held(s, p, i), held(s, p, i), recv_sem.at[s, p, i]).wait()

                    for m in range(2):
                        nodes = [r for r in range(8) if len(CHILDREN[p][r]) > m]
                        if not nodes:
                            continue
                        child = table(rel, [CHILDREN[p][r][m] if r in nodes else -1 for r in range(8)])

                        @pl.when(child >= 0)
                        def _():
                            to = dev(flip(child // 4, s), flip((child // 2) % 2, ra), flip(child % 2, rb), s)
                            pltpu.make_async_remote_copy(
                                src_ref=held(s, p, i),
                                dst_ref=held(s, p, i),
                                send_sem=send_sem.at[s, p, m],
                                recv_sem=recv_sem.at[s, p, i],
                                device_id=to,
                                device_id_type=MESH,
                            ).start()

                    pltpu.make_async_remote_copy(
                        src_ref=held(s, p, i),
                        dst_ref=final(s, p, i),
                        send_sem=side_send.at[s, p],
                        recv_sem=side_recv.at[s, p],
                        device_id=dev(z, y, x, 1 - q),
                        device_id_type=MESH,
                    ).start()
                    pltpu.make_async_copy(held(s, p, i), final(s, p, i), out_sem.at[s, p]).start()

    stay = [(z == y) & (y == x) & (x == q) & (q == k) for k in range(2)]

    def home_copy(k, p, i, slot):
        return pltpu.make_async_remote_copy(
            src_ref=source(k, p, i),
            dst_ref=home(z, p, i),
            send_sem=home_send.at[k, slot],
            recv_sem=home_recv.at[z, p],
            device_id=dev(y, x, q, k),
            device_id_type=MESH,
        )

    def step(g, carry):
        @pl.when(g < N + DEEPEST)
        def _():
            hot_wave(g)

        slot = g % WINDOW
        for k in range(2):

            @pl.when(jnp.logical_not(stay[k]) & (g >= WINDOW))
            def _():
                home_copy(k, 0, 0, slot).wait_send()

            for p in range(3):

                @pl.when((g % 3 == p) & jnp.logical_not(stay[k]))
                def _():
                    home_copy(k, p, g // 3, slot).start()

                @pl.when((g % 3 == p) & stay[k])
                def _():
                    pltpu.make_async_copy(source(k, p, g // 3), home(z, p, g // 3), home_recv.at[z, p]).start()

        return carry

    lax.fori_loop(0, 3 * N, step, 0)

    for k in range(2):

        @pl.when(jnp.logical_not(stay[k]))
        def _():
            for slot in range(WINDOW):
                home_copy(k, 0, 0, slot).wait_send()

    for s in range(2):
        rel, relay = state[s][:2]
        for p in range(3):
            pltpu.make_async_copy(home(s, p), home(s, p), home_recv.at[s, p]).wait()

            @pl.when(relay)
            def _():
                for m in range(2):
                    nodes = [r for r in range(8) if len(CHILDREN[p][r]) > m]
                    if not nodes:
                        continue

                    @pl.when(table(rel, [1 if r in nodes else 0 for r in range(8)]) == 1)
                    def _():
                        pltpu.make_async_copy(held(s, p), held(s, p), send_sem.at[s, p, m]).wait()

                pltpu.make_async_copy(held(s, p), held(s, p), side_send.at[s, p]).wait()
                pltpu.make_async_copy(held(s, p), final(s, p), out_sem.at[s, p]).wait()

            @pl.when(jnp.logical_not(relay))
            def _():
                pltpu.make_async_copy(final(s, p), final(s, p), side_recv.at[s, p]).wait()


def place_kernel(slots, home13, homed, hot13, hotd, out13, outd, va, vb, zero, in_sem, out_sem):
    me = lax.axis_index("stage") * 8 + lax.axis_index("expert")
    vah, vaH = va
    vbh, vbH = vb
    zero[...] = jnp.zeros_like(zero)
    pairs = []
    for g in range(4):
        layer, r = g // 2, g % 2
        rows = pl.ds(r * 1024, 1024)
        pairs.append((home13.at[layer, rows], vah.at[layer, rows], lambda t, layer=layer, rows=rows: out13.at[layer, t, rows], False, 0))
        pairs.append((hot13.at[layer, rows], vaH.at[layer, rows], lambda t, layer=layer, rows=rows: out13.at[layer, t, rows], True, 0))
    for layer in range(2):
        pairs.append((homed.at[layer], vbh.at[layer], lambda t, layer=layer: outd.at[layer, t], False, 1))
        pairs.append((hotd.at[layer], vbH.at[layer], lambda t, layer=layer: outd.at[layer, t], True, 1))
    for n, (src, mid, out, hot, kind) in enumerate(pairs):
        pltpu.make_async_copy(src, mid, in_sem.at[n]).start()
    for n, (src, mid, out, hot, kind) in enumerate(pairs):
        pltpu.make_async_copy(src, mid, in_sem.at[n]).wait()
        if not hot:
            pltpu.make_async_copy(mid, out(0), out_sem).start()
            continue
        for t in (1, 2):
            filled = slots[me, t - 1] >= 0

            @pl.when(filled)
            def _():
                pltpu.make_async_copy(mid, out(t), out_sem).start()

            @pl.when(jnp.logical_not(filled))
            def _():
                if kind == 0:
                    pltpu.make_async_copy(zero, out(t), out_sem).start()
                else:
                    for h in range(2):
                        pltpu.make_async_copy(zero.at[pl.ds(0, 512)], out(t).at[:, pl.ds(h * 1024, 1024)], out_sem).start()
    for n, (src, mid, out, hot, kind) in enumerate(pairs):
        for t in (1, 2) if hot else (0,):
            pltpu.make_async_copy(mid, out(t), out_sem).wait()


def solution(mesh):
    DMA = pltpu.SemaphoreType.DMA

    def local(gate, up, down, hot_units, slot_map):
        units13 = jax.ShapeDtypeStruct((2, 2048, 1024), BF16)
        unitsd = jax.ShapeDtypeStruct((2, 512, 2048), BF16)
        params = pltpu.CompilerParams(has_side_effects=True, vmem_limit_bytes=48 << 20)
        def move(unit):
            return pl.pallas_call(
                functools.partial(move_kernel, unit),
                out_shape=(units13, unitsd) * 2,
                in_specs=[ANY] * 3,
                out_specs=(ANY,) * 4,
                scratch_shapes=[
                    pltpu.VMEM((2, 2, 2048, 512), BF16),
                    pltpu.VMEM((2, 512, 2048), BF16),
                    DMA((3,)),
                    DMA((2, 3, N)),
                    DMA((2, 3, 2)),
                    DMA((2, 3)),
                    DMA((2, 3)),
                    DMA((2, 3)),
                    DMA((2, WINDOW)),
                    DMA((2, 3)),
                ],
                compiler_params=params,
                name=f"move{unit}",
            )

        moved = lax.switch(hot_units[0], [move(u) for u in range(16)], gate, up, down)
        return pl.pallas_call(
            place_kernel,
            out_shape=(
                jax.ShapeDtypeStruct((2, 3, 2048, 1024), BF16),
                jax.ShapeDtypeStruct((2, 3, 512, 2048), BF16),
            ),
            in_specs=[pl.BlockSpec(memory_space=pltpu.SMEM)] + [ANY] * 4,
            out_specs=(ANY, ANY),
            scratch_shapes=[
                [pltpu.VMEM((2, 2048, 1024), BF16)] * 2,
                [pltpu.VMEM((2, 512, 2048), BF16)] * 2,
                pltpu.VMEM((1024, 1024), BF16),
                DMA((12,)),
                DMA,
            ],
            compiler_params=pltpu.CompilerParams(vmem_limit_bytes=48 << 20),
            name="place",
        )(slot_map, *moved)

    spec = P("stage", "expert")
    out = P(None, ("stage", "expert"))
    return jax.shard_map(local, mesh=mesh, in_specs=(spec, spec, spec, P(), P()), out_specs=(out, out), check_vma=False)
```

```python
import functools

import jax
import jax.numpy as jnp
from jax import lax
from jax.experimental import pallas as pl
from jax.experimental.pallas import tpu as pltpu
from jax.sharding import PartitionSpec as P

MESH = pl.DeviceIdType.MESH
ANY = pl.BlockSpec(memory_space=pl.ANY)
BF16 = jnp.bfloat16

PARENT = (
    (None, 0, 3, 1, 5, 1, 7, 5),
    (None, 3, 0, 2, 6, 7, 2, 3),
    (None, 5, 6, 7, 0, 4, 4, 6),
)
DEPTH = (
    (0, 1, 3, 2, 3, 2, 4, 3),
    (0, 3, 1, 2, 3, 4, 2, 3),
    (0, 3, 3, 4, 1, 2, 2, 3),
)
CHILDREN = tuple(tuple(tuple(v for v in range(1, 8) if par[v] == r) for r in range(8)) for par in PARENT)
DEEPEST = max(map(max, DEPTH))
N = 16
WINDOW = 3


def coords():
    z = lax.axis_index("stage")
    j = lax.axis_index("expert")
    return z, j // 4, (j // 2) % 2, j % 2


def dev(z, y, x, q):
    return (z, y * 4 + x * 2 + q)


def flip(v, bit):
    return 1 - v if bit else v


def table(index, values):
    out = jnp.int32(values[0])
    for i, v in enumerate(values[1:], 1):
        if v != values[0]:
            out = jnp.where(index == i, jnp.int32(v), out)
    return out


def move_kernel(unit, gate, up, down, home13, homed, hot13, hotd, vg, vd, sg, sd, load_sem, stage_sem, recv_sem, send_sem, side_send, side_recv, out_sem, home_send, home_recv):
    e, half = unit // 2, unit % 2
    ra, rb, rc = e // 4, (e // 2) % 2, e % 2
    z, y, x, q = coords()

    def source(k, p, i=None):
        if p == 2:
            return down.at[0, 0, pl.ds(k * 512, 512), :] if i is None else down.at[0, 0, pl.ds(k * 512 + i * (512 // N), 512 // N), :]
        cols = pl.ds(k * 512, 512)
        return (gate, up)[p].at[0, 0, :, cols] if i is None else (gate, up)[p].at[0, 0, pl.ds(i * (2048 // N), 2048 // N), cols]

    def staged(k, p, i=None):
        if p == 2:
            return sd.at[k] if i is None else sd.at[k, pl.ds(i * (512 // N), 512 // N), :]
        return sg.at[k, p] if i is None else sg.at[k, p, pl.ds(i * (2048 // N), 2048 // N), :]

    def held(s, p, i=None):
        if p == 2:
            return vd.at[s] if i is None else vd.at[s, pl.ds(i * (512 // N), 512 // N), :]
        return vg.at[s, p] if i is None else vg.at[s, p, pl.ds(i * (2048 // N), 2048 // N), :]

    def place(out13, outd, s, p, i=None):
        if p == 2:
            return outd.at[s] if i is None else outd.at[s, pl.ds(i * (512 // N), 512 // N), :]
        cols = pl.ds(p * 512, 512)
        return out13.at[s, :, cols] if i is None else out13.at[s, pl.ds(i * (2048 // N), 2048 // N), cols]

    final = functools.partial(place, hot13, hotd)
    home = functools.partial(place, home13, homed)

    state = []
    for s in range(2):
        fz, fy, fx = flip(z, s), flip(y, ra), flip(x, rb)
        rel = fz * 4 + fy * 2 + fx
        relay = q == jnp.where(rel == 0, rc, s)
        state.append((rel, relay, fz, fy, fx))

    for p in range(3):
        for k in range(2):
            pltpu.make_async_copy(source(k, p), staged(k, p), stage_sem.at[k, p]).start()

    for s in range(2):
        rel, relay = state[s][:2]

        @pl.when(relay & (rel == 0))
        def _():
            for p in range(3):
                pltpu.make_async_copy(source(half, p), held(s, p), load_sem.at[p]).start()
            for p in range(3):
                pltpu.make_async_copy(source(half, p), held(s, p), load_sem.at[p]).wait()

    def hot_wave(t):
        for s in range(2):
            rel, relay, fz, fy, fx = state[s]
            for p in range(3):
                i = t - table(rel, DEPTH[p])

                @pl.when(relay & (i >= 0) & (i < N))
                def _():
                    @pl.when(rel != 0)
                    def _():
                        pltpu.make_async_copy(held(s, p, i), held(s, p, i), recv_sem.at[s, p, i]).wait()

                    for m in range(2):
                        nodes = [r for r in range(8) if len(CHILDREN[p][r]) > m]
                        if not nodes:
                            continue
                        child = table(rel, [CHILDREN[p][r][m] if r in nodes else -1 for r in range(8)])

                        @pl.when(child >= 0)
                        def _():
                            to = dev(flip(child // 4, s), flip((child // 2) % 2, ra), flip(child % 2, rb), s)
                            pltpu.make_async_remote_copy(
                                src_ref=held(s, p, i),
                                dst_ref=held(s, p, i),
                                send_sem=send_sem.at[s, p, m],
                                recv_sem=recv_sem.at[s, p, i],
                                device_id=to,
                                device_id_type=MESH,
                            ).start()

                    pltpu.make_async_remote_copy(
                        src_ref=held(s, p, i),
                        dst_ref=final(s, p, i),
                        send_sem=side_send.at[s, p],
                        recv_sem=side_recv.at[s, p],
                        device_id=dev(z, y, x, 1 - q),
                        device_id_type=MESH,
                    ).start()
                    pltpu.make_async_copy(held(s, p, i), final(s, p, i), out_sem.at[s, p]).start()

    stay = [(z == y) & (y == x) & (x == q) & (q == k) for k in range(2)]

    def home_copy(k, p, i, slot):
        return pltpu.make_async_remote_copy(
            src_ref=staged(k, p, i),
            dst_ref=home(z, p, i),
            send_sem=home_send.at[k, slot],
            recv_sem=home_recv.at[z, p],
            device_id=dev(y, x, q, k),
            device_id_type=MESH,
        )

    for p in range(3):
        for k in range(2):
            pltpu.make_async_copy(source(k, p), staged(k, p), stage_sem.at[k, p]).wait()

    def step(g, carry):
        @pl.when(g < N + DEEPEST)
        def _():
            hot_wave(g)

        slot = g % WINDOW
        for k in range(2):

            @pl.when(jnp.logical_not(stay[k]) & (g >= WINDOW))
            def _():
                home_copy(k, 0, 0, slot).wait_send()

            for p in range(3):

                @pl.when((g % 3 == p) & jnp.logical_not(stay[k]))
                def _():
                    home_copy(k, p, g // 3, slot).start()

                @pl.when((g % 3 == p) & stay[k])
                def _():
                    pltpu.make_async_copy(staged(k, p, g // 3), home(z, p, g // 3), home_recv.at[z, p]).start()

        return carry

    lax.fori_loop(0, 3 * N, step, 0)

    for k in range(2):

        @pl.when(jnp.logical_not(stay[k]))
        def _():
            for slot in range(WINDOW):
                home_copy(k, 0, 0, slot).wait_send()

    for s in range(2):
        rel, relay = state[s][:2]
        for p in range(3):
            pltpu.make_async_copy(home(s, p), home(s, p), home_recv.at[s, p]).wait()

            @pl.when(relay)
            def _():
                for m in range(2):
                    nodes = [r for r in range(8) if len(CHILDREN[p][r]) > m]
                    if not nodes:
                        continue

                    @pl.when(table(rel, [1 if r in nodes else 0 for r in range(8)]) == 1)
                    def _():
                        pltpu.make_async_copy(held(s, p), held(s, p), send_sem.at[s, p, m]).wait()

                pltpu.make_async_copy(held(s, p), held(s, p), side_send.at[s, p]).wait()
                pltpu.make_async_copy(held(s, p), final(s, p), out_sem.at[s, p]).wait()

            @pl.when(jnp.logical_not(relay))
            def _():
                pltpu.make_async_copy(final(s, p), final(s, p), side_recv.at[s, p]).wait()


def place_kernel(slots, home13, homed, hot13, hotd, out13, outd, va, vb, zero, in_sem, out_sem):
    me = lax.axis_index("stage") * 8 + lax.axis_index("expert")
    vah, vaH = va
    vbh, vbH = vb
    zero[...] = jnp.zeros_like(zero)
    pairs = []
    for g in range(4):
        layer, r = g // 2, g % 2
        rows = pl.ds(r * 1024, 1024)
        pairs.append((home13.at[layer, rows], vah.at[layer, rows], lambda t, layer=layer, rows=rows: out13.at[layer, t, rows], False, 0))
        pairs.append((hot13.at[layer, rows], vaH.at[layer, rows], lambda t, layer=layer, rows=rows: out13.at[layer, t, rows], True, 0))
    for layer in range(2):
        pairs.append((homed.at[layer], vbh.at[layer], lambda t, layer=layer: outd.at[layer, t], False, 1))
        pairs.append((hotd.at[layer], vbH.at[layer], lambda t, layer=layer: outd.at[layer, t], True, 1))
    for n, (src, mid, out, hot, kind) in enumerate(pairs):
        pltpu.make_async_copy(src, mid, in_sem.at[n]).start()
    for n, (src, mid, out, hot, kind) in enumerate(pairs):
        pltpu.make_async_copy(src, mid, in_sem.at[n]).wait()
        if not hot:
            pltpu.make_async_copy(mid, out(0), out_sem).start()
            continue
        for t in (1, 2):
            filled = slots[me, t - 1] >= 0

            @pl.when(filled)
            def _():
                pltpu.make_async_copy(mid, out(t), out_sem).start()

            @pl.when(jnp.logical_not(filled))
            def _():
                if kind == 0:
                    pltpu.make_async_copy(zero, out(t), out_sem).start()
                else:
                    for h in range(2):
                        pltpu.make_async_copy(zero.at[pl.ds(0, 512)], out(t).at[:, pl.ds(h * 1024, 1024)], out_sem).start()
    for n, (src, mid, out, hot, kind) in enumerate(pairs):
        for t in (1, 2) if hot else (0,):
            pltpu.make_async_copy(mid, out(t), out_sem).wait()


def solution(mesh):
    DMA = pltpu.SemaphoreType.DMA

    def local(gate, up, down, hot_units, slot_map):
        units13 = jax.ShapeDtypeStruct((2, 2048, 1024), BF16)
        unitsd = jax.ShapeDtypeStruct((2, 512, 2048), BF16)
        params = pltpu.CompilerParams(has_side_effects=True, vmem_limit_bytes=48 << 20)
        def move(unit):
            return pl.pallas_call(
                functools.partial(move_kernel, unit),
                out_shape=(units13, unitsd) * 2,
                in_specs=[ANY] * 3,
                out_specs=(ANY,) * 4,
                scratch_shapes=[
                    pltpu.VMEM((2, 2, 2048, 512), BF16),
                    pltpu.VMEM((2, 512, 2048), BF16),
                    pltpu.VMEM((2, 2, 2048, 512), BF16),
                    pltpu.VMEM((2, 512, 2048), BF16),
                    DMA((3,)),
                    DMA((2, 3)),
                    DMA((2, 3, N)),
                    DMA((2, 3, 2)),
                    DMA((2, 3)),
                    DMA((2, 3)),
                    DMA((2, 3)),
                    DMA((2, WINDOW)),
                    DMA((2, 3)),
                ],
                compiler_params=params,
                name=f"move{unit}",
            )

        moved = lax.switch(hot_units[0], [move(u) for u in range(16)], gate, up, down)
        return pl.pallas_call(
            place_kernel,
            out_shape=(
                jax.ShapeDtypeStruct((2, 3, 2048, 1024), BF16),
                jax.ShapeDtypeStruct((2, 3, 512, 2048), BF16),
            ),
            in_specs=[pl.BlockSpec(memory_space=pltpu.SMEM)] + [ANY] * 4,
            out_specs=(ANY, ANY),
            scratch_shapes=[
                [pltpu.VMEM((2, 2048, 1024), BF16)] * 2,
                [pltpu.VMEM((2, 512, 2048), BF16)] * 2,
                pltpu.VMEM((1024, 1024), BF16),
                DMA((12,)),
                DMA,
            ],
            compiler_params=pltpu.CompilerParams(vmem_limit_bytes=48 << 20),
            name="place",
        )(slot_map, *moved)

    spec = P("stage", "expert")
    out = P(None, ("stage", "expert"))
    return jax.shard_map(local, mesh=mesh, in_specs=(spec, spec, spec, P(), P()), out_specs=(out, out), check_vma=False)
```

```python
import functools

import jax
import jax.numpy as jnp
from jax import lax
from jax.experimental import pallas as pl
from jax.experimental.pallas import tpu as pltpu
from jax.sharding import PartitionSpec as P

MESH = pl.DeviceIdType.MESH
ANY = pl.BlockSpec(memory_space=pl.ANY)
BF16 = jnp.bfloat16

PARENT = (
    (None, 0, 3, 1, 5, 1, 7, 5),
    (None, 3, 0, 2, 6, 7, 2, 3),
    (None, 5, 6, 7, 0, 4, 4, 6),
)
DEPTH = (
    (0, 1, 3, 2, 3, 2, 4, 3),
    (0, 3, 1, 2, 3, 4, 2, 3),
    (0, 3, 3, 4, 1, 2, 2, 3),
)
CHILDREN = tuple(tuple(tuple(v for v in range(1, 8) if par[v] == r) for r in range(8)) for par in PARENT)
DEEPEST = max(map(max, DEPTH))
N = 16
LAG = 4
WINDOW = 3


def coords():
    z = lax.axis_index("stage")
    j = lax.axis_index("expert")
    return z, j // 4, (j // 2) % 2, j % 2


def dev(z, y, x, q):
    return (z, y * 4 + x * 2 + q)


def flip(v, bit):
    return 1 - v if bit else v


def table(index, values):
    out = jnp.int32(values[0])
    for i, v in enumerate(values[1:], 1):
        if v != values[0]:
            out = jnp.where(index == i, jnp.int32(v), out)
    return out


def move_kernel(unit, gate, up, down, home13, homed, hot13, hotd, vg, vd, sg, sd, load_sem, stage_sem, recv_sem, send_sem, side_send, side_recv, out_sem, home_send, home_recv):
    e, half = unit // 2, unit % 2
    ra, rb, rc = e // 4, (e // 2) % 2, e % 2
    z, y, x, q = coords()

    def source(k, p, i=None):
        if p == 2:
            return down.at[0, 0, pl.ds(k * 512, 512), :] if i is None else down.at[0, 0, pl.ds(k * 512 + i * (512 // N), 512 // N), :]
        cols = pl.ds(k * 512, 512)
        return (gate, up)[p].at[0, 0, :, cols] if i is None else (gate, up)[p].at[0, 0, pl.ds(i * (2048 // N), 2048 // N), cols]

    def staged(k, p, i=None):
        if p == 2:
            return sd.at[k] if i is None else sd.at[k, pl.ds(i * (512 // N), 512 // N), :]
        return sg.at[k, p] if i is None else sg.at[k, p, pl.ds(i * (2048 // N), 2048 // N), :]

    def held(s, p, i=None):
        if p == 2:
            return vd.at[s] if i is None else vd.at[s, pl.ds(i * (512 // N), 512 // N), :]
        return vg.at[s, p] if i is None else vg.at[s, p, pl.ds(i * (2048 // N), 2048 // N), :]

    def place(out13, outd, s, p, i=None):
        if p == 2:
            return outd.at[s] if i is None else outd.at[s, pl.ds(i * (512 // N), 512 // N), :]
        cols = pl.ds(p * 512, 512)
        return out13.at[s, :, cols] if i is None else out13.at[s, pl.ds(i * (2048 // N), 2048 // N), cols]

    final = functools.partial(place, hot13, hotd)
    home = functools.partial(place, home13, homed)

    state = []
    for s in range(2):
        fz, fy, fx = flip(z, s), flip(y, ra), flip(x, rb)
        rel = fz * 4 + fy * 2 + fx
        relay = q == jnp.where(rel == 0, rc, s)
        state.append((rel, relay, fz, fy, fx))

    for p in range(3):
        for k in range(2):
            pltpu.make_async_copy(source(k, p), staged(k, p), stage_sem.at[k, p]).start()

    for s in range(2):
        rel, relay = state[s][:2]

        @pl.when(relay & (rel == 0))
        def _():
            for p in range(3):
                pltpu.make_async_copy(source(half, p), held(s, p), load_sem.at[p]).start()
            for p in range(3):
                pltpu.make_async_copy(source(half, p), held(s, p), load_sem.at[p]).wait()

    def hot_wave(t):
        for s in range(2):
            rel, relay, fz, fy, fx = state[s]
            for p in range(3):
                i = t - LAG * table(rel, DEPTH[p])

                @pl.when(relay & (i >= 0) & (i < N))
                def _():
                    @pl.when(rel != 0)
                    def _():
                        pltpu.make_async_copy(held(s, p, i), held(s, p, i), recv_sem.at[s, p, i]).wait()

                    for m in range(2):
                        nodes = [r for r in range(8) if len(CHILDREN[p][r]) > m]
                        if not nodes:
                            continue
                        child = table(rel, [CHILDREN[p][r][m] if r in nodes else -1 for r in range(8)])

                        @pl.when(child >= 0)
                        def _():
                            to = dev(flip(child // 4, s), flip((child // 2) % 2, ra), flip(child % 2, rb), s)
                            pltpu.make_async_remote_copy(
                                src_ref=held(s, p, i),
                                dst_ref=held(s, p, i),
                                send_sem=send_sem.at[s, p, m],
                                recv_sem=recv_sem.at[s, p, i],
                                device_id=to,
                                device_id_type=MESH,
                            ).start()

                    pltpu.make_async_remote_copy(
                        src_ref=held(s, p, i),
                        dst_ref=final(s, p, i),
                        send_sem=side_send.at[s, p],
                        recv_sem=side_recv.at[s, p],
                        device_id=dev(z, y, x, 1 - q),
                        device_id_type=MESH,
                    ).start()
                    pltpu.make_async_copy(held(s, p, i), final(s, p, i), out_sem.at[s, p]).start()

    stay = [(z == y) & (y == x) & (x == q) & (q == k) for k in range(2)]

    def home_copy(k, p, i, slot):
        return pltpu.make_async_remote_copy(
            src_ref=staged(k, p, i),
            dst_ref=home(z, p, i),
            send_sem=home_send.at[k, slot],
            recv_sem=home_recv.at[z, p],
            device_id=dev(y, x, q, k),
            device_id_type=MESH,
        )

    for p in range(3):
        for k in range(2):
            pltpu.make_async_copy(source(k, p), staged(k, p), stage_sem.at[k, p]).wait()

    def step(g, carry):
        @pl.when(g < N + LAG * DEEPEST)
        def _():
            hot_wave(g)

        slot = g % WINDOW
        for k in range(2):

            @pl.when(jnp.logical_not(stay[k]) & (g >= WINDOW))
            def _():
                home_copy(k, 0, 0, slot).wait_send()

            for p in range(3):

                @pl.when((g % 3 == p) & jnp.logical_not(stay[k]))
                def _():
                    home_copy(k, p, g // 3, slot).start()

                @pl.when((g % 3 == p) & stay[k])
                def _():
                    pltpu.make_async_copy(staged(k, p, g // 3), home(z, p, g // 3), home_recv.at[z, p]).start()

        return carry

    lax.fori_loop(0, 3 * N, step, 0)

    for k in range(2):

        @pl.when(jnp.logical_not(stay[k]))
        def _():
            for slot in range(WINDOW):
                home_copy(k, 0, 0, slot).wait_send()

    for s in range(2):
        rel, relay = state[s][:2]
        for p in range(3):
            pltpu.make_async_copy(home(s, p), home(s, p), home_recv.at[s, p]).wait()

            @pl.when(relay)
            def _():
                for m in range(2):
                    nodes = [r for r in range(8) if len(CHILDREN[p][r]) > m]
                    if not nodes:
                        continue

                    @pl.when(table(rel, [1 if r in nodes else 0 for r in range(8)]) == 1)
                    def _():
                        pltpu.make_async_copy(held(s, p), held(s, p), send_sem.at[s, p, m]).wait()

                pltpu.make_async_copy(held(s, p), held(s, p), side_send.at[s, p]).wait()
                pltpu.make_async_copy(held(s, p), final(s, p), out_sem.at[s, p]).wait()

            @pl.when(jnp.logical_not(relay))
            def _():
                pltpu.make_async_copy(final(s, p), final(s, p), side_recv.at[s, p]).wait()


def place_kernel(slots, home13, homed, hot13, hotd, out13, outd, va, vb, zero, in_sem, out_sem):
    me = lax.axis_index("stage") * 8 + lax.axis_index("expert")
    vah, vaH = va
    vbh, vbH = vb
    zero[...] = jnp.zeros_like(zero)
    pairs = []
    for g in range(4):
        layer, r = g // 2, g % 2
        rows = pl.ds(r * 1024, 1024)
        pairs.append((home13.at[layer, rows], vah.at[layer, rows], lambda t, layer=layer, rows=rows: out13.at[layer, t, rows], False, 0))
        pairs.append((hot13.at[layer, rows], vaH.at[layer, rows], lambda t, layer=layer, rows=rows: out13.at[layer, t, rows], True, 0))
    for layer in range(2):
        pairs.append((homed.at[layer], vbh.at[layer], lambda t, layer=layer: outd.at[layer, t], False, 1))
        pairs.append((hotd.at[layer], vbH.at[layer], lambda t, layer=layer: outd.at[layer, t], True, 1))
    for n, (src, mid, out, hot, kind) in enumerate(pairs):
        pltpu.make_async_copy(src, mid, in_sem.at[n]).start()
    for n, (src, mid, out, hot, kind) in enumerate(pairs):
        pltpu.make_async_copy(src, mid, in_sem.at[n]).wait()
        if not hot:
            pltpu.make_async_copy(mid, out(0), out_sem).start()
            continue
        for t in (1, 2):
            filled = slots[me, t - 1] >= 0

            @pl.when(filled)
            def _():
                pltpu.make_async_copy(mid, out(t), out_sem).start()

            @pl.when(jnp.logical_not(filled))
            def _():
                if kind == 0:
                    pltpu.make_async_copy(zero, out(t), out_sem).start()
                else:
                    for h in range(2):
                        pltpu.make_async_copy(zero.at[pl.ds(0, 512)], out(t).at[:, pl.ds(h * 1024, 1024)], out_sem).start()
    for n, (src, mid, out, hot, kind) in enumerate(pairs):
        for t in (1, 2) if hot else (0,):
            pltpu.make_async_copy(mid, out(t), out_sem).wait()


def solution(mesh):
    DMA = pltpu.SemaphoreType.DMA

    def local(gate, up, down, hot_units, slot_map):
        units13 = jax.ShapeDtypeStruct((2, 2048, 1024), BF16)
        unitsd = jax.ShapeDtypeStruct((2, 512, 2048), BF16)
        params = pltpu.CompilerParams(has_side_effects=True, vmem_limit_bytes=48 << 20)
        def move(unit):
            return pl.pallas_call(
                functools.partial(move_kernel, unit),
                out_shape=(units13, unitsd) * 2,
                in_specs=[ANY] * 3,
                out_specs=(ANY,) * 4,
                scratch_shapes=[
                    pltpu.VMEM((2, 2, 2048, 512), BF16),
                    pltpu.VMEM((2, 512, 2048), BF16),
                    pltpu.VMEM((2, 2, 2048, 512), BF16),
                    pltpu.VMEM((2, 512, 2048), BF16),
                    DMA((3,)),
                    DMA((2, 3)),
                    DMA((2, 3, N)),
                    DMA((2, 3, 2)),
                    DMA((2, 3)),
                    DMA((2, 3)),
                    DMA((2, 3)),
                    DMA((2, WINDOW)),
                    DMA((2, 3)),
                ],
                compiler_params=params,
                name=f"move{unit}",
            )

        moved = lax.switch(hot_units[0], [move(u) for u in range(16)], gate, up, down)
        return pl.pallas_call(
            place_kernel,
            out_shape=(
                jax.ShapeDtypeStruct((2, 3, 2048, 1024), BF16),
                jax.ShapeDtypeStruct((2, 3, 512, 2048), BF16),
            ),
            in_specs=[pl.BlockSpec(memory_space=pltpu.SMEM)] + [ANY] * 4,
            out_specs=(ANY, ANY),
            scratch_shapes=[
                [pltpu.VMEM((2, 2048, 1024), BF16)] * 2,
                [pltpu.VMEM((2, 512, 2048), BF16)] * 2,
                pltpu.VMEM((1024, 1024), BF16),
                DMA((12,)),
                DMA,
            ],
            compiler_params=pltpu.CompilerParams(vmem_limit_bytes=48 << 20),
            name="place",
        )(slot_map, *moved)

    spec = P("stage", "expert")
    out = P(None, ("stage", "expert"))
    return jax.shard_map(local, mesh=mesh, in_specs=(spec, spec, spec, P(), P()), out_specs=(out, out), check_vma=False)
```

```python
import functools

import jax
import jax.numpy as jnp
from jax import lax
from jax.experimental import pallas as pl
from jax.experimental.pallas import tpu as pltpu
from jax.sharding import PartitionSpec as P

MESH = pl.DeviceIdType.MESH
ANY = pl.BlockSpec(memory_space=pl.ANY)
BF16 = jnp.bfloat16

PARENT = (
    (None, 0, 3, 1, 5, 1, 7, 5),
    (None, 3, 0, 2, 6, 7, 2, 3),
    (None, 5, 6, 7, 0, 4, 4, 6),
)
DEPTH = (
    (0, 1, 3, 2, 3, 2, 4, 3),
    (0, 3, 1, 2, 3, 4, 2, 3),
    (0, 3, 3, 4, 1, 2, 2, 3),
)
CHILDREN = tuple(tuple(tuple(v for v in range(1, 8) if par[v] == r) for r in range(8)) for par in PARENT)
DEEPEST = max(map(max, DEPTH))
N = 16
LAG = 2


def coords():
    z = lax.axis_index("stage")
    j = lax.axis_index("expert")
    return z, j // 4, (j // 2) % 2, j % 2


def dev(z, y, x, q):
    return (z, y * 4 + x * 2 + q)


def flip(v, bit):
    return 1 - v if bit else v


def table(index, values):
    out = jnp.int32(values[0])
    for i, v in enumerate(values[1:], 1):
        if v != values[0]:
            out = jnp.where(index == i, jnp.int32(v), out)
    return out


def roles(s, rb, rc):
    depth, passes, sends = [], [], []
    for p in range(3):
        def sender(r, v):
            x = (r & 1) ^ rb
            return x if r ^ v == 1 else 1 - x

        def entry(r):
            if r == 0:
                return rc
            children = CHILDREN[p][r]
            return sender(r, children[0]) if children else s

        depth.append([LAG * DEPTH[p][r] + (q != entry(r)) for r in range(8) for q in range(2)])
        passes.append([int(q == entry(r)) for r in range(8) for q in range(2)])
        to = [[v * 2 + entry(v) for v in CHILDREN[p][r] if sender(r, v) == q] for r in range(8) for q in range(2)]
        sends.append([[t[m] if len(t) > m else -1 for t in to] for m in range(max(map(len, to)))])
    return depth, passes, sends


def move_kernel(unit, gate, up, down, home13, homed, hot13, hotd, vg, vd, sg, sd, load_sem, stage_sem, recv_sem, send_sem, side_send, out_sem, home_send, home_recv):
    e, half = unit // 2, unit % 2
    ra, rb, rc = e // 4, (e // 2) % 2, e % 2
    z, y, x, q = coords()

    def source(k, p):
        return down.at[0, 0, pl.ds(k * 512, 512), :] if p == 2 else (gate, up)[p].at[0, 0, :, pl.ds(k * 512, 512)]

    def staged(k, p):
        return sd.at[k] if p == 2 else sg.at[k, p]

    def held(s, p, i=None):
        if p == 2:
            return vd.at[s] if i is None else vd.at[s, pl.ds(i * (512 // N), 512 // N), :]
        return vg.at[s, p] if i is None else vg.at[s, p, pl.ds(i * (2048 // N), 2048 // N), :]

    def place(out13, outd, s, p, i=None):
        if p == 2:
            return outd.at[s] if i is None else outd.at[s, pl.ds(i * (512 // N), 512 // N), :]
        cols = pl.ds(p * 512, 512)
        return out13.at[s, :, cols] if i is None else out13.at[s, pl.ds(i * (2048 // N), 2048 // N), cols]

    final = functools.partial(place, hot13, hotd)
    home = functools.partial(place, home13, homed)

    trees = [roles(s, rb, rc) for s in range(2)]
    rels = [flip(z, s) * 4 + flip(y, ra) * 2 + flip(x, rb) for s in range(2)]
    spots = [rel * 2 + q for rel in rels]
    stay = [(z == y) & (y == x) & (x == q) & (q == k) for k in range(2)]

    def stage(k, p):
        return pltpu.make_async_copy(source(k, p), staged(k, p), stage_sem.at[k, p])

    def load(s, p):
        return pltpu.make_async_copy(source(half, p), held(s, p), load_sem.at[p])

    def home_copy(k, p):
        return pltpu.make_async_remote_copy(
            src_ref=staged(k, p),
            dst_ref=home(z, p),
            send_sem=home_send.at[k, p],
            recv_sem=home_recv.at[z, p],
            device_id=dev(y, x, q, k),
            device_id_type=MESH,
        )

    for s in range(2):

        @pl.when(spots[s] == rc)
        def _():
            for p in range(3):
                load(s, p).start()

    for p in range(3):
        for k in range(2):
            stage(k, p).start()

    for p in range(3):
        for k in range(2):
            stage(k, p).wait()

            @pl.when(stay[k])
            def _():
                pltpu.make_async_copy(staged(k, p), home(z, p), home_recv.at[z, p]).start()

            @pl.when(jnp.logical_not(stay[k]))
            def _():
                home_copy(k, p).start()

    for s in range(2):

        @pl.when(spots[s] == rc)
        def _():
            for p in range(3):
                load(s, p).wait()

    def wave(t, carry):
        for s in range(2):
            spot = spots[s]
            depth, passes, sends = trees[s]
            for p in range(3):
                i = t - table(spot, depth[p])

                @pl.when((i >= 0) & (i < N))
                def _():
                    @pl.when(spot != rc)
                    def _():
                        pltpu.make_async_copy(held(s, p, i), held(s, p, i), recv_sem.at[s, p, i]).wait()

                    def forward(to, sem):
                        return pltpu.make_async_remote_copy(
                            src_ref=held(s, p, i),
                            dst_ref=held(s, p, i),
                            send_sem=sem,
                            recv_sem=recv_sem.at[s, p, i],
                            device_id=to,
                            device_id_type=MESH,
                        )

                    for m, row in enumerate(sends[p]):
                        child = table(spot, row)

                        @pl.when(child >= 0)
                        def _():
                            to = dev(flip(child // 8, s), flip((child // 4) % 2, ra), flip((child // 2) % 2, rb), child % 2)
                            forward(to, send_sem.at[s, p, m]).start()

                    @pl.when(table(spot, passes[p]) == 1)
                    def _():
                        forward(dev(z, y, x, 1 - q), side_send.at[s, p]).start()

                    pltpu.make_async_copy(held(s, p, i), final(s, p, i), out_sem.at[s, p]).start()

        return carry

    lax.fori_loop(0, N + LAG * DEEPEST + 1, wave, 0)

    for s in range(2):
        spot = spots[s]
        _, passes, sends = trees[s]
        for p in range(3):
            for m, row in enumerate(sends[p]):

                @pl.when(table(spot, row) >= 0)
                def _():
                    pltpu.make_async_copy(held(s, p), held(s, p), send_sem.at[s, p, m]).wait()

            @pl.when(table(spot, passes[p]) == 1)
            def _():
                pltpu.make_async_copy(held(s, p), held(s, p), side_send.at[s, p]).wait()

            pltpu.make_async_copy(held(s, p), final(s, p), out_sem.at[s, p]).wait()

    for k in range(2):

        @pl.when(jnp.logical_not(stay[k]))
        def _():
            for p in range(3):
                home_copy(k, p).wait_send()

    for s in range(2):
        for p in range(3):
            pltpu.make_async_copy(home(s, p), home(s, p), home_recv.at[s, p]).wait()


def place_kernel(slots, home13, homed, hot13, hotd, out13, outd, va, vb, zero, in_sem, out_sem):
    me = lax.axis_index("stage") * 8 + lax.axis_index("expert")
    vah, vaH = va
    vbh, vbH = vb
    zero[...] = jnp.zeros_like(zero)
    pairs = []
    for g in range(4):
        layer, r = g // 2, g % 2
        rows = pl.ds(r * 1024, 1024)
        pairs.append((home13.at[layer, rows], vah.at[layer, rows], lambda t, layer=layer, rows=rows: out13.at[layer, t, rows], False, 0))
        pairs.append((hot13.at[layer, rows], vaH.at[layer, rows], lambda t, layer=layer, rows=rows: out13.at[layer, t, rows], True, 0))
    for layer in range(2):
        pairs.append((homed.at[layer], vbh.at[layer], lambda t, layer=layer: outd.at[layer, t], False, 1))
        pairs.append((hotd.at[layer], vbH.at[layer], lambda t, layer=layer: outd.at[layer, t], True, 1))
    for n, (src, mid, out, hot, kind) in enumerate(pairs):
        pltpu.make_async_copy(src, mid, in_sem.at[n]).start()
    for n, (src, mid, out, hot, kind) in enumerate(pairs):
        pltpu.make_async_copy(src, mid, in_sem.at[n]).wait()
        if not hot:
            pltpu.make_async_copy(mid, out(0), out_sem).start()
            continue
        for t in (1, 2):
            filled = slots[me, t - 1] >= 0

            @pl.when(filled)
            def _():
                pltpu.make_async_copy(mid, out(t), out_sem).start()

            @pl.when(jnp.logical_not(filled))
            def _():
                if kind == 0:
                    pltpu.make_async_copy(zero, out(t), out_sem).start()
                else:
                    for h in range(2):
                        pltpu.make_async_copy(zero.at[pl.ds(0, 512)], out(t).at[:, pl.ds(h * 1024, 1024)], out_sem).start()
    for n, (src, mid, out, hot, kind) in enumerate(pairs):
        for t in (1, 2) if hot else (0,):
            pltpu.make_async_copy(mid, out(t), out_sem).wait()


def solution(mesh):
    DMA = pltpu.SemaphoreType.DMA

    def local(gate, up, down, hot_units, slot_map):
        units13 = jax.ShapeDtypeStruct((2, 2048, 1024), BF16)
        unitsd = jax.ShapeDtypeStruct((2, 512, 2048), BF16)
        params = pltpu.CompilerParams(has_side_effects=True, vmem_limit_bytes=48 << 20)
        def move(unit):
            return pl.pallas_call(
                functools.partial(move_kernel, unit),
                out_shape=(units13, unitsd) * 2,
                in_specs=[ANY] * 3,
                out_specs=(ANY,) * 4,
                scratch_shapes=[
                    pltpu.VMEM((2, 2, 2048, 512), BF16),
                    pltpu.VMEM((2, 512, 2048), BF16),
                    pltpu.VMEM((2, 2, 2048, 512), BF16),
                    pltpu.VMEM((2, 512, 2048), BF16),
                    DMA((3,)),
                    DMA((2, 3)),
                    DMA((2, 3, N)),
                    DMA((2, 3, 2)),
                    DMA((2, 3)),
                    DMA((2, 3)),
                    DMA((2, 3)),
                    DMA((2, 3)),
                ],
                compiler_params=params,
                name=f"move{unit}",
            )

        moved = lax.switch(hot_units[0], [move(u) for u in range(16)], gate, up, down)
        return pl.pallas_call(
            place_kernel,
            out_shape=(
                jax.ShapeDtypeStruct((2, 3, 2048, 1024), BF16),
                jax.ShapeDtypeStruct((2, 3, 512, 2048), BF16),
            ),
            in_specs=[pl.BlockSpec(memory_space=pltpu.SMEM)] + [ANY] * 4,
            out_specs=(ANY, ANY),
            scratch_shapes=[
                [pltpu.VMEM((2, 2048, 1024), BF16)] * 2,
                [pltpu.VMEM((2, 512, 2048), BF16)] * 2,
                pltpu.VMEM((1024, 1024), BF16),
                DMA((12,)),
                DMA,
            ],
            compiler_params=pltpu.CompilerParams(vmem_limit_bytes=48 << 20),
            name="place",
        )(slot_map, *moved)

    spec = P("stage", "expert")
    out = P(None, ("stage", "expert"))
    return jax.shard_map(local, mesh=mesh, in_specs=(spec, spec, spec, P(), P()), out_specs=(out, out), check_vma=False)
```

```python
import functools

import jax
import jax.numpy as jnp
from jax import lax
from jax.experimental import pallas as pl
from jax.experimental.pallas import tpu as pltpu
from jax.sharding import PartitionSpec as P

MESH = pl.DeviceIdType.MESH
ANY = pl.BlockSpec(memory_space=pl.ANY)
BF16 = jnp.bfloat16

PARENT = (
    (None, 0, 3, 1, 5, 1, 7, 5),
    (None, 3, 0, 2, 6, 7, 2, 3),
    (None, 5, 6, 7, 0, 4, 4, 6),
)
DEPTH = (
    (0, 1, 3, 2, 3, 2, 4, 3),
    (0, 3, 1, 2, 3, 4, 2, 3),
    (0, 3, 3, 4, 1, 2, 2, 3),
)
CHILDREN = tuple(tuple(tuple(v for v in range(1, 8) if par[v] == r) for r in range(8)) for par in PARENT)
DEEPEST = max(map(max, DEPTH))
N = 32
LAG = 3


def coords():
    z = lax.axis_index("stage")
    j = lax.axis_index("expert")
    return z, j // 4, (j // 2) % 2, j % 2


def dev(z, y, x, q):
    return (z, y * 4 + x * 2 + q)


def flip(v, bit):
    return 1 - v if bit else v


def table(index, values):
    out = jnp.int32(values[0])
    for i, v in enumerate(values[1:], 1):
        if v != values[0]:
            out = jnp.where(index == i, jnp.int32(v), out)
    return out


def roles(s, rb, rc):
    depth, passes, sends = [], [], []
    for p in range(3):
        def sender(r, v):
            x = (r & 1) ^ rb
            return x if r ^ v == 1 else 1 - x

        def entry(r):
            if r == 0:
                return rc
            children = CHILDREN[p][r]
            return sender(r, children[0]) if children else s

        depth.append([LAG * DEPTH[p][r] + (q != entry(r)) for r in range(8) for q in range(2)])
        passes.append([int(q == entry(r)) for r in range(8) for q in range(2)])
        to = [[v * 2 + entry(v) for v in CHILDREN[p][r] if sender(r, v) == q] for r in range(8) for q in range(2)]
        sends.append([[t[m] if len(t) > m else -1 for t in to] for m in range(max(map(len, to)))])
    return depth, passes, sends


def move_kernel(unit, gate, up, down, home13, homed, vg, vd, sg, sd, load_sem, stage_sem, recv_sem, send_sem, side_send, home_send, home_recv):
    e, half = unit // 2, unit % 2
    ra, rb, rc = e // 4, (e // 2) % 2, e % 2
    z, y, x, q = coords()

    def source(k, p):
        return down.at[0, 0, pl.ds(k * 512, 512), :] if p == 2 else (gate, up)[p].at[0, 0, :, pl.ds(k * 512, 512)]

    def staged(k, p):
        return sd.at[k] if p == 2 else sg.at[k, p]

    def held(s, p, i=None):
        if p == 2:
            return vd.at[s] if i is None else vd.at[s, pl.ds(i * (512 // N), 512 // N), :]
        return vg.at[s, p] if i is None else vg.at[s, p, pl.ds(i * (2048 // N), 2048 // N), :]

    def home(s, p):
        return homed.at[s] if p == 2 else home13.at[s, :, pl.ds(p * 512, 512)]

    trees = [roles(s, rb, rc) for s in range(2)]
    rels = [flip(z, s) * 4 + flip(y, ra) * 2 + flip(x, rb) for s in range(2)]
    spots = [rel * 2 + q for rel in rels]
    stay = [(z == y) & (y == x) & (x == q) & (q == k) for k in range(2)]

    def stage(k, p):
        return pltpu.make_async_copy(source(k, p), staged(k, p), stage_sem.at[k, p])

    def load(s, p):
        return pltpu.make_async_copy(source(half, p), held(s, p), load_sem.at[p])

    def home_copy(k, p):
        return pltpu.make_async_remote_copy(
            src_ref=staged(k, p),
            dst_ref=home(z, p),
            send_sem=home_send.at[k, p],
            recv_sem=home_recv.at[z, p],
            device_id=dev(y, x, q, k),
            device_id_type=MESH,
        )

    for s in range(2):

        @pl.when(spots[s] == rc)
        def _():
            for p in range(3):
                load(s, p).start()

    for p in range(3):
        for k in range(2):
            stage(k, p).start()

    for p in range(3):
        for k in range(2):
            stage(k, p).wait()

            @pl.when(stay[k])
            def _():
                pltpu.make_async_copy(staged(k, p), home(z, p), home_recv.at[z, p]).start()

            @pl.when(jnp.logical_not(stay[k]))
            def _():
                home_copy(k, p).start()

    for s in range(2):

        @pl.when(spots[s] == rc)
        def _():
            for p in range(3):
                load(s, p).wait()

    def wave(t, carry):
        for s in range(2):
            spot = spots[s]
            depth, passes, sends = trees[s]
            for p in range(3):
                i = t - table(spot, depth[p])

                @pl.when((i >= 0) & (i < N))
                def _():
                    @pl.when(spot != rc)
                    def _():
                        pltpu.make_async_copy(held(s, p, i), held(s, p, i), recv_sem.at[s, p, i]).wait()

                    def forward(to, sem):
                        return pltpu.make_async_remote_copy(
                            src_ref=held(s, p, i),
                            dst_ref=held(s, p, i),
                            send_sem=sem,
                            recv_sem=recv_sem.at[s, p, i],
                            device_id=to,
                            device_id_type=MESH,
                        )

                    for m, row in enumerate(sends[p]):
                        child = table(spot, row)

                        @pl.when(child >= 0)
                        def _():
                            to = dev(flip(child // 8, s), flip((child // 4) % 2, ra), flip((child // 2) % 2, rb), child % 2)
                            forward(to, send_sem.at[s, p, m]).start()

                    @pl.when(table(spot, passes[p]) == 1)
                    def _():
                        forward(dev(z, y, x, 1 - q), side_send.at[s, p]).start()

        return carry

    lax.fori_loop(0, N + LAG * DEEPEST + 1, wave, 0)

    for s in range(2):
        spot = spots[s]
        _, passes, sends = trees[s]
        for p in range(3):
            for m, row in enumerate(sends[p]):

                @pl.when(table(spot, row) >= 0)
                def _():
                    pltpu.make_async_copy(held(s, p), held(s, p), send_sem.at[s, p, m]).wait()

            @pl.when(table(spot, passes[p]) == 1)
            def _():
                pltpu.make_async_copy(held(s, p), held(s, p), side_send.at[s, p]).wait()

    for k in range(2):

        @pl.when(jnp.logical_not(stay[k]))
        def _():
            for p in range(3):
                home_copy(k, p).wait_send()

    for s in range(2):
        for p in range(3):
            pltpu.make_async_copy(home(s, p), home(s, p), home_recv.at[s, p]).wait()


def place_kernel(slots, home13, homed, hot13, hotd, out13, outd, zero, sem):
    me = lax.axis_index("stage") * 8 + lax.axis_index("expert")
    zero[...] = jnp.zeros_like(zero)

    def pieces(layer, slot):
        return out13.at[layer, slot, :, pl.ds(0, 512)], out13.at[layer, slot, :, pl.ds(512, 512)], outd.at[layer, slot]

    for layer in range(2):
        pltpu.make_async_copy(home13.at[layer], out13.at[layer, 0], sem).start()
        pltpu.make_async_copy(homed.at[layer], outd.at[layer, 0], sem).start()
        for t in range(2):
            filled = slots[me, t] >= 0
            to = pieces(layer, t + 1)

            @pl.when(filled)
            def _():
                for p in range(3):
                    pltpu.make_async_copy(hotd.at[layer] if p == 2 else hot13.at[layer, p], to[p], sem).start()

            @pl.when(jnp.logical_not(filled))
            def _():
                for h in range(4):
                    pltpu.make_async_copy(zero, out13.at[layer, t + 1, pl.ds(h * 512, 512)], sem).start()
                for h in range(2):
                    pltpu.make_async_copy(zero, outd.at[layer, t + 1, :, pl.ds(h * 1024, 1024)], sem).start()

    for layer in range(2):
        for t in range(3):
            pltpu.make_async_copy(home13.at[layer], out13.at[layer, t], sem).wait()
            pltpu.make_async_copy(homed.at[layer], outd.at[layer, t], sem).wait()


def solution(mesh):
    DMA = pltpu.SemaphoreType.DMA

    VMEM = pl.BlockSpec(memory_space=pltpu.VMEM)

    def local(gate, up, down, hot_units, slot_map):
        def branch(unit, gate, up, down, slot_map):
            moved = pl.pallas_call(
                functools.partial(move_kernel, unit),
                out_shape=(
                    pltpu.VMEM((2, 2048, 1024), BF16),
                    pltpu.VMEM((2, 512, 2048), BF16),
                    pltpu.VMEM((2, 2, 2048, 512), BF16),
                    pltpu.VMEM((2, 512, 2048), BF16),
                ),
                in_specs=[ANY] * 3,
                out_specs=(VMEM,) * 4,
                scratch_shapes=[
                    pltpu.VMEM((2, 2, 2048, 512), BF16),
                    pltpu.VMEM((2, 512, 2048), BF16),
                    DMA((3,)),
                    DMA((2, 3)),
                    DMA((2, 3, N)),
                    DMA((2, 3, 2)),
                    DMA((2, 3)),
                    DMA((2, 3)),
                    DMA((2, 3)),
                ],
                compiler_params=pltpu.CompilerParams(has_side_effects=True, vmem_limit_bytes=14 << 20),
                name=f"move{unit}",
            )(gate, up, down)
            return pl.pallas_call(
                place_kernel,
                out_shape=(
                    jax.ShapeDtypeStruct((2, 3, 2048, 1024), BF16),
                    jax.ShapeDtypeStruct((2, 3, 512, 2048), BF16),
                ),
                in_specs=[pl.BlockSpec(memory_space=pltpu.SMEM)] + [VMEM] * 4,
                out_specs=(ANY, ANY),
                scratch_shapes=[pltpu.VMEM((512, 1024), BF16), DMA],
                compiler_params=pltpu.CompilerParams(vmem_limit_bytes=4 << 20),
                name="place",
            )(slot_map, *moved)

        return lax.switch(hot_units[0], [functools.partial(branch, u) for u in range(16)], gate, up, down, slot_map)

    spec = P("stage", "expert")
    out = P(None, ("stage", "expert"))
    return jax.shard_map(local, mesh=mesh, in_specs=(spec, spec, spec, P(), P()), out_specs=(out, out), check_vma=False)
```

```python
import functools

import jax
import jax.numpy as jnp
from jax import lax
from jax.experimental import pallas as pl
from jax.experimental.pallas import tpu as pltpu
from jax.sharding import PartitionSpec as P

MESH = pl.DeviceIdType.MESH
ANY = pl.BlockSpec(memory_space=pl.ANY)
BF16 = jnp.bfloat16

PARENT = (
    (None, 0, 3, 1, 5, 1, 7, 5),
    (None, 3, 0, 2, 6, 7, 2, 3),
    (None, 5, 6, 7, 0, 4, 4, 6),
)
DEPTH = (
    (0, 1, 3, 2, 3, 2, 4, 3),
    (0, 3, 1, 2, 3, 4, 2, 3),
    (0, 3, 3, 4, 1, 2, 2, 3),
)
CHILDREN = tuple(tuple(tuple(v for v in range(1, 8) if par[v] == r) for r in range(8)) for par in PARENT)
DEEPEST = max(map(max, DEPTH))
N = 64
LAG = 3


def coords():
    z = lax.axis_index("stage")
    j = lax.axis_index("expert")
    return z, j // 4, (j // 2) % 2, j % 2


def dev(z, y, x, q):
    return (z, y * 4 + x * 2 + q)


def flip(v, bit):
    return 1 - v if bit else v


def table(index, values):
    out = jnp.int32(values[0])
    for i, v in enumerate(values[1:], 1):
        if v != values[0]:
            out = jnp.where(index == i, jnp.int32(v), out)
    return out


def roles(s, rb, rc):
    depth, passes, sends = [], [], []
    for p in range(3):
        def sender(r, v):
            x = (r & 1) ^ rb
            return x if r ^ v == 1 else 1 - x

        def entry(r):
            if r == 0:
                return rc
            children = CHILDREN[p][r]
            return sender(r, children[0]) if children else s

        depth.append([LAG * DEPTH[p][r] + (q != entry(r)) for r in range(8) for q in range(2)])
        passes.append([int(q == entry(r)) for r in range(8) for q in range(2)])
        to = [[v * 2 + entry(v) for v in CHILDREN[p][r] if sender(r, v) == q] for r in range(8) for q in range(2)]
        sends.append([[t[m] if len(t) > m else -1 for t in to] for m in range(max(map(len, to)))])
    return depth, passes, sends


def move_kernel(unit, gate, up, down, home13, homed, vg, vd, sg, sd, load_sem, stage_sem, recv_sem, send_sem, side_send, home_send, home_recv):
    e, half = unit // 2, unit % 2
    ra, rb, rc = e // 4, (e // 2) % 2, e % 2
    z, y, x, q = coords()

    def source(k, p):
        return down.at[0, 0, pl.ds(k * 512, 512), :] if p == 2 else (gate, up)[p].at[0, 0, :, pl.ds(k * 512, 512)]

    def staged(k, p):
        return sd.at[k] if p == 2 else sg.at[k, p]

    def held(s, p, i=None):
        if p == 2:
            return vd.at[s] if i is None else vd.at[s, pl.ds(i * (512 // N), 512 // N), :]
        return vg.at[s, p] if i is None else vg.at[s, p, pl.ds(i * (2048 // N), 2048 // N), :]

    def home(s, p):
        return homed.at[s] if p == 2 else home13.at[s, :, pl.ds(p * 512, 512)]

    trees = [roles(s, rb, rc) for s in range(2)]
    rels = [flip(z, s) * 4 + flip(y, ra) * 2 + flip(x, rb) for s in range(2)]
    spots = [rel * 2 + q for rel in rels]
    stay = [(z == y) & (y == x) & (x == q) & (q == k) for k in range(2)]

    def stage(k, p):
        return pltpu.make_async_copy(source(k, p), staged(k, p), stage_sem.at[k, p])

    def load(s, p):
        return pltpu.make_async_copy(source(half, p), held(s, p), load_sem.at[p])

    def home_copy(k, p):
        return pltpu.make_async_remote_copy(
            src_ref=staged(k, p),
            dst_ref=home(z, p),
            send_sem=home_send.at[k, p],
            recv_sem=home_recv.at[z, p],
            device_id=dev(y, x, q, k),
            device_id_type=MESH,
        )

    for s in range(2):

        @pl.when(spots[s] == rc)
        def _():
            for p in range(3):
                load(s, p).start()

    for p in range(3):
        for k in range(2):
            stage(k, p).start()

    for p in range(3):
        for k in range(2):
            stage(k, p).wait()

            @pl.when(stay[k])
            def _():
                pltpu.make_async_copy(staged(k, p), home(z, p), home_recv.at[z, p]).start()

            @pl.when(jnp.logical_not(stay[k]))
            def _():
                home_copy(k, p).start()

    for s in range(2):

        @pl.when(spots[s] == rc)
        def _():
            for p in range(3):
                load(s, p).wait()

    def wave(t, carry):
        for s in range(2):
            spot = spots[s]
            depth, passes, sends = trees[s]
            for p in range(3):
                i = t - table(spot, depth[p])

                @pl.when((i >= 0) & (i < N))
                def _():
                    @pl.when(spot != rc)
                    def _():
                        pltpu.make_async_copy(held(s, p, i), held(s, p, i), recv_sem.at[s, p, i]).wait()

                    def forward(to, sem):
                        return pltpu.make_async_remote_copy(
                            src_ref=held(s, p, i),
                            dst_ref=held(s, p, i),
                            send_sem=sem,
                            recv_sem=recv_sem.at[s, p, i],
                            device_id=to,
                            device_id_type=MESH,
                        )

                    for m, row in enumerate(sends[p]):
                        child = table(spot, row)

                        @pl.when(child >= 0)
                        def _():
                            to = dev(flip(child // 8, s), flip((child // 4) % 2, ra), flip((child // 2) % 2, rb), child % 2)
                            forward(to, send_sem.at[s, p, m]).start()

                    @pl.when(table(spot, passes[p]) == 1)
                    def _():
                        forward(dev(z, y, x, 1 - q), side_send.at[s, p]).start()

        return carry

    lax.fori_loop(0, N + LAG * DEEPEST + 1, wave, 0)

    for s in range(2):
        spot = spots[s]
        _, passes, sends = trees[s]
        for p in range(3):
            for m, row in enumerate(sends[p]):

                @pl.when(table(spot, row) >= 0)
                def _():
                    pltpu.make_async_copy(held(s, p), held(s, p), send_sem.at[s, p, m]).wait()

            @pl.when(table(spot, passes[p]) == 1)
            def _():
                pltpu.make_async_copy(held(s, p), held(s, p), side_send.at[s, p]).wait()

    for k in range(2):

        @pl.when(jnp.logical_not(stay[k]))
        def _():
            for p in range(3):
                home_copy(k, p).wait_send()

    for s in range(2):
        for p in range(3):
            pltpu.make_async_copy(home(s, p), home(s, p), home_recv.at[s, p]).wait()


def place_kernel(slots, home13, homed, hot13, hotd, out13, outd, zero, sem):
    me = lax.axis_index("stage") * 8 + lax.axis_index("expert")
    zero[...] = jnp.zeros_like(zero)

    def pieces(layer, slot):
        return out13.at[layer, slot, :, pl.ds(0, 512)], out13.at[layer, slot, :, pl.ds(512, 512)], outd.at[layer, slot]

    for layer in range(2):
        pltpu.make_async_copy(home13.at[layer], out13.at[layer, 0], sem).start()
        pltpu.make_async_copy(homed.at[layer], outd.at[layer, 0], sem).start()
        for t in range(2):
            filled = slots[me, t] >= 0
            to = pieces(layer, t + 1)

            @pl.when(filled)
            def _():
                for p in range(3):
                    pltpu.make_async_copy(hotd.at[layer] if p == 2 else hot13.at[layer, p], to[p], sem).start()

            @pl.when(jnp.logical_not(filled))
            def _():
                for h in range(4):
                    pltpu.make_async_copy(zero, out13.at[layer, t + 1, pl.ds(h * 512, 512)], sem).start()
                for h in range(2):
                    pltpu.make_async_copy(zero, outd.at[layer, t + 1, :, pl.ds(h * 1024, 1024)], sem).start()

    for layer in range(2):
        for t in range(3):
            pltpu.make_async_copy(home13.at[layer], out13.at[layer, t], sem).wait()
            pltpu.make_async_copy(homed.at[layer], outd.at[layer, t], sem).wait()


def solution(mesh):
    DMA = pltpu.SemaphoreType.DMA

    VMEM = pl.BlockSpec(memory_space=pltpu.VMEM)

    def local(gate, up, down, hot_units, slot_map):
        def branch(unit, gate, up, down, slot_map):
            moved = pl.pallas_call(
                functools.partial(move_kernel, unit),
                out_shape=(
                    pltpu.VMEM((2, 2048, 1024), BF16),
                    pltpu.VMEM((2, 512, 2048), BF16),
                    pltpu.VMEM((2, 2, 2048, 512), BF16),
                    pltpu.VMEM((2, 512, 2048), BF16),
                ),
                in_specs=[ANY] * 3,
                out_specs=(VMEM,) * 4,
                scratch_shapes=[
                    pltpu.VMEM((2, 2, 2048, 512), BF16),
                    pltpu.VMEM((2, 512, 2048), BF16),
                    DMA((3,)),
                    DMA((2, 3)),
                    DMA((2, 3, N)),
                    DMA((2, 3, 2)),
                    DMA((2, 3)),
                    DMA((2, 3)),
                    DMA((2, 3)),
                ],
                compiler_params=pltpu.CompilerParams(has_side_effects=True, vmem_limit_bytes=14 << 20),
                name=f"move{unit}",
            )(gate, up, down)
            return pl.pallas_call(
                place_kernel,
                out_shape=(
                    jax.ShapeDtypeStruct((2, 3, 2048, 1024), BF16),
                    jax.ShapeDtypeStruct((2, 3, 512, 2048), BF16),
                ),
                in_specs=[pl.BlockSpec(memory_space=pltpu.SMEM)] + [VMEM] * 4,
                out_specs=(ANY, ANY),
                scratch_shapes=[pltpu.VMEM((512, 1024), BF16), DMA],
                compiler_params=pltpu.CompilerParams(vmem_limit_bytes=4 << 20),
                name="place",
            )(slot_map, *moved)

        return lax.switch(hot_units[0], [functools.partial(branch, u) for u in range(16)], gate, up, down, slot_map)

    spec = P("stage", "expert")
    out = P(None, ("stage", "expert"))
    return jax.shard_map(local, mesh=mesh, in_specs=(spec, spec, spec, P(), P()), out_specs=(out, out), check_vma=False)
```

```python
import functools

import jax
import jax.numpy as jnp
from jax import lax
from jax.experimental import pallas as pl
from jax.experimental.pallas import tpu as pltpu
from jax.sharding import PartitionSpec as P

MESH = pl.DeviceIdType.MESH
ANY = pl.BlockSpec(memory_space=pl.ANY)
BF16 = jnp.bfloat16

PARENT = (
    (None, 0, 3, 1, 5, 1, 7, 5),
    (None, 3, 0, 2, 6, 7, 2, 3),
    (None, 5, 6, 7, 0, 4, 4, 6),
)
DEPTH = (
    (0, 1, 3, 2, 3, 2, 4, 3),
    (0, 3, 1, 2, 3, 4, 2, 3),
    (0, 3, 3, 4, 1, 2, 2, 3),
)
CHILDREN = tuple(tuple(tuple(v for v in range(1, 8) if par[v] == r) for r in range(8)) for par in PARENT)
DEEPEST = max(map(max, DEPTH))
N = 64
HOME_AT = 64
LAG = 6


def coords():
    z = lax.axis_index("stage")
    j = lax.axis_index("expert")
    return z, j // 4, (j // 2) % 2, j % 2


def dev(z, y, x, q):
    return (z, y * 4 + x * 2 + q)


def flip(v, bit):
    return 1 - v if bit else v


def table(index, values):
    out = jnp.int32(values[0])
    for i, v in enumerate(values[1:], 1):
        if v != values[0]:
            out = jnp.where(index == i, jnp.int32(v), out)
    return out


def roles(s, rb, rc):
    depth, passes, sends = [], [], []
    for p in range(3):
        def sender(r, v):
            x = (r & 1) ^ rb
            return x if r ^ v == 1 else 1 - x

        def entry(r):
            if r == 0:
                return rc
            children = CHILDREN[p][r]
            return sender(r, children[0]) if children else s

        depth.append([LAG * DEPTH[p][r] + (q != entry(r)) for r in range(8) for q in range(2)])
        passes.append([int(q == entry(r)) for r in range(8) for q in range(2)])
        to = [[v * 2 + entry(v) for v in CHILDREN[p][r] if sender(r, v) == q] for r in range(8) for q in range(2)]
        sends.append([[t[m] if len(t) > m else -1 for t in to] for m in range(max(map(len, to)))])
    return depth, passes, sends


def move_kernel(unit, gate, up, down, home13, homed, vg, vd, sg, sd, load_sem, stage_sem, recv_sem, send_sem, side_send, home_send, home_recv):
    e, half = unit // 2, unit % 2
    ra, rb, rc = e // 4, (e // 2) % 2, e % 2
    z, y, x, q = coords()

    def source(k, p):
        return down.at[0, 0, pl.ds(k * 512, 512), :] if p == 2 else (gate, up)[p].at[0, 0, :, pl.ds(k * 512, 512)]

    def staged(k, p):
        return sd.at[k] if p == 2 else sg.at[k, p]

    def held(s, p, i=None):
        if p == 2:
            return vd.at[s] if i is None else vd.at[s, pl.ds(i * (512 // N), 512 // N), :]
        return vg.at[s, p] if i is None else vg.at[s, p, pl.ds(i * (2048 // N), 2048 // N), :]

    def home(s, p):
        return homed.at[s] if p == 2 else home13.at[s, :, pl.ds(p * 512, 512)]

    trees = [roles(s, rb, rc) for s in range(2)]
    rels = [flip(z, s) * 4 + flip(y, ra) * 2 + flip(x, rb) for s in range(2)]
    spots = [rel * 2 + q for rel in rels]
    stay = [(z == y) & (y == x) & (x == q) & (q == k) for k in range(2)]

    def stage(k, p):
        return pltpu.make_async_copy(source(k, p), staged(k, p), stage_sem.at[k, p])

    def load(s, p):
        return pltpu.make_async_copy(source(half, p), held(s, p), load_sem.at[p])

    def home_copy(k, p):
        return pltpu.make_async_remote_copy(
            src_ref=staged(k, p),
            dst_ref=home(z, p),
            send_sem=home_send.at[k, p],
            recv_sem=home_recv.at[z, p],
            device_id=dev(y, x, q, k),
            device_id_type=MESH,
        )

    for s in range(2):

        @pl.when(spots[s] == rc)
        def _():
            for p in range(3):
                load(s, p).start()

    for p in range(3):
        for k in range(2):
            stage(k, p).start()

    for s in range(2):

        @pl.when(spots[s] == rc)
        def _():
            for p in range(3):
                load(s, p).wait()

    def start_home():
        for p in range(3):
            for k in range(2):
                stage(k, p).wait()

                @pl.when(stay[k])
                def _():
                    pltpu.make_async_copy(staged(k, p), home(z, p), home_recv.at[z, p]).start()

                @pl.when(jnp.logical_not(stay[k]))
                def _():
                    home_copy(k, p).start()

    def wave(t, carry):
        @pl.when(t == HOME_AT)
        def _():
            start_home()

        for s in range(2):
            spot = spots[s]
            depth, passes, sends = trees[s]
            for p in range(3):
                i = t - table(spot, depth[p])

                @pl.when((i >= 0) & (i < N))
                def _():
                    @pl.when(spot != rc)
                    def _():
                        pltpu.make_async_copy(held(s, p, i), held(s, p, i), recv_sem.at[s, p, i]).wait()

                    def forward(to, sem):
                        return pltpu.make_async_remote_copy(
                            src_ref=held(s, p, i),
                            dst_ref=held(s, p, i),
                            send_sem=sem,
                            recv_sem=recv_sem.at[s, p, i],
                            device_id=to,
                            device_id_type=MESH,
                        )

                    for m, row in enumerate(sends[p]):
                        child = table(spot, row)

                        @pl.when(child >= 0)
                        def _():
                            to = dev(flip(child // 8, s), flip((child // 4) % 2, ra), flip((child // 2) % 2, rb), child % 2)
                            forward(to, send_sem.at[s, p, m]).start()

                    @pl.when(table(spot, passes[p]) == 1)
                    def _():
                        forward(dev(z, y, x, 1 - q), side_send.at[s, p]).start()

        return carry

    lax.fori_loop(0, N + LAG * DEEPEST + 1, wave, 0)

    for s in range(2):
        spot = spots[s]
        _, passes, sends = trees[s]
        for p in range(3):
            for m, row in enumerate(sends[p]):

                @pl.when(table(spot, row) >= 0)
                def _():
                    pltpu.make_async_copy(held(s, p), held(s, p), send_sem.at[s, p, m]).wait()

            @pl.when(table(spot, passes[p]) == 1)
            def _():
                pltpu.make_async_copy(held(s, p), held(s, p), side_send.at[s, p]).wait()

    for k in range(2):

        @pl.when(jnp.logical_not(stay[k]))
        def _():
            for p in range(3):
                home_copy(k, p).wait_send()

    for s in range(2):
        for p in range(3):
            pltpu.make_async_copy(home(s, p), home(s, p), home_recv.at[s, p]).wait()


def place_kernel(slots, home13, homed, hot13, hotd, out13, outd, zero, sem):
    me = lax.axis_index("stage") * 8 + lax.axis_index("expert")
    zero[...] = jnp.zeros_like(zero)

    def pieces(layer, slot):
        return out13.at[layer, slot, :, pl.ds(0, 512)], out13.at[layer, slot, :, pl.ds(512, 512)], outd.at[layer, slot]

    for layer in range(2):
        pltpu.make_async_copy(home13.at[layer], out13.at[layer, 0], sem).start()
        pltpu.make_async_copy(homed.at[layer], outd.at[layer, 0], sem).start()
        for t in range(2):
            filled = slots[me, t] >= 0
            to = pieces(layer, t + 1)

            @pl.when(filled)
            def _():
                for p in range(3):
                    pltpu.make_async_copy(hotd.at[layer] if p == 2 else hot13.at[layer, p], to[p], sem).start()

            @pl.when(jnp.logical_not(filled))
            def _():
                for h in range(4):
                    pltpu.make_async_copy(zero, out13.at[layer, t + 1, pl.ds(h * 512, 512)], sem).start()
                for h in range(2):
                    pltpu.make_async_copy(zero, outd.at[layer, t + 1, :, pl.ds(h * 1024, 1024)], sem).start()

    for layer in range(2):
        for t in range(3):
            pltpu.make_async_copy(home13.at[layer], out13.at[layer, t], sem).wait()
            pltpu.make_async_copy(homed.at[layer], outd.at[layer, t], sem).wait()


def solution(mesh):
    DMA = pltpu.SemaphoreType.DMA

    VMEM = pl.BlockSpec(memory_space=pltpu.VMEM)

    def local(gate, up, down, hot_units, slot_map):
        def branch(unit, gate, up, down, slot_map):
            moved = pl.pallas_call(
                functools.partial(move_kernel, unit),
                out_shape=(
                    pltpu.VMEM((2, 2048, 1024), BF16),
                    pltpu.VMEM((2, 512, 2048), BF16),
                    pltpu.VMEM((2, 2, 2048, 512), BF16),
                    pltpu.VMEM((2, 512, 2048), BF16),
                ),
                in_specs=[ANY] * 3,
                out_specs=(VMEM,) * 4,
                scratch_shapes=[
                    pltpu.VMEM((2, 2, 2048, 512), BF16),
                    pltpu.VMEM((2, 512, 2048), BF16),
                    DMA((3,)),
                    DMA((2, 3)),
                    DMA((2, 3, N)),
                    DMA((2, 3, 2)),
                    DMA((2, 3)),
                    DMA((2, 3)),
                    DMA((2, 3)),
                ],
                compiler_params=pltpu.CompilerParams(has_side_effects=True, vmem_limit_bytes=14 << 20),
                name=f"move{unit}",
            )(gate, up, down)
            return pl.pallas_call(
                place_kernel,
                out_shape=(
                    jax.ShapeDtypeStruct((2, 3, 2048, 1024), BF16),
                    jax.ShapeDtypeStruct((2, 3, 512, 2048), BF16),
                ),
                in_specs=[pl.BlockSpec(memory_space=pltpu.SMEM)] + [VMEM] * 4,
                out_specs=(ANY, ANY),
                scratch_shapes=[pltpu.VMEM((512, 1024), BF16), DMA],
                compiler_params=pltpu.CompilerParams(vmem_limit_bytes=4 << 20),
                name="place",
            )(slot_map, *moved)

        return lax.switch(hot_units[0], [functools.partial(branch, u) for u in range(16)], gate, up, down, slot_map)

    spec = P("stage", "expert")
    out = P(None, ("stage", "expert"))
    return jax.shard_map(local, mesh=mesh, in_specs=(spec, spec, spec, P(), P()), out_specs=(out, out), check_vma=False)
```

```python
import functools

import jax
import jax.numpy as jnp
from jax import lax
from jax.experimental import pallas as pl
from jax.experimental.pallas import tpu as pltpu
from jax.sharding import PartitionSpec as P

MESH = pl.DeviceIdType.MESH
ANY = pl.BlockSpec(memory_space=pl.ANY)
BF16 = jnp.bfloat16

PARENT = (
    (None, 0, 3, 1, 5, 1, 7, 5),
    (None, 3, 0, 2, 6, 7, 2, 3),
    (None, 5, 6, 7, 0, 4, 4, 6),
)
DEPTH = (
    (0, 1, 3, 2, 3, 2, 4, 3),
    (0, 3, 1, 2, 3, 4, 2, 3),
    (0, 3, 3, 4, 1, 2, 2, 3),
)
CHILDREN = tuple(tuple(tuple(v for v in range(1, 8) if par[v] == r) for r in range(8)) for par in PARENT)
DEEPEST = max(map(max, DEPTH))
N = 32
HOME_AT = 10
LAG = 3


def coords():
    z = lax.axis_index("stage")
    j = lax.axis_index("expert")
    return z, j // 4, (j // 2) % 2, j % 2


def dev(z, y, x, q):
    return (z, y * 4 + x * 2 + q)


def flip(v, bit):
    return 1 - v if bit else v


def table(index, values):
    out = jnp.int32(values[0])
    for i, v in enumerate(values[1:], 1):
        if v != values[0]:
            out = jnp.where(index == i, jnp.int32(v), out)
    return out


def roles(s, rb, rc):
    depth, passes, sends = [], [], []
    for p in range(3):
        def sender(r, v):
            x = (r & 1) ^ rb
            return x if r ^ v == 1 else 1 - x

        def entry(r):
            if r == 0:
                return rc
            children = CHILDREN[p][r]
            return sender(r, children[0]) if children else s

        depth.append([LAG * DEPTH[p][r] + (q != entry(r)) for r in range(8) for q in range(2)])
        passes.append([int(q == entry(r)) for r in range(8) for q in range(2)])
        to = [[v * 2 + entry(v) for v in CHILDREN[p][r] if sender(r, v) == q] for r in range(8) for q in range(2)]
        sends.append([[t[m] if len(t) > m else -1 for t in to] for m in range(max(map(len, to)))])
    return depth, passes, sends


def move_kernel(unit, gate, up, down, home13, homed, vg, vd, sg, sd, load_sem, stage_sem, recv_sem, send_sem, side_send, home_send, home_recv):
    e, half = unit // 2, unit % 2
    ra, rb, rc = e // 4, (e // 2) % 2, e % 2
    z, y, x, q = coords()

    def source(k, p):
        return down.at[0, 0, pl.ds(k * 512, 512), :] if p == 2 else (gate, up)[p].at[0, 0, :, pl.ds(k * 512, 512)]

    def staged(k, p):
        return sd.at[k] if p == 2 else sg.at[k, p]

    def held(s, p, i=None):
        if p == 2:
            return vd.at[s] if i is None else vd.at[s, pl.ds(i * (512 // N), 512 // N), :]
        return vg.at[s, p] if i is None else vg.at[s, p, pl.ds(i * (2048 // N), 2048 // N), :]

    def home(s, p):
        return homed.at[s] if p == 2 else home13.at[s, :, pl.ds(p * 512, 512)]

    trees = [roles(s, rb, rc) for s in range(2)]
    rels = [flip(z, s) * 4 + flip(y, ra) * 2 + flip(x, rb) for s in range(2)]
    spots = [rel * 2 + q for rel in rels]
    stay = [(z == y) & (y == x) & (x == q) & (q == k) for k in range(2)]

    def stage(k, p):
        return pltpu.make_async_copy(source(k, p), staged(k, p), stage_sem.at[k, p])

    def load(s, p):
        return pltpu.make_async_copy(source(half, p), held(s, p), load_sem.at[p])

    def home_copy(k, p):
        return pltpu.make_async_remote_copy(
            src_ref=staged(k, p),
            dst_ref=home(z, p),
            send_sem=home_send.at[k, p],
            recv_sem=home_recv.at[z, p],
            device_id=dev(y, x, q, k),
            device_id_type=MESH,
        )

    for s in range(2):

        @pl.when(spots[s] == rc)
        def _():
            for p in range(3):
                load(s, p).start()

    for p in range(3):
        for k in range(2):
            stage(k, p).start()

    for s in range(2):

        @pl.when(spots[s] == rc)
        def _():
            for p in range(3):
                load(s, p).wait()

    def start_home():
        for p in range(3):
            for k in range(2):
                stage(k, p).wait()

                @pl.when(stay[k])
                def _():
                    pltpu.make_async_copy(staged(k, p), home(z, p), home_recv.at[z, p]).start()

                @pl.when(jnp.logical_not(stay[k]))
                def _():
                    home_copy(k, p).start()

    def wave(t, carry):
        @pl.when(t == HOME_AT)
        def _():
            start_home()

        for s in range(2):
            spot = spots[s]
            depth, passes, sends = trees[s]
            for p in range(3):
                i = t - table(spot, depth[p])

                @pl.when((i >= 0) & (i < N))
                def _():
                    @pl.when(spot != rc)
                    def _():
                        pltpu.make_async_copy(held(s, p, i), held(s, p, i), recv_sem.at[s, p, i]).wait()

                    def forward(to, sem):
                        return pltpu.make_async_remote_copy(
                            src_ref=held(s, p, i),
                            dst_ref=held(s, p, i),
                            send_sem=sem,
                            recv_sem=recv_sem.at[s, p, i],
                            device_id=to,
                            device_id_type=MESH,
                        )

                    for m, row in enumerate(sends[p]):
                        child = table(spot, row)

                        @pl.when(child >= 0)
                        def _():
                            to = dev(flip(child // 8, s), flip((child // 4) % 2, ra), flip((child // 2) % 2, rb), child % 2)
                            forward(to, send_sem.at[s, p, m]).start()

                    @pl.when(table(spot, passes[p]) == 1)
                    def _():
                        forward(dev(z, y, x, 1 - q), side_send.at[s, p]).start()

        return carry

    lax.fori_loop(0, N + LAG * DEEPEST + 1, wave, 0)

    for s in range(2):
        spot = spots[s]
        _, passes, sends = trees[s]
        for p in range(3):
            for m, row in enumerate(sends[p]):

                @pl.when(table(spot, row) >= 0)
                def _():
                    pltpu.make_async_copy(held(s, p), held(s, p), send_sem.at[s, p, m]).wait()

            @pl.when(table(spot, passes[p]) == 1)
            def _():
                pltpu.make_async_copy(held(s, p), held(s, p), side_send.at[s, p]).wait()

    for k in range(2):

        @pl.when(jnp.logical_not(stay[k]))
        def _():
            for p in range(3):
                home_copy(k, p).wait_send()

    for s in range(2):
        for p in range(3):
            pltpu.make_async_copy(home(s, p), home(s, p), home_recv.at[s, p]).wait()


def place_kernel(slots, home13, homed, hot13, hotd, out13, outd, zero, sem):
    me = lax.axis_index("stage") * 8 + lax.axis_index("expert")
    zero[...] = jnp.zeros_like(zero)

    def pieces(layer, slot):
        return out13.at[layer, slot, :, pl.ds(0, 512)], out13.at[layer, slot, :, pl.ds(512, 512)], outd.at[layer, slot]

    for layer in range(2):
        pltpu.make_async_copy(home13.at[layer], out13.at[layer, 0], sem).start()
        pltpu.make_async_copy(homed.at[layer], outd.at[layer, 0], sem).start()
        for t in range(2):
            filled = slots[me, t] >= 0
            to = pieces(layer, t + 1)

            @pl.when(filled)
            def _():
                for p in range(3):
                    pltpu.make_async_copy(hotd.at[layer] if p == 2 else hot13.at[layer, p], to[p], sem).start()

            @pl.when(jnp.logical_not(filled))
            def _():
                for h in range(4):
                    pltpu.make_async_copy(zero, out13.at[layer, t + 1, pl.ds(h * 512, 512)], sem).start()
                for h in range(2):
                    pltpu.make_async_copy(zero, outd.at[layer, t + 1, :, pl.ds(h * 1024, 1024)], sem).start()

    for layer in range(2):
        for t in range(3):
            pltpu.make_async_copy(home13.at[layer], out13.at[layer, t], sem).wait()
            pltpu.make_async_copy(homed.at[layer], outd.at[layer, t], sem).wait()


def solution(mesh):
    DMA = pltpu.SemaphoreType.DMA

    VMEM = pl.BlockSpec(memory_space=pltpu.VMEM)

    def local(gate, up, down, hot_units, slot_map):
        def branch(unit, gate, up, down, slot_map):
            moved = pl.pallas_call(
                functools.partial(move_kernel, unit),
                out_shape=(
                    pltpu.VMEM((2, 2048, 1024), BF16),
                    pltpu.VMEM((2, 512, 2048), BF16),
                    pltpu.VMEM((2, 2, 2048, 512), BF16),
                    pltpu.VMEM((2, 512, 2048), BF16),
                ),
                in_specs=[ANY] * 3,
                out_specs=(VMEM,) * 4,
                scratch_shapes=[
                    pltpu.VMEM((2, 2, 2048, 512), BF16),
                    pltpu.VMEM((2, 512, 2048), BF16),
                    DMA((3,)),
                    DMA((2, 3)),
                    DMA((2, 3, N)),
                    DMA((2, 3, 2)),
                    DMA((2, 3)),
                    DMA((2, 3)),
                    DMA((2, 3)),
                ],
                compiler_params=pltpu.CompilerParams(has_side_effects=True, vmem_limit_bytes=14 << 20),
                name=f"move{unit}",
            )(gate, up, down)
            return pl.pallas_call(
                place_kernel,
                out_shape=(
                    jax.ShapeDtypeStruct((2, 3, 2048, 1024), BF16),
                    jax.ShapeDtypeStruct((2, 3, 512, 2048), BF16),
                ),
                in_specs=[pl.BlockSpec(memory_space=pltpu.SMEM)] + [VMEM] * 4,
                out_specs=(ANY, ANY),
                scratch_shapes=[pltpu.VMEM((512, 1024), BF16), DMA],
                compiler_params=pltpu.CompilerParams(vmem_limit_bytes=4 << 20),
                name="place",
            )(slot_map, *moved)

        return lax.switch(hot_units[0], [functools.partial(branch, u) for u in range(16)], gate, up, down, slot_map)

    spec = P("stage", "expert")
    out = P(None, ("stage", "expert"))
    return jax.shard_map(local, mesh=mesh, in_specs=(spec, spec, spec, P(), P()), out_specs=(out, out), check_vma=False)
```

```python
import functools

import jax
import jax.numpy as jnp
from jax import lax
from jax.experimental import pallas as pl
from jax.experimental.pallas import tpu as pltpu
from jax.sharding import PartitionSpec as P

MESH = pl.DeviceIdType.MESH
ANY = pl.BlockSpec(memory_space=pl.ANY)
BF16 = jnp.bfloat16

PARENT = (
    (None, 0, 3, 1, 5, 1, 7, 5),
    (None, 3, 0, 2, 6, 7, 2, 3),
    (None, 5, 6, 7, 0, 4, 4, 6),
)
DEPTH = (
    (0, 1, 3, 2, 3, 2, 4, 3),
    (0, 3, 1, 2, 3, 4, 2, 3),
    (0, 3, 3, 4, 1, 2, 2, 3),
)
CHILDREN = tuple(tuple(tuple(v for v in range(1, 8) if par[v] == r) for r in range(8)) for par in PARENT)
DEEPEST = max(map(max, DEPTH))
N = 16
HOME_AT = 0
LAG = 2


def coords():
    z = lax.axis_index("stage")
    j = lax.axis_index("expert")
    return z, j // 4, (j // 2) % 2, j % 2


def dev(z, y, x, q):
    return (z, y * 4 + x * 2 + q)


def flip(v, bit):
    return 1 - v if bit else v


def table(index, values):
    out = jnp.int32(values[0])
    for i, v in enumerate(values[1:], 1):
        if v != values[0]:
            out = jnp.where(index == i, jnp.int32(v), out)
    return out


def roles(s, rb, rc):
    depth, passes, sends = [], [], []
    for p in range(3):
        def sender(r, v):
            x = (r & 1) ^ rb
            return x if r ^ v == 1 else 1 - x

        def entry(r):
            if r == 0:
                return rc
            children = CHILDREN[p][r]
            return sender(r, children[0]) if children else s

        depth.append([LAG * DEPTH[p][r] + (q != entry(r)) for r in range(8) for q in range(2)])
        passes.append([int(q == entry(r)) for r in range(8) for q in range(2)])
        to = [[v * 2 + entry(v) for v in CHILDREN[p][r] if sender(r, v) == q] for r in range(8) for q in range(2)]
        sends.append([[t[m] if len(t) > m else -1 for t in to] for m in range(max(map(len, to)))])
    return depth, passes, sends


def move_kernel(unit, gate, up, down, home13, homed, vg, vd, sg, sd, load_sem, stage_sem, recv_sem, send_sem, side_send, home_send, home_recv):
    e, half = unit // 2, unit % 2
    ra, rb, rc = e // 4, (e // 2) % 2, e % 2
    z, y, x, q = coords()

    def source(k, p):
        return down.at[0, 0, pl.ds(k * 512, 512), :] if p == 2 else (gate, up)[p].at[0, 0, :, pl.ds(k * 512, 512)]

    def staged(k, p):
        return sd.at[k] if p == 2 else sg.at[k, p]

    def held(s, p, i=None):
        if p == 2:
            return vd.at[s] if i is None else vd.at[s, pl.ds(i * (512 // N), 512 // N), :]
        return vg.at[s, p] if i is None else vg.at[s, p, pl.ds(i * (2048 // N), 2048 // N), :]

    def home(s, p):
        return homed.at[s] if p == 2 else home13.at[s, :, pl.ds(p * 512, 512)]

    trees = [roles(s, rb, rc) for s in range(2)]
    rels = [flip(z, s) * 4 + flip(y, ra) * 2 + flip(x, rb) for s in range(2)]
    spots = [rel * 2 + q for rel in rels]
    stay = [(z == y) & (y == x) & (x == q) & (q == k) for k in range(2)]

    def stage(k, p):
        return pltpu.make_async_copy(source(k, p), staged(k, p), stage_sem.at[k, p])

    def load(s, p):
        return pltpu.make_async_copy(source(half, p), held(s, p), load_sem.at[p])

    def home_copy(k, p):
        return pltpu.make_async_remote_copy(
            src_ref=staged(k, p),
            dst_ref=home(z, p),
            send_sem=home_send.at[k, p],
            recv_sem=home_recv.at[z, p],
            device_id=dev(y, x, q, k),
            device_id_type=MESH,
        )

    for s in range(2):

        @pl.when(spots[s] == rc)
        def _():
            for p in range(3):
                load(s, p).start()

    for p in range(3):
        for k in range(2):
            stage(k, p).start()

    for s in range(2):

        @pl.when(spots[s] == rc)
        def _():
            for p in range(3):
                load(s, p).wait()

    def start_home():
        for p in range(3):
            for k in range(2):
                stage(k, p).wait()

                @pl.when(stay[k])
                def _():
                    pltpu.make_async_copy(staged(k, p), home(z, p), home_recv.at[z, p]).start()

                @pl.when(jnp.logical_not(stay[k]))
                def _():
                    home_copy(k, p).start()

    def wave(t, carry):
        @pl.when(t == HOME_AT)
        def _():
            start_home()

        for s in range(2):
            spot = spots[s]
            depth, passes, sends = trees[s]
            for p in range(3):
                i = t - table(spot, depth[p])

                @pl.when((i >= 0) & (i < N))
                def _():
                    @pl.when(spot != rc)
                    def _():
                        pltpu.make_async_copy(held(s, p, i), held(s, p, i), recv_sem.at[s, p, i]).wait()

                    def forward(to, sem):
                        return pltpu.make_async_remote_copy(
                            src_ref=held(s, p, i),
                            dst_ref=held(s, p, i),
                            send_sem=sem,
                            recv_sem=recv_sem.at[s, p, i],
                            device_id=to,
                            device_id_type=MESH,
                        )

                    for m, row in enumerate(sends[p]):
                        child = table(spot, row)

                        @pl.when(child >= 0)
                        def _():
                            to = dev(flip(child // 8, s), flip((child // 4) % 2, ra), flip((child // 2) % 2, rb), child % 2)
                            forward(to, send_sem.at[s, p, m]).start()

                    @pl.when(table(spot, passes[p]) == 1)
                    def _():
                        forward(dev(z, y, x, 1 - q), side_send.at[s, p]).start()

        return carry

    lax.fori_loop(0, N + LAG * DEEPEST + 1, wave, 0)

    for s in range(2):
        spot = spots[s]
        _, passes, sends = trees[s]
        for p in range(3):
            for m, row in enumerate(sends[p]):

                @pl.when(table(spot, row) >= 0)
                def _():
                    pltpu.make_async_copy(held(s, p), held(s, p), send_sem.at[s, p, m]).wait()

            @pl.when(table(spot, passes[p]) == 1)
            def _():
                pltpu.make_async_copy(held(s, p), held(s, p), side_send.at[s, p]).wait()

    for k in range(2):

        @pl.when(jnp.logical_not(stay[k]))
        def _():
            for p in range(3):
                home_copy(k, p).wait_send()

    for s in range(2):
        for p in range(3):
            pltpu.make_async_copy(home(s, p), home(s, p), home_recv.at[s, p]).wait()


def place_kernel(slots, home13, homed, hot13, hotd, out13, outd, zero, sem):
    me = lax.axis_index("stage") * 8 + lax.axis_index("expert")
    zero[...] = jnp.zeros_like(zero)

    def pieces(layer, slot):
        return out13.at[layer, slot, :, pl.ds(0, 512)], out13.at[layer, slot, :, pl.ds(512, 512)], outd.at[layer, slot]

    for layer in range(2):
        pltpu.make_async_copy(home13.at[layer], out13.at[layer, 0], sem).start()
        pltpu.make_async_copy(homed.at[layer], outd.at[layer, 0], sem).start()
        for t in range(2):
            filled = slots[me, t] >= 0
            to = pieces(layer, t + 1)

            @pl.when(filled)
            def _():
                for p in range(3):
                    pltpu.make_async_copy(hotd.at[layer] if p == 2 else hot13.at[layer, p], to[p], sem).start()

            @pl.when(jnp.logical_not(filled))
            def _():
                for h in range(4):
                    pltpu.make_async_copy(zero, out13.at[layer, t + 1, pl.ds(h * 512, 512)], sem).start()
                for h in range(2):
                    pltpu.make_async_copy(zero, outd.at[layer, t + 1, :, pl.ds(h * 1024, 1024)], sem).start()

    for layer in range(2):
        for t in range(3):
            pltpu.make_async_copy(home13.at[layer], out13.at[layer, t], sem).wait()
            pltpu.make_async_copy(homed.at[layer], outd.at[layer, t], sem).wait()


def solution(mesh):
    DMA = pltpu.SemaphoreType.DMA

    VMEM = pl.BlockSpec(memory_space=pltpu.VMEM)

    def local(gate, up, down, hot_units, slot_map):
        def branch(unit, gate, up, down, slot_map):
            moved = pl.pallas_call(
                functools.partial(move_kernel, unit),
                out_shape=(
                    pltpu.VMEM((2, 2048, 1024), BF16),
                    pltpu.VMEM((2, 512, 2048), BF16),
                    pltpu.VMEM((2, 2, 2048, 512), BF16),
                    pltpu.VMEM((2, 512, 2048), BF16),
                ),
                in_specs=[ANY] * 3,
                out_specs=(VMEM,) * 4,
                scratch_shapes=[
                    pltpu.VMEM((2, 2, 2048, 512), BF16),
                    pltpu.VMEM((2, 512, 2048), BF16),
                    DMA((3,)),
                    DMA((2, 3)),
                    DMA((2, 3, N)),
                    DMA((2, 3, 2)),
                    DMA((2, 3)),
                    DMA((2, 3)),
                    DMA((2, 3)),
                ],
                compiler_params=pltpu.CompilerParams(has_side_effects=True, vmem_limit_bytes=14 << 20),
                name=f"move{unit}",
            )(gate, up, down)
            return pl.pallas_call(
                place_kernel,
                out_shape=(
                    jax.ShapeDtypeStruct((2, 3, 2048, 1024), BF16),
                    jax.ShapeDtypeStruct((2, 3, 512, 2048), BF16),
                ),
                in_specs=[pl.BlockSpec(memory_space=pltpu.SMEM)] + [VMEM] * 4,
                out_specs=(ANY, ANY),
                scratch_shapes=[pltpu.VMEM((512, 1024), BF16), DMA],
                compiler_params=pltpu.CompilerParams(vmem_limit_bytes=4 << 20),
                name="place",
            )(slot_map, *moved)

        return lax.switch(hot_units[0], [functools.partial(branch, u) for u in range(16)], gate, up, down, slot_map)

    spec = P("stage", "expert")
    out = P(None, ("stage", "expert"))
    return jax.shard_map(local, mesh=mesh, in_specs=(spec, spec, spec, P(), P()), out_specs=(out, out), check_vma=False)
```

```python
import functools

import jax
import jax.numpy as jnp
from jax import lax
from jax.experimental import pallas as pl
from jax.experimental.pallas import tpu as pltpu
from jax.sharding import PartitionSpec as P

MESH = pl.DeviceIdType.MESH
ANY = pl.BlockSpec(memory_space=pl.ANY)
BF16 = jnp.bfloat16

PARENT = (
    (None, 0, 3, 1, 5, 1, 7, 5),
    (None, 3, 0, 2, 6, 7, 2, 3),
    (None, 5, 6, 7, 0, 4, 4, 6),
)
DEPTH = (
    (0, 1, 3, 2, 3, 2, 4, 3),
    (0, 3, 1, 2, 3, 4, 2, 3),
    (0, 3, 3, 4, 1, 2, 2, 3),
)
CHILDREN = tuple(tuple(tuple(v for v in range(1, 8) if par[v] == r) for r in range(8)) for par in PARENT)
DEEPEST = max(map(max, DEPTH))
N = 32
HOME_AT = 2
LAG = 2


def coords():
    z = lax.axis_index("stage")
    j = lax.axis_index("expert")
    return z, j // 4, (j // 2) % 2, j % 2


def dev(z, y, x, q):
    return (z, y * 4 + x * 2 + q)


def flip(v, bit):
    return 1 - v if bit else v


def table(index, values):
    out = jnp.int32(values[0])
    for i, v in enumerate(values[1:], 1):
        if v != values[0]:
            out = jnp.where(index == i, jnp.int32(v), out)
    return out


def roles(s, rb, rc):
    depth, passes, sends = [], [], []
    for p in range(3):
        def sender(r, v):
            x = (r & 1) ^ rb
            return x if r ^ v == 1 else 1 - x

        def entry(r):
            if r == 0:
                return rc
            children = CHILDREN[p][r]
            return sender(r, children[0]) if children else s

        depth.append([LAG * DEPTH[p][r] + (q != entry(r)) for r in range(8) for q in range(2)])
        passes.append([int(q == entry(r)) for r in range(8) for q in range(2)])
        to = [[v * 2 + entry(v) for v in CHILDREN[p][r] if sender(r, v) == q] for r in range(8) for q in range(2)]
        sends.append([[t[m] if len(t) > m else -1 for t in to] for m in range(max(map(len, to)))])
    return depth, passes, sends


def move_kernel(unit, gate, up, down, home13, homed, vg, vd, sg, sd, load_sem, stage_sem, recv_sem, send_sem, side_send, home_send, home_recv):
    e, half = unit // 2, unit % 2
    ra, rb, rc = e // 4, (e // 2) % 2, e % 2
    z, y, x, q = coords()

    def source(k, p):
        return down.at[0, 0, pl.ds(k * 512, 512), :] if p == 2 else (gate, up)[p].at[0, 0, :, pl.ds(k * 512, 512)]

    def staged(k, p):
        return sd.at[k] if p == 2 else sg.at[k, p]

    def held(s, p, i=None):
        if p == 2:
            return vd.at[s] if i is None else vd.at[s, pl.ds(i * (512 // N), 512 // N), :]
        return vg.at[s, p] if i is None else vg.at[s, p, pl.ds(i * (2048 // N), 2048 // N), :]

    def home(s, p):
        return homed.at[s] if p == 2 else home13.at[s, :, pl.ds(p * 512, 512)]

    trees = [roles(s, rb, rc) for s in range(2)]
    rels = [flip(z, s) * 4 + flip(y, ra) * 2 + flip(x, rb) for s in range(2)]
    spots = [rel * 2 + q for rel in rels]
    stay = [(z == y) & (y == x) & (x == q) & (q == k) for k in range(2)]

    def stage(k, p):
        return pltpu.make_async_copy(source(k, p), staged(k, p), stage_sem.at[k, p])

    def load(s, p):
        return pltpu.make_async_copy(source(half, p), held(s, p), load_sem.at[p])

    def home_copy(k, p):
        return pltpu.make_async_remote_copy(
            src_ref=staged(k, p),
            dst_ref=home(z, p),
            send_sem=home_send.at[k, p],
            recv_sem=home_recv.at[z, p],
            device_id=dev(y, x, q, k),
            device_id_type=MESH,
        )

    for s in range(2):

        @pl.when(spots[s] == rc)
        def _():
            for p in range(3):
                load(s, p).start()

    for p in range(3):
        for k in range(2):
            stage(k, p).start()

    for s in range(2):

        @pl.when(spots[s] == rc)
        def _():
            for p in range(3):
                load(s, p).wait()

    def start_home():
        for p in range(3):
            for k in range(2):
                stage(k, p).wait()

                @pl.when(stay[k])
                def _():
                    pltpu.make_async_copy(staged(k, p), home(z, p), home_recv.at[z, p]).start()

                @pl.when(jnp.logical_not(stay[k]))
                def _():
                    home_copy(k, p).start()

    def wave(t, carry):
        @pl.when(t == HOME_AT)
        def _():
            start_home()

        for s in range(2):
            spot = spots[s]
            depth, passes, sends = trees[s]
            for p in range(3):
                i = t - table(spot, depth[p])

                @pl.when((i >= 0) & (i < N))
                def _():
                    @pl.when(spot != rc)
                    def _():
                        pltpu.make_async_copy(held(s, p, i), held(s, p, i), recv_sem.at[s, p, i]).wait()

                    def forward(to, sem):
                        return pltpu.make_async_remote_copy(
                            src_ref=held(s, p, i),
                            dst_ref=held(s, p, i),
                            send_sem=sem,
                            recv_sem=recv_sem.at[s, p, i],
                            device_id=to,
                            device_id_type=MESH,
                        )

                    for m, row in enumerate(sends[p]):
                        child = table(spot, row)

                        @pl.when(child >= 0)
                        def _():
                            to = dev(flip(child // 8, s), flip((child // 4) % 2, ra), flip((child // 2) % 2, rb), child % 2)
                            forward(to, send_sem.at[s, p, m]).start()

                    @pl.when(table(spot, passes[p]) == 1)
                    def _():
                        forward(dev(z, y, x, 1 - q), side_send.at[s, p]).start()

        return carry

    lax.fori_loop(0, N + LAG * DEEPEST + 1, wave, 0)

    for s in range(2):
        spot = spots[s]
        _, passes, sends = trees[s]
        for p in range(3):
            for m, row in enumerate(sends[p]):

                @pl.when(table(spot, row) >= 0)
                def _():
                    pltpu.make_async_copy(held(s, p), held(s, p), send_sem.at[s, p, m]).wait()

            @pl.when(table(spot, passes[p]) == 1)
            def _():
                pltpu.make_async_copy(held(s, p), held(s, p), side_send.at[s, p]).wait()

    for k in range(2):

        @pl.when(jnp.logical_not(stay[k]))
        def _():
            for p in range(3):
                home_copy(k, p).wait_send()

    for s in range(2):
        for p in range(3):
            pltpu.make_async_copy(home(s, p), home(s, p), home_recv.at[s, p]).wait()


def place_kernel(slots, home13, homed, hot13, hotd, out13, outd, zero, sem):
    me = lax.axis_index("stage") * 8 + lax.axis_index("expert")
    zero[...] = jnp.zeros_like(zero)

    def pieces(layer, slot):
        return out13.at[layer, slot, :, pl.ds(0, 512)], out13.at[layer, slot, :, pl.ds(512, 512)], outd.at[layer, slot]

    for layer in range(2):
        pltpu.make_async_copy(home13.at[layer], out13.at[layer, 0], sem).start()
        pltpu.make_async_copy(homed.at[layer], outd.at[layer, 0], sem).start()
        for t in range(2):
            filled = slots[me, t] >= 0
            to = pieces(layer, t + 1)

            @pl.when(filled)
            def _():
                for p in range(3):
                    pltpu.make_async_copy(hotd.at[layer] if p == 2 else hot13.at[layer, p], to[p], sem).start()

            @pl.when(jnp.logical_not(filled))
            def _():
                for h in range(4):
                    pltpu.make_async_copy(zero, out13.at[layer, t + 1, pl.ds(h * 512, 512)], sem).start()
                for h in range(2):
                    pltpu.make_async_copy(zero, outd.at[layer, t + 1, :, pl.ds(h * 1024, 1024)], sem).start()

    for layer in range(2):
        for t in range(3):
            pltpu.make_async_copy(home13.at[layer], out13.at[layer, t], sem).wait()
            pltpu.make_async_copy(homed.at[layer], outd.at[layer, t], sem).wait()


def solution(mesh):
    DMA = pltpu.SemaphoreType.DMA

    VMEM = pl.BlockSpec(memory_space=pltpu.VMEM)

    def local(gate, up, down, hot_units, slot_map):
        def branch(unit, gate, up, down, slot_map):
            moved = pl.pallas_call(
                functools.partial(move_kernel, unit),
                out_shape=(
                    pltpu.VMEM((2, 2048, 1024), BF16),
                    pltpu.VMEM((2, 512, 2048), BF16),
                    pltpu.VMEM((2, 2, 2048, 512), BF16),
                    pltpu.VMEM((2, 512, 2048), BF16),
                ),
                in_specs=[ANY] * 3,
                out_specs=(VMEM,) * 4,
                scratch_shapes=[
                    pltpu.VMEM((2, 2, 2048, 512), BF16),
                    pltpu.VMEM((2, 512, 2048), BF16),
                    DMA((3,)),
                    DMA((2, 3)),
                    DMA((2, 3, N)),
                    DMA((2, 3, 2)),
                    DMA((2, 3)),
                    DMA((2, 3)),
                    DMA((2, 3)),
                ],
                compiler_params=pltpu.CompilerParams(has_side_effects=True, vmem_limit_bytes=14 << 20),
                name=f"move{unit}",
            )(gate, up, down)
            return pl.pallas_call(
                place_kernel,
                out_shape=(
                    jax.ShapeDtypeStruct((2, 3, 2048, 1024), BF16),
                    jax.ShapeDtypeStruct((2, 3, 512, 2048), BF16),
                ),
                in_specs=[pl.BlockSpec(memory_space=pltpu.SMEM)] + [VMEM] * 4,
                out_specs=(ANY, ANY),
                scratch_shapes=[pltpu.VMEM((512, 1024), BF16), DMA],
                compiler_params=pltpu.CompilerParams(vmem_limit_bytes=4 << 20),
                name="place",
            )(slot_map, *moved)

        return lax.switch(hot_units[0], [functools.partial(branch, u) for u in range(16)], gate, up, down, slot_map)

    spec = P("stage", "expert")
    out = P(None, ("stage", "expert"))
    return jax.shard_map(local, mesh=mesh, in_specs=(spec, spec, spec, P(), P()), out_specs=(out, out), check_vma=False)
```

```python
import functools

import jax
import jax.numpy as jnp
from jax import lax
from jax.experimental import pallas as pl
from jax.experimental.pallas import tpu as pltpu
from jax.sharding import PartitionSpec as P

MESH = pl.DeviceIdType.MESH
ANY = pl.BlockSpec(memory_space=pl.ANY)
BF16 = jnp.bfloat16

PARENT = (
    (None, 0, 3, 1, 5, 1, 7, 5),
    (None, 3, 0, 2, 6, 7, 2, 3),
    (None, 5, 6, 7, 0, 4, 4, 6),
)
DEPTH = (
    (0, 1, 3, 2, 3, 2, 4, 3),
    (0, 3, 1, 2, 3, 4, 2, 3),
    (0, 3, 3, 4, 1, 2, 2, 3),
)
CHILDREN = tuple(tuple(tuple(v for v in range(1, 8) if par[v] == r) for r in range(8)) for par in PARENT)
DEEPEST = max(map(max, DEPTH))
N = 32
HOME_AT = 0
LAG = 5


def coords():
    z = lax.axis_index("stage")
    j = lax.axis_index("expert")
    return z, j // 4, (j // 2) % 2, j % 2


def dev(z, y, x, q):
    return (z, y * 4 + x * 2 + q)


def flip(v, bit):
    return 1 - v if bit else v


def table(index, values):
    out = jnp.int32(values[0])
    for i, v in enumerate(values[1:], 1):
        if v != values[0]:
            out = jnp.where(index == i, jnp.int32(v), out)
    return out


def roles(s, rb, rc):
    depth, passes, sends = [], [], []
    for p in range(3):
        def sender(r, v):
            x = (r & 1) ^ rb
            return x if r ^ v == 1 else 1 - x

        def entry(r):
            if r == 0:
                return rc
            children = CHILDREN[p][r]
            return sender(r, children[0]) if children else s

        depth.append([LAG * DEPTH[p][r] + (q != entry(r)) for r in range(8) for q in range(2)])
        passes.append([int(q == entry(r)) for r in range(8) for q in range(2)])
        to = [[v * 2 + entry(v) for v in CHILDREN[p][r] if sender(r, v) == q] for r in range(8) for q in range(2)]
        sends.append([[t[m] if len(t) > m else -1 for t in to] for m in range(max(map(len, to)))])
    return depth, passes, sends


def move_kernel(unit, gate, up, down, home13, homed, vg, vd, sg, sd, load_sem, stage_sem, recv_sem, send_sem, side_send, home_send, home_recv):
    e, half = unit // 2, unit % 2
    ra, rb, rc = e // 4, (e // 2) % 2, e % 2
    z, y, x, q = coords()

    def source(k, p):
        return down.at[0, 0, pl.ds(k * 512, 512), :] if p == 2 else (gate, up)[p].at[0, 0, :, pl.ds(k * 512, 512)]

    def staged(k, p):
        return sd.at[k] if p == 2 else sg.at[k, p]

    def held(s, p, i=None):
        if p == 2:
            return vd.at[s] if i is None else vd.at[s, pl.ds(i * (512 // N), 512 // N), :]
        return vg.at[s, p] if i is None else vg.at[s, p, pl.ds(i * (2048 // N), 2048 // N), :]

    def home(s, p):
        return homed.at[s] if p == 2 else home13.at[s, :, pl.ds(p * 512, 512)]

    trees = [roles(s, rb, rc) for s in range(2)]
    rels = [flip(z, s) * 4 + flip(y, ra) * 2 + flip(x, rb) for s in range(2)]
    spots = [rel * 2 + q for rel in rels]
    stay = [(z == y) & (y == x) & (x == q) & (q == k) for k in range(2)]

    def stage(k, p):
        return pltpu.make_async_copy(source(k, p), staged(k, p), stage_sem.at[k, p])

    def load(s, p):
        return pltpu.make_async_copy(source(half, p), held(s, p), load_sem.at[p])

    def home_copy(k, p):
        return pltpu.make_async_remote_copy(
            src_ref=staged(k, p),
            dst_ref=home(z, p),
            send_sem=home_send.at[k, p],
            recv_sem=home_recv.at[z, p],
            device_id=dev(y, x, q, k),
            device_id_type=MESH,
        )

    for s in range(2):

        @pl.when(spots[s] == rc)
        def _():
            for p in range(3):
                load(s, p).start()

    for p in range(3):
        for k in range(2):
            stage(k, p).start()

    for s in range(2):

        @pl.when(spots[s] == rc)
        def _():
            for p in range(3):
                load(s, p).wait()

    def start_home():
        for p in range(3):
            for k in range(2):
                stage(k, p).wait()

                @pl.when(stay[k])
                def _():
                    pltpu.make_async_copy(staged(k, p), home(z, p), home_recv.at[z, p]).start()

                @pl.when(jnp.logical_not(stay[k]))
                def _():
                    home_copy(k, p).start()

    def wave(t, carry):
        @pl.when(t == HOME_AT)
        def _():
            start_home()

        for s in range(2):
            spot = spots[s]
            depth, passes, sends = trees[s]
            for p in range(3):
                i = t - table(spot, depth[p])

                @pl.when((i >= 0) & (i < N))
                def _():
                    @pl.when(spot != rc)
                    def _():
                        pltpu.make_async_copy(held(s, p, i), held(s, p, i), recv_sem.at[s, p, i]).wait()

                    def forward(to, sem):
                        return pltpu.make_async_remote_copy(
                            src_ref=held(s, p, i),
                            dst_ref=held(s, p, i),
                            send_sem=sem,
                            recv_sem=recv_sem.at[s, p, i],
                            device_id=to,
                            device_id_type=MESH,
                        )

                    for m, row in enumerate(sends[p]):
                        child = table(spot, row)

                        @pl.when(child >= 0)
                        def _():
                            to = dev(flip(child // 8, s), flip((child // 4) % 2, ra), flip((child // 2) % 2, rb), child % 2)
                            forward(to, send_sem.at[s, p, m]).start()

                    @pl.when(table(spot, passes[p]) == 1)
                    def _():
                        forward(dev(z, y, x, 1 - q), side_send.at[s, p]).start()

        return carry

    lax.fori_loop(0, N + LAG * DEEPEST + 1, wave, 0)

    for s in range(2):
        spot = spots[s]
        _, passes, sends = trees[s]
        for p in range(3):
            for m, row in enumerate(sends[p]):

                @pl.when(table(spot, row) >= 0)
                def _():
                    pltpu.make_async_copy(held(s, p), held(s, p), send_sem.at[s, p, m]).wait()

            @pl.when(table(spot, passes[p]) == 1)
            def _():
                pltpu.make_async_copy(held(s, p), held(s, p), side_send.at[s, p]).wait()

    for k in range(2):

        @pl.when(jnp.logical_not(stay[k]))
        def _():
            for p in range(3):
                home_copy(k, p).wait_send()

    for s in range(2):
        for p in range(3):
            pltpu.make_async_copy(home(s, p), home(s, p), home_recv.at[s, p]).wait()


def place_kernel(slots, home13, homed, hot13, hotd, out13, outd, zero, sem):
    me = lax.axis_index("stage") * 8 + lax.axis_index("expert")
    zero[...] = jnp.zeros_like(zero)

    def pieces(layer, slot):
        return out13.at[layer, slot, :, pl.ds(0, 512)], out13.at[layer, slot, :, pl.ds(512, 512)], outd.at[layer, slot]

    for layer in range(2):
        pltpu.make_async_copy(home13.at[layer], out13.at[layer, 0], sem).start()
        pltpu.make_async_copy(homed.at[layer], outd.at[layer, 0], sem).start()
        for t in range(2):
            filled = slots[me, t] >= 0
            to = pieces(layer, t + 1)

            @pl.when(filled)
            def _():
                for p in range(3):
                    pltpu.make_async_copy(hotd.at[layer] if p == 2 else hot13.at[layer, p], to[p], sem).start()

            @pl.when(jnp.logical_not(filled))
            def _():
                for h in range(4):
                    pltpu.make_async_copy(zero, out13.at[layer, t + 1, pl.ds(h * 512, 512)], sem).start()
                for h in range(2):
                    pltpu.make_async_copy(zero, outd.at[layer, t + 1, :, pl.ds(h * 1024, 1024)], sem).start()

    for layer in range(2):
        for t in range(3):
            pltpu.make_async_copy(home13.at[layer], out13.at[layer, t], sem).wait()
            pltpu.make_async_copy(homed.at[layer], outd.at[layer, t], sem).wait()


def solution(mesh):
    DMA = pltpu.SemaphoreType.DMA

    VMEM = pl.BlockSpec(memory_space=pltpu.VMEM)

    def local(gate, up, down, hot_units, slot_map):
        def branch(unit, gate, up, down, slot_map):
            moved = pl.pallas_call(
                functools.partial(move_kernel, unit),
                out_shape=(
                    pltpu.VMEM((2, 2048, 1024), BF16),
                    pltpu.VMEM((2, 512, 2048), BF16),
                    pltpu.VMEM((2, 2, 2048, 512), BF16),
                    pltpu.VMEM((2, 512, 2048), BF16),
                ),
                in_specs=[ANY] * 3,
                out_specs=(VMEM,) * 4,
                scratch_shapes=[
                    pltpu.VMEM((2, 2, 2048, 512), BF16),
                    pltpu.VMEM((2, 512, 2048), BF16),
                    DMA((3,)),
                    DMA((2, 3)),
                    DMA((2, 3, N)),
                    DMA((2, 3, 2)),
                    DMA((2, 3)),
                    DMA((2, 3)),
                    DMA((2, 3)),
                ],
                compiler_params=pltpu.CompilerParams(has_side_effects=True, vmem_limit_bytes=14 << 20),
                name=f"move{unit}",
            )(gate, up, down)
            return pl.pallas_call(
                place_kernel,
                out_shape=(
                    jax.ShapeDtypeStruct((2, 3, 2048, 1024), BF16),
                    jax.ShapeDtypeStruct((2, 3, 512, 2048), BF16),
                ),
                in_specs=[pl.BlockSpec(memory_space=pltpu.SMEM)] + [VMEM] * 4,
                out_specs=(ANY, ANY),
                scratch_shapes=[pltpu.VMEM((512, 1024), BF16), DMA],
                compiler_params=pltpu.CompilerParams(vmem_limit_bytes=4 << 20),
                name="place",
            )(slot_map, *moved)

        return lax.switch(hot_units[0], [functools.partial(branch, u) for u in range(16)], gate, up, down, slot_map)

    spec = P("stage", "expert")
    out = P(None, ("stage", "expert"))
    return jax.shard_map(local, mesh=mesh, in_specs=(spec, spec, spec, P(), P()), out_specs=(out, out), check_vma=False)
```

```python
import functools

import jax
import jax.numpy as jnp
from jax import lax
from jax.experimental import pallas as pl
from jax.experimental.pallas import tpu as pltpu
from jax.sharding import PartitionSpec as P

MESH = pl.DeviceIdType.MESH
ANY = pl.BlockSpec(memory_space=pl.ANY)
BF16 = jnp.bfloat16

PARENT = (
    (None, 0, 3, 1, 5, 1, 7, 5),
    (None, 3, 0, 2, 6, 7, 2, 3),
    (None, 5, 6, 7, 0, 4, 4, 6),
)
DEPTH = (
    (0, 1, 3, 2, 3, 2, 4, 3),
    (0, 3, 1, 2, 3, 4, 2, 3),
    (0, 3, 3, 4, 1, 2, 2, 3),
)
CHILDREN = tuple(tuple(tuple(v for v in range(1, 8) if par[v] == r) for r in range(8)) for par in PARENT)
DEEPEST = max(map(max, DEPTH))
SENDS = tuple(tuple(tuple(c[m] if len(c) > m else -1 for c in tree) for m in range(max(map(len, tree)))) for tree in CHILDREN)
N = 64
LAG = 5


def coords():
    z = lax.axis_index("stage")
    j = lax.axis_index("expert")
    return z, j // 4, (j // 2) % 2, j % 2


def dev(z, y, x, q):
    return (z, y * 4 + x * 2 + q)


def flip(v, bit):
    return 1 - v if bit else v


def table(index, values):
    out = jnp.int32(values[0])
    for i, v in enumerate(values[1:], 1):
        if v != values[0]:
            out = jnp.where(index == i, jnp.int32(v), out)
    return out


def move_kernel(unit, gate, up, down, home13, homed, vg, vd, sg, sd, load_sem, stage_sem, recv_sem, send_sem, side_send, side_recv, home_send, home_recv):
    e, half = unit // 2, unit % 2
    ra, rb, rc = e // 4, (e // 2) % 2, e % 2
    z, y, x, q = coords()

    def source(k, p):
        return down.at[0, 0, pl.ds(k * 512, 512), :] if p == 2 else (gate, up)[p].at[0, 0, :, pl.ds(k * 512, 512)]

    def staged(k, p):
        return sd.at[k] if p == 2 else sg.at[k, p]

    def held(s, p, i=None):
        if p == 2:
            return vd.at[s] if i is None else vd.at[s, pl.ds(i * (512 // N), 512 // N), :]
        return vg.at[s, p] if i is None else vg.at[s, p, pl.ds(i * (2048 // N), 2048 // N), :]

    def home(s, p):
        return homed.at[s] if p == 2 else home13.at[s, :, pl.ds(p * 512, 512)]

    rels = [flip(z, s) * 4 + flip(y, ra) * 2 + flip(x, rb) for s in range(2)]
    relays = [q == jnp.where(rels[s] == 0, rc, s) for s in range(2)]
    roots = [relays[s] & (rels[s] == 0) for s in range(2)]
    stay = [(z == y) & (y == x) & (x == q) & (q == k) for k in range(2)]

    def stage(k, p):
        return pltpu.make_async_copy(source(k, p), staged(k, p), stage_sem.at[k, p])

    def load(s, p):
        return pltpu.make_async_copy(source(half, p), held(s, p), load_sem.at[p])

    def home_copy(k, p):
        return pltpu.make_async_remote_copy(
            src_ref=staged(k, p),
            dst_ref=home(z, p),
            send_sem=home_send.at[k, p],
            recv_sem=home_recv.at[z, p],
            device_id=dev(y, x, q, k),
            device_id_type=MESH,
        )

    for s in range(2):

        @pl.when(roots[s])
        def _():
            for p in range(3):
                load(s, p).start()

    for p in range(3):
        for k in range(2):
            stage(k, p).start()

    barrier = pltpu.get_barrier_semaphore()

    def greet(d, carry):
        @pl.when((d // 8 != z) | (d % 8 != y * 4 + x * 2 + q))
        def _():
            pl.semaphore_signal(barrier, inc=1, device_id=(d // 8, d % 8), device_id_type=MESH)

        return carry

    lax.fori_loop(0, 16, greet, 0)
    pl.semaphore_wait(barrier, 15)

    for s in range(2):

        @pl.when(roots[s])
        def _():
            for p in range(3):
                load(s, p).wait()

    def start_home():
        for p in range(3):
            for k in range(2):
                stage(k, p).wait()

                @pl.when(stay[k])
                def _():
                    pltpu.make_async_copy(staged(k, p), home(z, p), home_recv.at[z, p]).start()

                @pl.when(jnp.logical_not(stay[k]))
                def _():
                    home_copy(k, p).start()

    last = jnp.int32(0)
    for s in range(2):
        deepest = table(rels[s], [max(DEPTH[p][r] for p in range(3) if CHILDREN[p][r] or r == 0) for r in range(8)])
        last = jnp.maximum(last, jnp.where(relays[s], deepest, 0))
    home_at = N + LAG * last

    def wave(t, carry):
        for s in range(2):
            rel = rels[s]
            for p in range(3):
                i = t - LAG * table(rel, DEPTH[p])

                @pl.when(relays[s] & (i >= 0) & (i < N))
                def _():
                    @pl.when(rel != 0)
                    def _():
                        pltpu.make_async_copy(held(s, p, i), held(s, p, i), recv_sem.at[s, p, i]).wait()

                    def forward(to, sem, arrival):
                        pltpu.make_async_remote_copy(
                            src_ref=held(s, p, i),
                            dst_ref=held(s, p, i),
                            send_sem=sem,
                            recv_sem=arrival,
                            device_id=to,
                            device_id_type=MESH,
                        ).start()

                    for m, row in enumerate(SENDS[p]):
                        child = table(rel, row)

                        @pl.when(child >= 0)
                        def _():
                            to = dev(flip(child // 4, s), flip((child // 2) % 2, ra), flip(child % 2, rb), s)
                            forward(to, send_sem.at[s, p, m], recv_sem.at[s, p, i])

                    forward(dev(z, y, x, 1 - q), side_send.at[s, p], side_recv.at[s, p])

        @pl.when(t == home_at)
        def _():
            start_home()

        return carry

    lax.fori_loop(0, N + LAG * DEEPEST + 1, wave, 0)

    for s in range(2):
        for p in range(3):

            @pl.when(relays[s])
            def _():
                for m, row in enumerate(SENDS[p]):

                    @pl.when(table(rels[s], row) >= 0)
                    def _():
                        pltpu.make_async_copy(held(s, p), held(s, p), send_sem.at[s, p, m]).wait()

                pltpu.make_async_copy(held(s, p), held(s, p), side_send.at[s, p]).wait()

            @pl.when(jnp.logical_not(relays[s]))
            def _():
                pltpu.make_async_copy(held(s, p), held(s, p), side_recv.at[s, p]).wait()

    for k in range(2):

        @pl.when(jnp.logical_not(stay[k]))
        def _():
            for p in range(3):
                home_copy(k, p).wait_send()

    for s in range(2):
        for p in range(3):
            pltpu.make_async_copy(home(s, p), home(s, p), home_recv.at[s, p]).wait()


def place_kernel(slots, home13, homed, hot13, hotd, out13, outd, zero, sem):
    me = lax.axis_index("stage") * 8 + lax.axis_index("expert")
    zero[...] = jnp.zeros_like(zero)

    def pieces(layer, slot):
        return out13.at[layer, slot, :, pl.ds(0, 512)], out13.at[layer, slot, :, pl.ds(512, 512)], outd.at[layer, slot]

    for layer in range(2):
        pltpu.make_async_copy(home13.at[layer], out13.at[layer, 0], sem).start()
        pltpu.make_async_copy(homed.at[layer], outd.at[layer, 0], sem).start()
        for t in range(2):
            filled = slots[me, t] >= 0
            to = pieces(layer, t + 1)

            @pl.when(filled)
            def _():
                for p in range(3):
                    pltpu.make_async_copy(hotd.at[layer] if p == 2 else hot13.at[layer, p], to[p], sem).start()

            @pl.when(jnp.logical_not(filled))
            def _():
                for h in range(4):
                    pltpu.make_async_copy(zero, out13.at[layer, t + 1, pl.ds(h * 512, 512)], sem).start()
                for h in range(2):
                    pltpu.make_async_copy(zero, outd.at[layer, t + 1, :, pl.ds(h * 1024, 1024)], sem).start()

    for layer in range(2):
        for t in range(3):
            pltpu.make_async_copy(home13.at[layer], out13.at[layer, t], sem).wait()
            pltpu.make_async_copy(homed.at[layer], outd.at[layer, t], sem).wait()


def solution(mesh):
    DMA = pltpu.SemaphoreType.DMA

    VMEM = pl.BlockSpec(memory_space=pltpu.VMEM)

    def local(gate, up, down, hot_units, slot_map):
        def branch(unit, gate, up, down, slot_map):
            moved = pl.pallas_call(
                functools.partial(move_kernel, unit),
                out_shape=(
                    pltpu.VMEM((2, 2048, 1024), BF16),
                    pltpu.VMEM((2, 512, 2048), BF16),
                    pltpu.VMEM((2, 2, 2048, 512), BF16),
                    pltpu.VMEM((2, 512, 2048), BF16),
                ),
                in_specs=[ANY] * 3,
                out_specs=(VMEM,) * 4,
                scratch_shapes=[
                    pltpu.VMEM((2, 2, 2048, 512), BF16),
                    pltpu.VMEM((2, 512, 2048), BF16),
                    DMA((3,)),
                    DMA((2, 3)),
                    DMA((2, 3, N)),
                    DMA((2, 3, 2)),
                    DMA((2, 3)),
                    DMA((2, 3)),
                    DMA((2, 3)),
                    DMA((2, 3)),
                ],
                compiler_params=pltpu.CompilerParams(has_side_effects=True, collective_id=0, vmem_limit_bytes=14 << 20),
                name=f"move{unit}",
            )(gate, up, down)
            return pl.pallas_call(
                place_kernel,
                out_shape=(
                    jax.ShapeDtypeStruct((2, 3, 2048, 1024), BF16),
                    jax.ShapeDtypeStruct((2, 3, 512, 2048), BF16),
                ),
                in_specs=[pl.BlockSpec(memory_space=pltpu.SMEM)] + [VMEM] * 4,
                out_specs=(ANY, ANY),
                scratch_shapes=[pltpu.VMEM((512, 1024), BF16), DMA],
                compiler_params=pltpu.CompilerParams(vmem_limit_bytes=4 << 20),
                name="place",
            )(slot_map, *moved)

        return lax.switch(hot_units[0], [functools.partial(branch, u) for u in range(16)], gate, up, down, slot_map)

    spec = P("stage", "expert")
    out = P(None, ("stage", "expert"))
    return jax.shard_map(local, mesh=mesh, in_specs=(spec, spec, spec, P(), P()), out_specs=(out, out), check_vma=False)
```

```python
import functools

import jax
import jax.numpy as jnp
from jax import lax
from jax.experimental import pallas as pl
from jax.experimental.pallas import tpu as pltpu
from jax.sharding import PartitionSpec as P

MESH = pl.DeviceIdType.MESH
ANY = pl.BlockSpec(memory_space=pl.ANY)
BF16 = jnp.bfloat16

PARENT = (
    (None, 0, 3, 1, 5, 1, 7, 5),
    (None, 3, 0, 2, 6, 7, 2, 3),
    (None, 5, 6, 7, 0, 4, 4, 6),
)
DEPTH = (
    (0, 1, 3, 2, 3, 2, 4, 3),
    (0, 3, 1, 2, 3, 4, 2, 3),
    (0, 3, 3, 4, 1, 2, 2, 3),
)
CHILDREN = tuple(tuple(tuple(v for v in range(1, 8) if par[v] == r) for r in range(8)) for par in PARENT)
DEEPEST = max(map(max, DEPTH))
N = 32
HOME_AT = 3
LAG = 4


def coords():
    z = lax.axis_index("stage")
    j = lax.axis_index("expert")
    return z, j // 4, (j // 2) % 2, j % 2


def dev(z, y, x, q):
    return (z, y * 4 + x * 2 + q)


def flip(v, bit):
    return 1 - v if bit else v


def table(index, values):
    out = jnp.int32(values[0])
    for i, v in enumerate(values[1:], 1):
        if v != values[0]:
            out = jnp.where(index == i, jnp.int32(v), out)
    return out


def roles(s, rb, rc):
    depth, passes, sends = [], [], []
    for p in range(3):
        def sender(r, v):
            x = (r & 1) ^ rb
            return x if r ^ v == 1 else 1 - x

        def entry(r):
            if r == 0:
                return rc
            children = CHILDREN[p][r]
            return sender(r, children[0]) if children else s

        depth.append([LAG * DEPTH[p][r] + (q != entry(r)) for r in range(8) for q in range(2)])
        passes.append([int(q == entry(r)) for r in range(8) for q in range(2)])
        to = [[v * 2 + entry(v) for v in CHILDREN[p][r] if sender(r, v) == q] for r in range(8) for q in range(2)]
        sends.append([[t[m] if len(t) > m else -1 for t in to] for m in range(max(map(len, to)))])
    return depth, passes, sends


def move_kernel(unit, gate, up, down, home13, homed, vg, vd, sg, sd, load_sem, stage_sem, recv_sem, send_sem, side_send, home_send, home_recv):
    e, half = unit // 2, unit % 2
    ra, rb, rc = e // 4, (e // 2) % 2, e % 2
    z, y, x, q = coords()

    def source(k, p):
        return down.at[0, 0, pl.ds(k * 512, 512), :] if p == 2 else (gate, up)[p].at[0, 0, :, pl.ds(k * 512, 512)]

    def staged(k, p):
        return sd.at[k] if p == 2 else sg.at[k, p]

    def held(s, p, i=None):
        if p == 2:
            return vd.at[s] if i is None else vd.at[s, pl.ds(i * (512 // N), 512 // N), :]
        return vg.at[s, p] if i is None else vg.at[s, p, pl.ds(i * (2048 // N), 2048 // N), :]

    def home(s, p):
        return homed.at[s] if p == 2 else home13.at[s, :, pl.ds(p * 512, 512)]

    trees = [roles(s, rb, rc) for s in range(2)]
    rels = [flip(z, s) * 4 + flip(y, ra) * 2 + flip(x, rb) for s in range(2)]
    spots = [rel * 2 + q for rel in rels]
    stay = [(z == y) & (y == x) & (x == q) & (q == k) for k in range(2)]

    def stage(k, p):
        return pltpu.make_async_copy(source(k, p), staged(k, p), stage_sem.at[k, p])

    def load(s, p):
        return pltpu.make_async_copy(source(half, p), held(s, p), load_sem.at[p])

    def home_copy(k, p):
        return pltpu.make_async_remote_copy(
            src_ref=staged(k, p),
            dst_ref=home(z, p),
            send_sem=home_send.at[k, p],
            recv_sem=home_recv.at[z, p],
            device_id=dev(y, x, q, k),
            device_id_type=MESH,
        )

    for s in range(2):

        @pl.when(spots[s] == rc)
        def _():
            for p in range(3):
                load(s, p).start()

    for p in range(3):
        for k in range(2):
            stage(k, p).start()

    barrier = pltpu.get_barrier_semaphore()

    def greet(d, carry):
        @pl.when((d // 8 != z) | (d % 8 != y * 4 + x * 2 + q))
        def _():
            pl.semaphore_signal(barrier, inc=1, device_id=(d // 8, d % 8), device_id_type=MESH)

        return carry

    lax.fori_loop(0, 16, greet, 0)
    pl.semaphore_wait(barrier, 15)

    for s in range(2):

        @pl.when(spots[s] == rc)
        def _():
            for p in range(3):
                load(s, p).wait()

    def start_home():
        for p in range(3):
            for k in range(2):
                stage(k, p).wait()

                @pl.when(stay[k])
                def _():
                    pltpu.make_async_copy(staged(k, p), home(z, p), home_recv.at[z, p]).start()

                @pl.when(jnp.logical_not(stay[k]))
                def _():
                    home_copy(k, p).start()

    def wave(t, carry):
        @pl.when(t == HOME_AT)
        def _():
            start_home()

        for s in range(2):
            spot = spots[s]
            depth, passes, sends = trees[s]
            for p in range(3):
                i = t - table(spot, depth[p])

                @pl.when((i >= 0) & (i < N))
                def _():
                    @pl.when(spot != rc)
                    def _():
                        pltpu.make_async_copy(held(s, p, i), held(s, p, i), recv_sem.at[s, p, i]).wait()

                    def forward(to, sem):
                        return pltpu.make_async_remote_copy(
                            src_ref=held(s, p, i),
                            dst_ref=held(s, p, i),
                            send_sem=sem,
                            recv_sem=recv_sem.at[s, p, i],
                            device_id=to,
                            device_id_type=MESH,
                        )

                    for m, row in enumerate(sends[p]):
                        child = table(spot, row)

                        @pl.when(child >= 0)
                        def _():
                            to = dev(flip(child // 8, s), flip((child // 4) % 2, ra), flip((child // 2) % 2, rb), child % 2)
                            forward(to, send_sem.at[s, p, m]).start()

                    @pl.when(table(spot, passes[p]) == 1)
                    def _():
                        forward(dev(z, y, x, 1 - q), side_send.at[s, p]).start()

        return carry

    lax.fori_loop(0, N + LAG * DEEPEST + 1, wave, 0)

    for s in range(2):
        spot = spots[s]
        _, passes, sends = trees[s]
        for p in range(3):
            for m, row in enumerate(sends[p]):

                @pl.when(table(spot, row) >= 0)
                def _():
                    pltpu.make_async_copy(held(s, p), held(s, p), send_sem.at[s, p, m]).wait()

            @pl.when(table(spot, passes[p]) == 1)
            def _():
                pltpu.make_async_copy(held(s, p), held(s, p), side_send.at[s, p]).wait()

    for k in range(2):

        @pl.when(jnp.logical_not(stay[k]))
        def _():
            for p in range(3):
                home_copy(k, p).wait_send()

    for s in range(2):
        for p in range(3):
            pltpu.make_async_copy(home(s, p), home(s, p), home_recv.at[s, p]).wait()


def place_kernel(slots, home13, homed, hot13, hotd, out13, outd, zero, sem):
    me = lax.axis_index("stage") * 8 + lax.axis_index("expert")
    zero[...] = jnp.zeros_like(zero)

    def pieces(layer, slot):
        return out13.at[layer, slot, :, pl.ds(0, 512)], out13.at[layer, slot, :, pl.ds(512, 512)], outd.at[layer, slot]

    for layer in range(2):
        pltpu.make_async_copy(home13.at[layer], out13.at[layer, 0], sem).start()
        pltpu.make_async_copy(homed.at[layer], outd.at[layer, 0], sem).start()
        for t in range(2):
            filled = slots[me, t] >= 0
            to = pieces(layer, t + 1)

            @pl.when(filled)
            def _():
                for p in range(3):
                    pltpu.make_async_copy(hotd.at[layer] if p == 2 else hot13.at[layer, p], to[p], sem).start()

            @pl.when(jnp.logical_not(filled))
            def _():
                for h in range(4):
                    pltpu.make_async_copy(zero, out13.at[layer, t + 1, pl.ds(h * 512, 512)], sem).start()
                for h in range(2):
                    pltpu.make_async_copy(zero, outd.at[layer, t + 1, :, pl.ds(h * 1024, 1024)], sem).start()

    for layer in range(2):
        for t in range(3):
            pltpu.make_async_copy(home13.at[layer], out13.at[layer, t], sem).wait()
            pltpu.make_async_copy(homed.at[layer], outd.at[layer, t], sem).wait()


def solution(mesh):
    DMA = pltpu.SemaphoreType.DMA

    VMEM = pl.BlockSpec(memory_space=pltpu.VMEM)

    def local(gate, up, down, hot_units, slot_map):
        def branch(unit, gate, up, down, slot_map):
            moved = pl.pallas_call(
                functools.partial(move_kernel, unit),
                out_shape=(
                    pltpu.VMEM((2, 2048, 1024), BF16),
                    pltpu.VMEM((2, 512, 2048), BF16),
                    pltpu.VMEM((2, 2, 2048, 512), BF16),
                    pltpu.VMEM((2, 512, 2048), BF16),
                ),
                in_specs=[ANY] * 3,
                out_specs=(VMEM,) * 4,
                scratch_shapes=[
                    pltpu.VMEM((2, 2, 2048, 512), BF16),
                    pltpu.VMEM((2, 512, 2048), BF16),
                    DMA((3,)),
                    DMA((2, 3)),
                    DMA((2, 3, N)),
                    DMA((2, 3, 2)),
                    DMA((2, 3)),
                    DMA((2, 3)),
                    DMA((2, 3)),
                ],
                compiler_params=pltpu.CompilerParams(has_side_effects=True, collective_id=0, vmem_limit_bytes=14 << 20),
                name=f"move{unit}",
            )(gate, up, down)
            return pl.pallas_call(
                place_kernel,
                out_shape=(
                    jax.ShapeDtypeStruct((2, 3, 2048, 1024), BF16),
                    jax.ShapeDtypeStruct((2, 3, 512, 2048), BF16),
                ),
                in_specs=[pl.BlockSpec(memory_space=pltpu.SMEM)] + [VMEM] * 4,
                out_specs=(ANY, ANY),
                scratch_shapes=[pltpu.VMEM((512, 1024), BF16), DMA],
                compiler_params=pltpu.CompilerParams(vmem_limit_bytes=4 << 20),
                name="place",
            )(slot_map, *moved)

        return lax.switch(hot_units[0], [functools.partial(branch, u) for u in range(16)], gate, up, down, slot_map)

    spec = P("stage", "expert")
    out = P(None, ("stage", "expert"))
    return jax.shard_map(local, mesh=mesh, in_specs=(spec, spec, spec, P(), P()), out_specs=(out, out), check_vma=False)
```

```python
import functools

import jax
import jax.numpy as jnp
from jax import lax
from jax.experimental import pallas as pl
from jax.experimental.pallas import tpu as pltpu
from jax.sharding import PartitionSpec as P

MESH = pl.DeviceIdType.MESH
ANY = pl.BlockSpec(memory_space=pl.ANY)
BF16 = jnp.bfloat16

PARENT = (
    (None, 0, 3, 1, 5, 1, 7, 5),
    (None, 3, 0, 2, 6, 7, 2, 3),
    (None, 5, 6, 7, 0, 4, 4, 6),
)
DEPTH = (
    (0, 1, 3, 2, 3, 2, 4, 3),
    (0, 3, 1, 2, 3, 4, 2, 3),
    (0, 3, 3, 4, 1, 2, 2, 3),
)
CHILDREN = tuple(tuple(tuple(v for v in range(1, 8) if par[v] == r) for r in range(8)) for par in PARENT)
DEEPEST = max(map(max, DEPTH))
N = 32
HOME_AT = 6
LAG = 4


def coords():
    z = lax.axis_index("stage")
    j = lax.axis_index("expert")
    return z, j // 4, (j // 2) % 2, j % 2


def dev(z, y, x, q):
    return (z, y * 4 + x * 2 + q)


def flip(v, bit):
    return 1 - v if bit else v


def table(index, values):
    out = jnp.int32(values[0])
    for i, v in enumerate(values[1:], 1):
        if v != values[0]:
            out = jnp.where(index == i, jnp.int32(v), out)
    return out


def roles(s, rb, rc):
    depth, passes, sends = [], [], []
    for p in range(3):
        def sender(r, v):
            x = (r & 1) ^ rb
            return x if r ^ v == 1 else 1 - x

        def entry(r):
            if r == 0:
                return rc
            children = CHILDREN[p][r]
            return sender(r, children[0]) if children else s

        depth.append([LAG * DEPTH[p][r] + (q != entry(r)) for r in range(8) for q in range(2)])
        passes.append([int(q == entry(r)) for r in range(8) for q in range(2)])
        to = [[v * 2 + entry(v) for v in CHILDREN[p][r] if sender(r, v) == q] for r in range(8) for q in range(2)]
        sends.append([[t[m] if len(t) > m else -1 for t in to] for m in range(max(map(len, to)))])
    return depth, passes, sends


def move_kernel(unit, gate, up, down, home13, homed, vg, vd, sg, sd, load_sem, stage_sem, recv_sem, send_sem, side_send, home_send, home_recv):
    e, half = unit // 2, unit % 2
    ra, rb, rc = e // 4, (e // 2) % 2, e % 2
    z, y, x, q = coords()

    def source(k, p):
        return down.at[0, 0, pl.ds(k * 512, 512), :] if p == 2 else (gate, up)[p].at[0, 0, :, pl.ds(k * 512, 512)]

    def staged(k, p):
        return sd.at[k] if p == 2 else sg.at[k, p]

    def held(s, p, i=None):
        if p == 2:
            return vd.at[s] if i is None else vd.at[s, pl.ds(i * (512 // N), 512 // N), :]
        return vg.at[s, p] if i is None else vg.at[s, p, pl.ds(i * (2048 // N), 2048 // N), :]

    def home(s, p):
        return homed.at[s] if p == 2 else home13.at[s, :, pl.ds(p * 512, 512)]

    trees = [roles(s, rb, rc) for s in range(2)]
    rels = [flip(z, s) * 4 + flip(y, ra) * 2 + flip(x, rb) for s in range(2)]
    spots = [rel * 2 + q for rel in rels]
    stay = [(z == y) & (y == x) & (x == q) & (q == k) for k in range(2)]

    def stage(k, p):
        return pltpu.make_async_copy(source(k, p), staged(k, p), stage_sem.at[k, p])

    def load(s, p):
        return pltpu.make_async_copy(source(half, p), held(s, p), load_sem.at[p])

    def home_copy(k, p):
        return pltpu.make_async_remote_copy(
            src_ref=staged(k, p),
            dst_ref=home(z, p),
            send_sem=home_send.at[k, p],
            recv_sem=home_recv.at[z, p],
            device_id=dev(y, x, q, k),
            device_id_type=MESH,
        )

    for s in range(2):

        @pl.when(spots[s] == rc)
        def _():
            for p in range(3):
                load(s, p).start()

    for p in range(3):
        for k in range(2):
            stage(k, p).start()

    barrier = pltpu.get_barrier_semaphore()

    def greet(d, carry):
        @pl.when((d // 8 != z) | (d % 8 != y * 4 + x * 2 + q))
        def _():
            pl.semaphore_signal(barrier, inc=1, device_id=(d // 8, d % 8), device_id_type=MESH)

        return carry

    with jax.named_scope("greet"):
        lax.fori_loop(0, 16, greet, 0)
        pl.semaphore_wait(barrier, 15)

    for s in range(2):

        @pl.when(spots[s] == rc)
        def _():
            for p in range(3):
                load(s, p).wait()

    def start_home():
        for p in range(3):
            for k in range(2):
                stage(k, p).wait()

                @pl.when(stay[k])
                def _():
                    pltpu.make_async_copy(staged(k, p), home(z, p), home_recv.at[z, p]).start()

                @pl.when(jnp.logical_not(stay[k]))
                def _():
                    home_copy(k, p).start()

    def wave(t, carry):
        @pl.when(t == HOME_AT)
        def _():
            start_home()

        for s in range(2):
            spot = spots[s]
            depth, passes, sends = trees[s]
            for p in range(3):
                i = t - table(spot, depth[p])

                @pl.when((i >= 0) & (i < N))
                def _():
                    @pl.when(spot != rc)
                    def _():
                        pltpu.make_async_copy(held(s, p, i), held(s, p, i), recv_sem.at[s, p, i]).wait()

                    def forward(to, sem):
                        return pltpu.make_async_remote_copy(
                            src_ref=held(s, p, i),
                            dst_ref=held(s, p, i),
                            send_sem=sem,
                            recv_sem=recv_sem.at[s, p, i],
                            device_id=to,
                            device_id_type=MESH,
                        )

                    for m, row in enumerate(sends[p]):
                        child = table(spot, row)

                        @pl.when(child >= 0)
                        def _():
                            to = dev(flip(child // 8, s), flip((child // 4) % 2, ra), flip((child // 2) % 2, rb), child % 2)
                            forward(to, send_sem.at[s, p, m]).start()

                    @pl.when(table(spot, passes[p]) == 1)
                    def _():
                        forward(dev(z, y, x, 1 - q), side_send.at[s, p]).start()

        return carry

    with jax.named_scope("waves"):
        lax.fori_loop(0, N + LAG * DEEPEST + 1, wave, 0)

    with jax.named_scope("hot_sent"):
        for s in range(2):
            spot = spots[s]
            _, passes, sends = trees[s]
            for p in range(3):
                for m, row in enumerate(sends[p]):

                    @pl.when(table(spot, row) >= 0)
                    def _():
                        pltpu.make_async_copy(held(s, p), held(s, p), send_sem.at[s, p, m]).wait()

                @pl.when(table(spot, passes[p]) == 1)
                def _():
                    pltpu.make_async_copy(held(s, p), held(s, p), side_send.at[s, p]).wait()

    with jax.named_scope("home_sent"):
        for k in range(2):

            @pl.when(jnp.logical_not(stay[k]))
            def _():
                for p in range(3):
                    home_copy(k, p).wait_send()

    with jax.named_scope("home_here"):
        for s in range(2):
            for p in range(3):
                pltpu.make_async_copy(home(s, p), home(s, p), home_recv.at[s, p]).wait()


def place_kernel(slots, home13, homed, hot13, hotd, out13, outd, zero, sem):
    me = lax.axis_index("stage") * 8 + lax.axis_index("expert")
    zero[...] = jnp.zeros_like(zero)

    def pieces(layer, slot):
        return out13.at[layer, slot, :, pl.ds(0, 512)], out13.at[layer, slot, :, pl.ds(512, 512)], outd.at[layer, slot]

    for layer in range(2):
        pltpu.make_async_copy(home13.at[layer], out13.at[layer, 0], sem).start()
        pltpu.make_async_copy(homed.at[layer], outd.at[layer, 0], sem).start()
        for t in range(2):
            filled = slots[me, t] >= 0
            to = pieces(layer, t + 1)

            @pl.when(filled)
            def _():
                for p in range(3):
                    pltpu.make_async_copy(hotd.at[layer] if p == 2 else hot13.at[layer, p], to[p], sem).start()

            @pl.when(jnp.logical_not(filled))
            def _():
                for h in range(4):
                    pltpu.make_async_copy(zero, out13.at[layer, t + 1, pl.ds(h * 512, 512)], sem).start()
                for h in range(2):
                    pltpu.make_async_copy(zero, outd.at[layer, t + 1, :, pl.ds(h * 1024, 1024)], sem).start()

    for layer in range(2):
        for t in range(3):
            pltpu.make_async_copy(home13.at[layer], out13.at[layer, t], sem).wait()
            pltpu.make_async_copy(homed.at[layer], outd.at[layer, t], sem).wait()


def solution(mesh):
    DMA = pltpu.SemaphoreType.DMA

    VMEM = pl.BlockSpec(memory_space=pltpu.VMEM)

    def local(gate, up, down, hot_units, slot_map):
        def branch(unit, gate, up, down, slot_map):
            moved = pl.pallas_call(
                functools.partial(move_kernel, unit),
                out_shape=(
                    pltpu.VMEM((2, 2048, 1024), BF16),
                    pltpu.VMEM((2, 512, 2048), BF16),
                    pltpu.VMEM((2, 2, 2048, 512), BF16),
                    pltpu.VMEM((2, 512, 2048), BF16),
                ),
                in_specs=[ANY] * 3,
                out_specs=(VMEM,) * 4,
                scratch_shapes=[
                    pltpu.VMEM((2, 2, 2048, 512), BF16),
                    pltpu.VMEM((2, 512, 2048), BF16),
                    DMA((3,)),
                    DMA((2, 3)),
                    DMA((2, 3, N)),
                    DMA((2, 3, 2)),
                    DMA((2, 3)),
                    DMA((2, 3)),
                    DMA((2, 3)),
                ],
                compiler_params=pltpu.CompilerParams(has_side_effects=True, collective_id=0, vmem_limit_bytes=14 << 20),
                name=f"move{unit}",
            )(gate, up, down)
            return pl.pallas_call(
                place_kernel,
                out_shape=(
                    jax.ShapeDtypeStruct((2, 3, 2048, 1024), BF16),
                    jax.ShapeDtypeStruct((2, 3, 512, 2048), BF16),
                ),
                in_specs=[pl.BlockSpec(memory_space=pltpu.SMEM)] + [VMEM] * 4,
                out_specs=(ANY, ANY),
                scratch_shapes=[pltpu.VMEM((512, 1024), BF16), DMA],
                compiler_params=pltpu.CompilerParams(vmem_limit_bytes=4 << 20),
                name="place",
            )(slot_map, *moved)

        return lax.switch(hot_units[0], [functools.partial(branch, u) for u in range(16)], gate, up, down, slot_map)

    spec = P("stage", "expert")
    out = P(None, ("stage", "expert"))
    return jax.shard_map(local, mesh=mesh, in_specs=(spec, spec, spec, P(), P()), out_specs=(out, out), check_vma=False)
```

```python
import functools

import jax
import jax.numpy as jnp
from jax import lax
from jax.experimental import pallas as pl
from jax.experimental.pallas import tpu as pltpu
from jax.sharding import PartitionSpec as P

MESH = pl.DeviceIdType.MESH
ANY = pl.BlockSpec(memory_space=pl.ANY)
BF16 = jnp.bfloat16

PARENT = (
    (None, 0, 3, 1, 5, 1, 7, 5),
    (None, 3, 0, 2, 6, 7, 2, 3),
    (None, 5, 6, 7, 0, 4, 4, 6),
)
DEPTH = (
    (0, 1, 3, 2, 3, 2, 4, 3),
    (0, 3, 1, 2, 3, 4, 2, 3),
    (0, 3, 3, 4, 1, 2, 2, 3),
)
CHILDREN = tuple(tuple(tuple(v for v in range(1, 8) if par[v] == r) for r in range(8)) for par in PARENT)
DEEPEST = max(map(max, DEPTH))
N = 32
HOME_AT = 4
LAG = 3


def coords():
    z = lax.axis_index("stage")
    j = lax.axis_index("expert")
    return z, j // 4, (j // 2) % 2, j % 2


def dev(z, y, x, q):
    return (z, y * 4 + x * 2 + q)


def flip(v, bit):
    return 1 - v if bit else v


def table(index, values):
    out = jnp.int32(values[0])
    for i, v in enumerate(values[1:], 1):
        if v != values[0]:
            out = jnp.where(index == i, jnp.int32(v), out)
    return out


def roles(s, rb, rc):
    depth, passes, sends = [], [], []
    for p in range(3):
        def sender(r, v):
            x = (r & 1) ^ rb
            return x if r ^ v == 1 else 1 - x

        def entry(r):
            if r == 0:
                return rc
            children = CHILDREN[p][r]
            return sender(r, children[0]) if children else s

        depth.append([LAG * DEPTH[p][r] + (q != entry(r)) for r in range(8) for q in range(2)])
        passes.append([int(q == entry(r)) for r in range(8) for q in range(2)])
        to = [[v * 2 + entry(v) for v in CHILDREN[p][r] if sender(r, v) == q] for r in range(8) for q in range(2)]
        sends.append([[t[m] if len(t) > m else -1 for t in to] for m in range(max(map(len, to)))])
    return depth, passes, sends


def move_kernel(unit, gate, up, down, home13, homed, vg, vd, sg, sd, load_sem, stage_sem, recv_sem, send_sem, side_send, home_send, home_recv):
    e, half = unit // 2, unit % 2
    ra, rb, rc = e // 4, (e // 2) % 2, e % 2
    z, y, x, q = coords()

    def source(k, p):
        return down.at[0, 0, pl.ds(k * 512, 512), :] if p == 2 else (gate, up)[p].at[0, 0, :, pl.ds(k * 512, 512)]

    def staged(k, p):
        return sd.at[k] if p == 2 else sg.at[k, p]

    def held(s, p, i=None):
        if p == 2:
            return vd.at[s] if i is None else vd.at[s, pl.ds(i * (512 // N), 512 // N), :]
        return vg.at[s, p] if i is None else vg.at[s, p, pl.ds(i * (2048 // N), 2048 // N), :]

    def home(s, p):
        return homed.at[s] if p == 2 else home13.at[s, :, pl.ds(p * 512, 512)]

    trees = [roles(s, rb, rc) for s in range(2)]
    rels = [flip(z, s) * 4 + flip(y, ra) * 2 + flip(x, rb) for s in range(2)]
    spots = [rel * 2 + q for rel in rels]
    stay = [(z == y) & (y == x) & (x == q) & (q == k) for k in range(2)]

    def stage(k, p):
        return pltpu.make_async_copy(source(k, p), staged(k, p), stage_sem.at[k, p])

    def load(s, p):
        return pltpu.make_async_copy(source(half, p), held(s, p), load_sem.at[p])

    def home_copy(k, p):
        return pltpu.make_async_remote_copy(
            src_ref=staged(k, p),
            dst_ref=home(z, p),
            send_sem=home_send.at[k, p],
            recv_sem=home_recv.at[z, p],
            device_id=dev(y, x, q, k),
            device_id_type=MESH,
        )

    for s in range(2):

        @pl.when(spots[s] == rc)
        def _():
            for p in range(3):
                load(s, p).start()

    for p in range(3):
        for k in range(2):
            stage(k, p).start()

    barrier = pltpu.get_barrier_semaphore()

    def greet(d, carry):
        @pl.when((d // 8 != z) | (d % 8 != y * 4 + x * 2 + q))
        def _():
            pl.semaphore_signal(barrier, inc=1, device_id=(d // 8, d % 8), device_id_type=MESH)

        return carry

    lax.fori_loop(0, 16, greet, 0)
    pl.semaphore_wait(barrier, 15)

    for s in range(2):

        @pl.when(spots[s] == rc)
        def _():
            for p in range(3):
                load(s, p).wait()

    def start_home():
        for p in range(3):
            for k in range(2):
                stage(k, p).wait()

                @pl.when(stay[k])
                def _():
                    pltpu.make_async_copy(staged(k, p), home(z, p), home_recv.at[z, p]).start()

                @pl.when(jnp.logical_not(stay[k]))
                def _():
                    home_copy(k, p).start()

    def wave(t, carry):
        @pl.when(t == HOME_AT)
        def _():
            start_home()

        for s in range(2):
            spot = spots[s]
            depth, passes, sends = trees[s]
            for p in range(3):
                i = t - table(spot, depth[p])

                @pl.when((i >= 0) & (i < N))
                def _():
                    @pl.when(spot != rc)
                    def _():
                        pltpu.make_async_copy(held(s, p, i), held(s, p, i), recv_sem.at[s, p, i]).wait()

                    def forward(to, sem):
                        return pltpu.make_async_remote_copy(
                            src_ref=held(s, p, i),
                            dst_ref=held(s, p, i),
                            send_sem=sem,
                            recv_sem=recv_sem.at[s, p, i],
                            device_id=to,
                            device_id_type=MESH,
                        )

                    for m, row in enumerate(sends[p]):
                        child = table(spot, row)

                        @pl.when(child >= 0)
                        def _():
                            to = dev(flip(child // 8, s), flip((child // 4) % 2, ra), flip((child // 2) % 2, rb), child % 2)
                            forward(to, send_sem.at[s, p, m]).start()

                    @pl.when(table(spot, passes[p]) == 1)
                    def _():
                        forward(dev(z, y, x, 1 - q), side_send.at[s, p]).start()

        return carry

    lax.fori_loop(0, N + LAG * DEEPEST + 1, wave, 0)

    for s in range(2):
        spot = spots[s]
        _, passes, sends = trees[s]
        for p in range(3):
            for m, row in enumerate(sends[p]):

                @pl.when(table(spot, row) >= 0)
                def _():
                    pltpu.make_async_copy(held(s, p), held(s, p), send_sem.at[s, p, m]).wait()

            @pl.when(table(spot, passes[p]) == 1)
            def _():
                pltpu.make_async_copy(held(s, p), held(s, p), side_send.at[s, p]).wait()

    for k in range(2):

        @pl.when(jnp.logical_not(stay[k]))
        def _():
            for p in range(3):
                home_copy(k, p).wait_send()

    for s in range(2):
        for p in range(3):
            pltpu.make_async_copy(home(s, p), home(s, p), home_recv.at[s, p]).wait()


def place_kernel(slot_map, home13, homed, hot13, hotd, out13, outd, slots, zero, slots_sem, sem):
    me = lax.axis_index("stage") * 8 + lax.axis_index("expert")
    fetch = pltpu.make_async_copy(slot_map, slots, slots_sem)
    fetch.start()
    zero[...] = jnp.zeros_like(zero)

    def pieces(layer, slot):
        return out13.at[layer, slot, :, pl.ds(0, 512)], out13.at[layer, slot, :, pl.ds(512, 512)], outd.at[layer, slot]

    for layer in range(2):
        pltpu.make_async_copy(home13.at[layer], out13.at[layer, 0], sem).start()
        pltpu.make_async_copy(homed.at[layer], outd.at[layer, 0], sem).start()

    fetch.wait()
    for layer in range(2):
        for t in range(2):
            filled = slots[me, t] >= 0
            to = pieces(layer, t + 1)

            @pl.when(filled)
            def _():
                for p in range(3):
                    pltpu.make_async_copy(hotd.at[layer] if p == 2 else hot13.at[layer, p], to[p], sem).start()

            @pl.when(jnp.logical_not(filled))
            def _():
                for h in range(4):
                    pltpu.make_async_copy(zero, out13.at[layer, t + 1, pl.ds(h * 512, 512)], sem).start()
                for h in range(2):
                    pltpu.make_async_copy(zero, outd.at[layer, t + 1, :, pl.ds(h * 1024, 1024)], sem).start()

    for layer in range(2):
        for t in range(3):
            pltpu.make_async_copy(home13.at[layer], out13.at[layer, t], sem).wait()
            pltpu.make_async_copy(homed.at[layer], outd.at[layer, t], sem).wait()


def solution(mesh):
    DMA = pltpu.SemaphoreType.DMA

    VMEM = pl.BlockSpec(memory_space=pltpu.VMEM)

    def local(gate, up, down, hot_units, slot_map):
        def branch(unit, gate, up, down, slot_map):
            moved = pl.pallas_call(
                functools.partial(move_kernel, unit),
                out_shape=(
                    pltpu.VMEM((2, 2048, 1024), BF16),
                    pltpu.VMEM((2, 512, 2048), BF16),
                    pltpu.VMEM((2, 2, 2048, 512), BF16),
                    pltpu.VMEM((2, 512, 2048), BF16),
                ),
                in_specs=[ANY] * 3,
                out_specs=(VMEM,) * 4,
                scratch_shapes=[
                    pltpu.VMEM((2, 2, 2048, 512), BF16),
                    pltpu.VMEM((2, 512, 2048), BF16),
                    DMA((3,)),
                    DMA((2, 3)),
                    DMA((2, 3, N)),
                    DMA((2, 3, 2)),
                    DMA((2, 3)),
                    DMA((2, 3)),
                    DMA((2, 3)),
                ],
                compiler_params=pltpu.CompilerParams(has_side_effects=True, collective_id=0, vmem_limit_bytes=14 << 20),
                name=f"move{unit}",
            )(gate, up, down)
            return pl.pallas_call(
                place_kernel,
                out_shape=(
                    jax.ShapeDtypeStruct((2, 3, 2048, 1024), BF16),
                    jax.ShapeDtypeStruct((2, 3, 512, 2048), BF16),
                ),
                in_specs=[ANY] + [VMEM] * 4,
                out_specs=(ANY, ANY),
                scratch_shapes=[pltpu.SMEM((16, 2), jnp.int32), pltpu.VMEM((512, 1024), BF16), DMA, DMA],
                compiler_params=pltpu.CompilerParams(vmem_limit_bytes=4 << 20),
                name="place",
            )(slot_map, *moved)

        return lax.switch(hot_units[0], [functools.partial(branch, u) for u in range(16)], gate, up, down, slot_map)

    spec = P("stage", "expert")
    out = P(None, ("stage", "expert"))
    return jax.shard_map(local, mesh=mesh, in_specs=(spec, spec, spec, P(), P()), out_specs=(out, out), check_vma=False)
```

```python
import functools

import jax
import jax.numpy as jnp
from jax import lax
from jax.experimental import pallas as pl
from jax.experimental.pallas import tpu as pltpu
from jax.sharding import PartitionSpec as P

MESH = pl.DeviceIdType.MESH
ANY = pl.BlockSpec(memory_space=pl.ANY)
BF16 = jnp.bfloat16

PARENT = (
    (None, 0, 3, 1, 5, 1, 7, 5),
    (None, 3, 0, 2, 6, 7, 2, 3),
    (None, 5, 6, 7, 0, 4, 4, 6),
)
DEPTH = (
    (0, 1, 3, 2, 3, 2, 4, 3),
    (0, 3, 1, 2, 3, 4, 2, 3),
    (0, 3, 3, 4, 1, 2, 2, 3),
)
CHILDREN = tuple(tuple(tuple(v for v in range(1, 8) if par[v] == r) for r in range(8)) for par in PARENT)
DEEPEST = max(map(max, DEPTH))
N = 32
HOME_AT = 3
LAG = 4


def coords():
    z = lax.axis_index("stage")
    j = lax.axis_index("expert")
    return z, j // 4, (j // 2) % 2, j % 2


def dev(z, y, x, q):
    return (z, y * 4 + x * 2 + q)


def flip(v, bit):
    return 1 - v if bit else v


def table(index, values):
    out = jnp.int32(values[0])
    for i, v in enumerate(values[1:], 1):
        if v != values[0]:
            out = jnp.where(index == i, jnp.int32(v), out)
    return out


def roles(s, rb, rc):
    depth, passes, sends = [], [], []
    for p in range(3):
        def sender(r, v):
            x = (r & 1) ^ rb
            return x if r ^ v == 1 else 1 - x

        def entry(r):
            if r == 0:
                return rc
            children = CHILDREN[p][r]
            return sender(r, children[0]) if children else s

        depth.append([LAG * DEPTH[p][r] + (q != entry(r)) for r in range(8) for q in range(2)])
        passes.append([int(q == entry(r)) for r in range(8) for q in range(2)])
        to = [[v * 2 + entry(v) for v in CHILDREN[p][r] if sender(r, v) == q] for r in range(8) for q in range(2)]
        sends.append([[t[m] if len(t) > m else -1 for t in to] for m in range(max(map(len, to)))])
    return depth, passes, sends


def move_kernel(unit, gate, up, down, home13, homed, vg, vd, sg, sd, load_sem, stage_sem, recv_sem, send_sem, side_send, home_send, home_recv):
    e, half = unit // 2, unit % 2
    ra, rb, rc = e // 4, (e // 2) % 2, e % 2
    z, y, x, q = coords()

    def source(k, p):
        return down.at[0, 0, pl.ds(k * 512, 512), :] if p == 2 else (gate, up)[p].at[0, 0, :, pl.ds(k * 512, 512)]

    def staged(k, p):
        return sd.at[k] if p == 2 else sg.at[k, p]

    def held(s, p, i=None):
        if p == 2:
            return vd.at[s] if i is None else vd.at[s, pl.ds(i * (512 // N), 512 // N), :]
        return vg.at[s, p] if i is None else vg.at[s, p, pl.ds(i * (2048 // N), 2048 // N), :]

    def home(s, p):
        return homed.at[s] if p == 2 else home13.at[s, :, pl.ds(p * 512, 512)]

    trees = [roles(s, rb, rc) for s in range(2)]
    rels = [flip(z, s) * 4 + flip(y, ra) * 2 + flip(x, rb) for s in range(2)]
    spots = [rel * 2 + q for rel in rels]
    holder = (y == ra) & (x == rb) & (q == rc)
    due = [jnp.logical_not(holder) if k == half else (z >= 0) for k in range(2)]
    same = [(z == y) & (y == x) & (x == q) & (q == k) for k in range(2)]
    stay = [due[k] & same[k] for k in range(2)]
    leave = [due[k] & jnp.logical_not(same[k]) for k in range(2)]

    def stage(k, p):
        return pltpu.make_async_copy(source(k, p), staged(k, p), stage_sem.at[k, p])

    def load(s, p):
        return pltpu.make_async_copy(source(half, p), held(s, p), load_sem.at[p])

    def home_copy(k, p):
        return pltpu.make_async_remote_copy(
            src_ref=staged(k, p),
            dst_ref=home(z, p),
            send_sem=home_send.at[k, p],
            recv_sem=home_recv.at[z, p],
            device_id=dev(y, x, q, k),
            device_id_type=MESH,
        )

    for s in range(2):

        @pl.when(spots[s] == rc)
        def _():
            for p in range(3):
                load(s, p).start()

    for p in range(3):
        for k in range(2):
            stage(k, p).start()

    barrier = pltpu.get_barrier_semaphore()

    def greet(d, carry):
        @pl.when((d // 8 != z) | (d % 8 != y * 4 + x * 2 + q))
        def _():
            pl.semaphore_signal(barrier, inc=1, device_id=(d // 8, d % 8), device_id_type=MESH)

        return carry

    lax.fori_loop(0, 16, greet, 0)
    pl.semaphore_wait(barrier, 15)

    for s in range(2):

        @pl.when(spots[s] == rc)
        def _():
            for p in range(3):
                load(s, p).wait()

    def start_home():
        for p in range(3):
            for k in range(2):
                stage(k, p).wait()

                @pl.when(stay[k])
                def _():
                    pltpu.make_async_copy(staged(k, p), home(z, p), home_recv.at[z, p]).start()

                @pl.when(leave[k])
                def _():
                    home_copy(k, p).start()

    def wave(t, carry):
        @pl.when(t == HOME_AT)
        def _():
            start_home()

        for s in range(2):
            spot = spots[s]
            depth, passes, sends = trees[s]
            for p in range(3):
                i = t - table(spot, depth[p])

                @pl.when((i >= 0) & (i < N))
                def _():
                    @pl.when(spot != rc)
                    def _():
                        pltpu.make_async_copy(held(s, p, i), held(s, p, i), recv_sem.at[s, p, i]).wait()

                    def forward(to, sem):
                        return pltpu.make_async_remote_copy(
                            src_ref=held(s, p, i),
                            dst_ref=held(s, p, i),
                            send_sem=sem,
                            recv_sem=recv_sem.at[s, p, i],
                            device_id=to,
                            device_id_type=MESH,
                        )

                    for m, row in enumerate(sends[p]):
                        child = table(spot, row)

                        @pl.when(child >= 0)
                        def _():
                            to = dev(flip(child // 8, s), flip((child // 4) % 2, ra), flip((child // 2) % 2, rb), child % 2)
                            forward(to, send_sem.at[s, p, m]).start()

                    @pl.when(table(spot, passes[p]) == 1)
                    def _():
                        forward(dev(z, y, x, 1 - q), side_send.at[s, p]).start()

        return carry

    lax.fori_loop(0, N + LAG * DEEPEST + 1, wave, 0)

    for s in range(2):
        spot = spots[s]
        _, passes, sends = trees[s]
        for p in range(3):
            for m, row in enumerate(sends[p]):

                @pl.when(table(spot, row) >= 0)
                def _():
                    pltpu.make_async_copy(held(s, p), held(s, p), send_sem.at[s, p, m]).wait()

            @pl.when(table(spot, passes[p]) == 1)
            def _():
                pltpu.make_async_copy(held(s, p), held(s, p), side_send.at[s, p]).wait()

    for k in range(2):

        @pl.when(leave[k])
        def _():
            for p in range(3):
                home_copy(k, p).wait_send()

    @pl.when(jnp.logical_not((z == ra) & (y == rb) & (x == rc) & (q == half)))
    def _():
        for s in range(2):
            for p in range(3):
                pltpu.make_async_copy(home(s, p), home(s, p), home_recv.at[s, p]).wait()


def place_kernel(unit, slot_map, home13, homed, hot13, hotd, out13, outd, slots, zero, slots_sem, sem):
    me = lax.axis_index("stage") * 8 + lax.axis_index("expert")
    fetch = pltpu.make_async_copy(slot_map, slots, slots_sem)
    fetch.start()
    zero[...] = jnp.zeros_like(zero)

    def pieces(layer, slot):
        return out13.at[layer, slot, :, pl.ds(0, 512)], out13.at[layer, slot, :, pl.ds(512, 512)], outd.at[layer, slot]

    def place_hot(layer, slot):
        to = pieces(layer, slot)
        for p in range(3):
            pltpu.make_async_copy(hotd.at[layer] if p == 2 else hot13.at[layer, p], to[p], sem).start()

    @pl.when(me != unit)
    def _():
        for layer in range(2):
            pltpu.make_async_copy(home13.at[layer], out13.at[layer, 0], sem).start()
            pltpu.make_async_copy(homed.at[layer], outd.at[layer, 0], sem).start()

    @pl.when(me == unit)
    def _():
        for layer in range(2):
            place_hot(layer, 0)

    fetch.wait()
    for layer in range(2):
        for t in range(2):
            filled = slots[me, t] >= 0

            @pl.when(filled)
            def _():
                place_hot(layer, t + 1)

            @pl.when(jnp.logical_not(filled))
            def _():
                for h in range(4):
                    pltpu.make_async_copy(zero, out13.at[layer, t + 1, pl.ds(h * 512, 512)], sem).start()
                for h in range(2):
                    pltpu.make_async_copy(zero, outd.at[layer, t + 1, :, pl.ds(h * 1024, 1024)], sem).start()

    for layer in range(2):
        for t in range(3):
            pltpu.make_async_copy(home13.at[layer], out13.at[layer, t], sem).wait()
            pltpu.make_async_copy(homed.at[layer], outd.at[layer, t], sem).wait()


def solution(mesh):
    DMA = pltpu.SemaphoreType.DMA

    VMEM = pl.BlockSpec(memory_space=pltpu.VMEM)

    def local(gate, up, down, hot_units, slot_map):
        def branch(unit, gate, up, down, slot_map):
            moved = pl.pallas_call(
                functools.partial(move_kernel, unit),
                out_shape=(
                    pltpu.VMEM((2, 2048, 1024), BF16),
                    pltpu.VMEM((2, 512, 2048), BF16),
                    pltpu.VMEM((2, 2, 2048, 512), BF16),
                    pltpu.VMEM((2, 512, 2048), BF16),
                ),
                in_specs=[ANY] * 3,
                out_specs=(VMEM,) * 4,
                scratch_shapes=[
                    pltpu.VMEM((2, 2, 2048, 512), BF16),
                    pltpu.VMEM((2, 512, 2048), BF16),
                    DMA((3,)),
                    DMA((2, 3)),
                    DMA((2, 3, N)),
                    DMA((2, 3, 2)),
                    DMA((2, 3)),
                    DMA((2, 3)),
                    DMA((2, 3)),
                ],
                compiler_params=pltpu.CompilerParams(has_side_effects=True, collective_id=0, vmem_limit_bytes=14 << 20),
                name=f"move{unit}",
            )(gate, up, down)
            return pl.pallas_call(
                functools.partial(place_kernel, unit),
                out_shape=(
                    jax.ShapeDtypeStruct((2, 3, 2048, 1024), BF16),
                    jax.ShapeDtypeStruct((2, 3, 512, 2048), BF16),
                ),
                in_specs=[pl.BlockSpec(memory_space=pltpu.HBM)] + [VMEM] * 4,
                out_specs=(ANY, ANY),
                scratch_shapes=[pltpu.SMEM((16, 2), jnp.int32), pltpu.VMEM((512, 1024), BF16), DMA, DMA],
                compiler_params=pltpu.CompilerParams(vmem_limit_bytes=4 << 20),
                name="place",
            )(slot_map, *moved)

        return lax.switch(hot_units[0], [functools.partial(branch, u) for u in range(16)], gate, up, down, slot_map)

    spec = P("stage", "expert")
    out = P(None, ("stage", "expert"))
    return jax.shard_map(local, mesh=mesh, in_specs=(spec, spec, spec, P(), P()), out_specs=(out, out), check_vma=False)
```

```python
import functools

import jax
import jax.numpy as jnp
from jax import lax
from jax.experimental import pallas as pl
from jax.experimental.pallas import tpu as pltpu
from jax.sharding import PartitionSpec as P

MESH = pl.DeviceIdType.MESH
ANY = pl.BlockSpec(memory_space=pl.ANY)
BF16 = jnp.bfloat16

PARENT = (
    (None, 0, 3, 1, 5, 1, 7, 5),
    (None, 3, 0, 2, 6, 7, 2, 3),
    (None, 5, 6, 7, 0, 4, 4, 6),
)
DEPTH = (
    (0, 1, 3, 2, 3, 2, 4, 3),
    (0, 3, 1, 2, 3, 4, 2, 3),
    (0, 3, 3, 4, 1, 2, 2, 3),
)
CHILDREN = tuple(tuple(tuple(v for v in range(1, 8) if par[v] == r) for r in range(8)) for par in PARENT)
DEEPEST = max(map(max, DEPTH))
N = 32
HOME_AT = 3
LAG = 4


def coords():
    z = lax.axis_index("stage")
    j = lax.axis_index("expert")
    return z, j // 4, (j // 2) % 2, j % 2


def dev(z, y, x, q):
    return (z, y * 4 + x * 2 + q)


def flip(v, bit):
    return 1 - v if bit else v


def table(index, values):
    out = jnp.int32(values[0])
    for i, v in enumerate(values[1:], 1):
        if v != values[0]:
            out = jnp.where(index == i, jnp.int32(v), out)
    return out


def roles(s, rb, rc):
    depth, passes, sends = [], [], []
    for p in range(3):
        def sender(r, v):
            x = (r & 1) ^ rb
            return x if r ^ v == 1 else 1 - x

        def entry(r):
            if r == 0:
                return rc
            children = CHILDREN[p][r]
            return sender(r, children[0]) if children else s

        depth.append([LAG * DEPTH[p][r] + (q != entry(r)) for r in range(8) for q in range(2)])
        passes.append([int(q == entry(r)) for r in range(8) for q in range(2)])
        to = [[v * 2 + entry(v) for v in CHILDREN[p][r] if sender(r, v) == q] for r in range(8) for q in range(2)]
        sends.append([[t[m] if len(t) > m else -1 for t in to] for m in range(max(map(len, to)))])
    return depth, passes, sends


def move_kernel(unit, gate, up, down, home13, homed, vg, vd, sg, sd, load_sem, stage_sem, recv_sem, send_sem, side_send, home_send, home_recv):
    e, half = unit // 2, unit % 2
    ra, rb, rc = e // 4, (e // 2) % 2, e % 2
    z, y, x, q = coords()

    def source(k, p):
        return down.at[0, 0, pl.ds(k * 512, 512), :] if p == 2 else (gate, up)[p].at[0, 0, :, pl.ds(k * 512, 512)]

    def staged(k, p):
        return sd.at[k] if p == 2 else sg.at[k, p]

    def held(s, p, i=None):
        if p == 2:
            return vd.at[s] if i is None else vd.at[s, pl.ds(i * (512 // N), 512 // N), :]
        return vg.at[s, p] if i is None else vg.at[s, p, pl.ds(i * (2048 // N), 2048 // N), :]

    def home(s, p):
        return homed.at[s] if p == 2 else home13.at[s, :, pl.ds(p * 512, 512)]

    trees = [roles(s, rb, rc) for s in range(2)]
    rels = [flip(z, s) * 4 + flip(y, ra) * 2 + flip(x, rb) for s in range(2)]
    spots = [rel * 2 + q for rel in rels]
    holder = (y == ra) & (x == rb) & (q == rc)
    due = [jnp.logical_not(holder) if k == half else (z >= 0) for k in range(2)]
    same = [(z == y) & (y == x) & (x == q) & (q == k) for k in range(2)]
    stay = [due[k] & same[k] for k in range(2)]
    leave = [due[k] & jnp.logical_not(same[k]) for k in range(2)]

    def stage(k, p):
        return pltpu.make_async_copy(source(k, p), staged(k, p), stage_sem.at[k, p])

    def load(s, p):
        return pltpu.make_async_copy(source(half, p), held(s, p), load_sem.at[p])

    def home_copy(k, p):
        return pltpu.make_async_remote_copy(
            src_ref=staged(k, p),
            dst_ref=home(z, p),
            send_sem=home_send.at[k, p],
            recv_sem=home_recv.at[z, p],
            device_id=dev(y, x, q, k),
            device_id_type=MESH,
        )

    for s in range(2):

        @pl.when(spots[s] == rc)
        def _():
            for p in range(3):
                load(s, p).start()

    for p in range(3):
        for k in range(2):
            stage(k, p).start()

    barrier = pltpu.get_barrier_semaphore()

    def greet(d, carry):
        @pl.when((d // 8 != z) | (d % 8 != y * 4 + x * 2 + q))
        def _():
            pl.semaphore_signal(barrier, inc=1, device_id=(d // 8, d % 8), device_id_type=MESH)

        return carry

    lax.fori_loop(0, 16, greet, 0)
    pl.semaphore_wait(barrier, 15)

    for s in range(2):

        @pl.when(spots[s] == rc)
        def _():
            for p in range(3):
                load(s, p).wait()

    def start_home():
        for p in range(3):
            for k in range(2):
                stage(k, p).wait()

                @pl.when(stay[k])
                def _():
                    pltpu.make_async_copy(staged(k, p), home(z, p), home_recv.at[z, p]).start()

                @pl.when(leave[k])
                def _():
                    home_copy(k, p).start()

    def wave(t, carry):
        @pl.when(t == HOME_AT)
        def _():
            start_home()

        for s in range(2):
            spot = spots[s]
            depth, passes, sends = trees[s]
            for p in range(3):
                i = t - table(spot, depth[p])

                @pl.when((i >= 0) & (i < N))
                def _():
                    @pl.when(spot != rc)
                    def _():
                        pltpu.make_async_copy(held(s, p, i), held(s, p, i), recv_sem.at[s, p, i]).wait()

                    def forward(to, sem):
                        return pltpu.make_async_remote_copy(
                            src_ref=held(s, p, i),
                            dst_ref=held(s, p, i),
                            send_sem=sem,
                            recv_sem=recv_sem.at[s, p, i],
                            device_id=to,
                            device_id_type=MESH,
                        )

                    for m, row in enumerate(sends[p]):
                        child = table(spot, row)

                        @pl.when(child >= 0)
                        def _():
                            to = dev(flip(child // 8, s), flip((child // 4) % 2, ra), flip((child // 2) % 2, rb), child % 2)
                            forward(to, send_sem.at[s, p, m]).start()

                    @pl.when(table(spot, passes[p]) == 1)
                    def _():
                        forward(dev(z, y, x, 1 - q), side_send.at[s, p]).start()

        return carry

    lax.fori_loop(0, N + LAG * DEEPEST + 1, wave, 0)

    for s in range(2):
        spot = spots[s]
        _, passes, sends = trees[s]
        for p in range(3):
            for m, row in enumerate(sends[p]):

                @pl.when(table(spot, row) >= 0)
                def _():
                    pltpu.make_async_copy(held(s, p), held(s, p), send_sem.at[s, p, m]).wait()

            @pl.when(table(spot, passes[p]) == 1)
            def _():
                pltpu.make_async_copy(held(s, p), held(s, p), side_send.at[s, p]).wait()

    for k in range(2):

        @pl.when(leave[k])
        def _():
            for p in range(3):
                home_copy(k, p).wait_send()

    @pl.when(jnp.logical_not((z == ra) & (y == rb) & (x == rc) & (q == half)))
    def _():
        for s in range(2):
            for p in range(3):
                pltpu.make_async_copy(home(s, p), home(s, p), home_recv.at[s, p]).wait()


def place_kernel(unit, slot_map, home13, homed, hot13, hotd, out13, outd, slots, zero, slots_sem, sem):
    me = lax.axis_index("stage") * 8 + lax.axis_index("expert")
    fetch = pltpu.make_async_copy(slot_map, slots, slots_sem)
    fetch.start()
    zero[...] = jnp.zeros_like(zero)

    def pieces(layer, slot):
        return out13.at[layer, slot, :, pl.ds(0, 512)], out13.at[layer, slot, :, pl.ds(512, 512)], outd.at[layer, slot]

    def place_hot(layer, slot):
        to = pieces(layer, slot)
        for p in range(3):
            pltpu.make_async_copy(hotd.at[layer] if p == 2 else hot13.at[layer, p], to[p], sem).start()

    @pl.when(me != unit)
    def _():
        for layer in range(2):
            pltpu.make_async_copy(home13.at[layer], out13.at[layer, 0], sem).start()
            pltpu.make_async_copy(homed.at[layer], outd.at[layer, 0], sem).start()

    @pl.when(me == unit)
    def _():
        for layer in range(2):
            place_hot(layer, 0)

    fetch.wait()
    for layer in range(2):
        for t in range(2):
            filled = slots[t, me] >= 0

            @pl.when(filled)
            def _():
                place_hot(layer, t + 1)

            @pl.when(jnp.logical_not(filled))
            def _():
                for h in range(4):
                    pltpu.make_async_copy(zero, out13.at[layer, t + 1, pl.ds(h * 512, 512)], sem).start()
                for h in range(2):
                    pltpu.make_async_copy(zero, outd.at[layer, t + 1, :, pl.ds(h * 1024, 1024)], sem).start()

    for layer in range(2):
        for t in range(3):
            pltpu.make_async_copy(home13.at[layer], out13.at[layer, t], sem).wait()
            pltpu.make_async_copy(homed.at[layer], outd.at[layer, t], sem).wait()


def solution(mesh):
    DMA = pltpu.SemaphoreType.DMA

    VMEM = pl.BlockSpec(memory_space=pltpu.VMEM)

    def local(gate, up, down, hot_units, slot_map):
        def branch(unit, gate, up, down, slot_map):
            moved = pl.pallas_call(
                functools.partial(move_kernel, unit),
                out_shape=(
                    pltpu.VMEM((2, 2048, 1024), BF16),
                    pltpu.VMEM((2, 512, 2048), BF16),
                    pltpu.VMEM((2, 2, 2048, 512), BF16),
                    pltpu.VMEM((2, 512, 2048), BF16),
                ),
                in_specs=[ANY] * 3,
                out_specs=(VMEM,) * 4,
                scratch_shapes=[
                    pltpu.VMEM((2, 2, 2048, 512), BF16),
                    pltpu.VMEM((2, 512, 2048), BF16),
                    DMA((3,)),
                    DMA((2, 3)),
                    DMA((2, 3, N)),
                    DMA((2, 3, 2)),
                    DMA((2, 3)),
                    DMA((2, 3)),
                    DMA((2, 3)),
                ],
                compiler_params=pltpu.CompilerParams(has_side_effects=True, collective_id=0, vmem_limit_bytes=14 << 20),
                name=f"move{unit}",
            )(gate, up, down)
            return pl.pallas_call(
                functools.partial(place_kernel, unit),
                out_shape=(
                    jax.ShapeDtypeStruct((2, 3, 2048, 1024), BF16),
                    jax.ShapeDtypeStruct((2, 3, 512, 2048), BF16),
                ),
                in_specs=[pl.BlockSpec(memory_space=pltpu.HBM)] + [VMEM] * 4,
                out_specs=(ANY, ANY),
                scratch_shapes=[pltpu.SMEM((2, 16), jnp.int32), pltpu.VMEM((512, 1024), BF16), DMA, DMA],
                compiler_params=pltpu.CompilerParams(vmem_limit_bytes=4 << 20),
                name="place",
            )(slot_map.T, *moved)

        return lax.switch(hot_units[0], [functools.partial(branch, u) for u in range(16)], gate, up, down, slot_map)

    spec = P("stage", "expert")
    out = P(None, ("stage", "expert"))
    return jax.shard_map(local, mesh=mesh, in_specs=(spec, spec, spec, P(), P()), out_specs=(out, out), check_vma=False)
```

```python
import functools

import jax
import jax.numpy as jnp
from jax import lax
from jax.experimental import pallas as pl
from jax.experimental.pallas import tpu as pltpu
from jax.sharding import PartitionSpec as P

MESH = pl.DeviceIdType.MESH
ANY = pl.BlockSpec(memory_space=pl.ANY)
BF16 = jnp.bfloat16

PARENT = (
    (None, 0, 3, 1, 5, 1, 7, 5),
    (None, 3, 0, 2, 6, 7, 2, 3),
    (None, 5, 6, 7, 0, 4, 4, 6),
)
DEPTH = (
    (0, 1, 3, 2, 3, 2, 4, 3),
    (0, 3, 1, 2, 3, 4, 2, 3),
    (0, 3, 3, 4, 1, 2, 2, 3),
)
CHILDREN = tuple(tuple(tuple(v for v in range(1, 8) if par[v] == r) for r in range(8)) for par in PARENT)
DEEPEST = max(map(max, DEPTH))
N = 32
HOME_AT = 1
LAG = 4


def coords():
    z = lax.axis_index("stage")
    j = lax.axis_index("expert")
    return z, j // 4, (j // 2) % 2, j % 2


def dev(z, y, x, q):
    return (z, y * 4 + x * 2 + q)


def flip(v, bit):
    return 1 - v if bit else v


def table(index, values):
    out = jnp.int32(values[0])
    for i, v in enumerate(values[1:], 1):
        if v != values[0]:
            out = jnp.where(index == i, jnp.int32(v), out)
    return out


def roles(s, rb, rc):
    depth, passes, sends = [], [], []
    for p in range(3):
        def sender(r, v):
            x = (r & 1) ^ rb
            return x if r ^ v == 1 else 1 - x

        def entry(r):
            if r == 0:
                return rc
            children = CHILDREN[p][r]
            return sender(r, children[0]) if children else s

        depth.append([LAG * DEPTH[p][r] + (q != entry(r)) for r in range(8) for q in range(2)])
        passes.append([int(q == entry(r)) for r in range(8) for q in range(2)])
        to = [[v * 2 + entry(v) for v in CHILDREN[p][r] if sender(r, v) == q] for r in range(8) for q in range(2)]
        sends.append([[t[m] if len(t) > m else -1 for t in to] for m in range(max(map(len, to)))])
    return depth, passes, sends


def move_kernel(unit, gate, up, down, home13, homed, vg, vd, sg, sd, load_sem, stage_sem, recv_sem, send_sem, side_send, home_send, home_recv):
    e, half = unit // 2, unit % 2
    ra, rb, rc = e // 4, (e // 2) % 2, e % 2
    z, y, x, q = coords()

    def source(k, p):
        return down.at[0, 0, pl.ds(k * 512, 512), :] if p == 2 else (gate, up)[p].at[0, 0, :, pl.ds(k * 512, 512)]

    def staged(k, p):
        return sd.at[k] if p == 2 else sg.at[k, p]

    def held(s, p, i=None):
        if p == 2:
            return vd.at[s] if i is None else vd.at[s, pl.ds(i * (512 // N), 512 // N), :]
        return vg.at[s, p] if i is None else vg.at[s, p, pl.ds(i * (2048 // N), 2048 // N), :]

    def home(s, p):
        return homed.at[s] if p == 2 else home13.at[s, :, pl.ds(p * 512, 512)]

    trees = [roles(s, rb, rc) for s in range(2)]
    rels = [flip(z, s) * 4 + flip(y, ra) * 2 + flip(x, rb) for s in range(2)]
    spots = [rel * 2 + q for rel in rels]
    holder = (y == ra) & (x == rb) & (q == rc)
    due = [jnp.logical_not(holder) if k == half else (z >= 0) for k in range(2)]
    same = [(z == y) & (y == x) & (x == q) & (q == k) for k in range(2)]
    stay = [due[k] & same[k] for k in range(2)]
    leave = [due[k] & jnp.logical_not(same[k]) for k in range(2)]

    def stage(k, p):
        return pltpu.make_async_copy(source(k, p), staged(k, p), stage_sem.at[k, p])

    def load(s, p):
        return pltpu.make_async_copy(source(half, p), held(s, p), load_sem.at[p])

    def home_copy(k, p):
        return pltpu.make_async_remote_copy(
            src_ref=staged(k, p),
            dst_ref=home(z, p),
            send_sem=home_send.at[k, p],
            recv_sem=home_recv.at[z, p],
            device_id=dev(y, x, q, k),
            device_id_type=MESH,
        )

    for s in range(2):

        @pl.when(spots[s] == rc)
        def _():
            for p in range(3):
                load(s, p).start()

    for p in range(3):
        for k in range(2):
            stage(k, p).start()

    barrier = pltpu.get_barrier_semaphore()

    def greet(d, carry):
        @pl.when((d // 8 != z) | (d % 8 != y * 4 + x * 2 + q))
        def _():
            pl.semaphore_signal(barrier, inc=1, device_id=(d // 8, d % 8), device_id_type=MESH)

        return carry

    lax.fori_loop(0, 16, greet, 0)
    pl.semaphore_wait(barrier, 15)

    for s in range(2):

        @pl.when(spots[s] == rc)
        def _():
            for p in range(3):
                load(s, p).wait()

    def start_home():
        for p in range(3):
            for k in range(2):
                stage(k, p).wait()

                @pl.when(stay[k])
                def _():
                    pltpu.make_async_copy(staged(k, p), home(z, p), home_recv.at[z, p]).start()

                @pl.when(leave[k])
                def _():
                    home_copy(k, p).start()

    def wave(t, carry):
        @pl.when(t == HOME_AT)
        def _():
            start_home()

        for s in range(2):
            spot = spots[s]
            depth, passes, sends = trees[s]
            for p in range(3):
                i = t - table(spot, depth[p])

                @pl.when((i >= 0) & (i < N))
                def _():
                    @pl.when(spot != rc)
                    def _():
                        pltpu.make_async_copy(held(s, p, i), held(s, p, i), recv_sem.at[s, p, i]).wait()

                    def forward(to, sem):
                        return pltpu.make_async_remote_copy(
                            src_ref=held(s, p, i),
                            dst_ref=held(s, p, i),
                            send_sem=sem,
                            recv_sem=recv_sem.at[s, p, i],
                            device_id=to,
                            device_id_type=MESH,
                        )

                    for m, row in enumerate(sends[p]):
                        child = table(spot, row)

                        @pl.when(child >= 0)
                        def _():
                            to = dev(flip(child // 8, s), flip((child // 4) % 2, ra), flip((child // 2) % 2, rb), child % 2)
                            forward(to, send_sem.at[s, p, m]).start()

                    @pl.when(table(spot, passes[p]) == 1)
                    def _():
                        forward(dev(z, y, x, 1 - q), side_send.at[s, p]).start()

        return carry

    lax.fori_loop(0, N + LAG * DEEPEST + 1, wave, 0)

    for s in range(2):
        spot = spots[s]
        _, passes, sends = trees[s]
        for p in range(3):
            for m, row in enumerate(sends[p]):

                @pl.when(table(spot, row) >= 0)
                def _():
                    pltpu.make_async_copy(held(s, p), held(s, p), send_sem.at[s, p, m]).wait()

            @pl.when(table(spot, passes[p]) == 1)
            def _():
                pltpu.make_async_copy(held(s, p), held(s, p), side_send.at[s, p]).wait()

    for k in range(2):

        @pl.when(leave[k])
        def _():
            for p in range(3):
                home_copy(k, p).wait_send()

    @pl.when(jnp.logical_not((z == ra) & (y == rb) & (x == rc) & (q == half)))
    def _():
        for s in range(2):
            for p in range(3):
                pltpu.make_async_copy(home(s, p), home(s, p), home_recv.at[s, p]).wait()


def place_kernel(unit, slot_map, home13, homed, hot13, hotd, out13, outd, slots, zero, slots_sem, sem):
    me = lax.axis_index("stage") * 8 + lax.axis_index("expert")
    fetch = pltpu.make_async_copy(slot_map, slots, slots_sem)
    fetch.start()
    zero[...] = jnp.zeros_like(zero)

    def pieces(layer, slot):
        return out13.at[layer, slot, :, pl.ds(0, 512)], out13.at[layer, slot, :, pl.ds(512, 512)], outd.at[layer, slot]

    def place_hot(layer, slot):
        to = pieces(layer, slot)
        for p in range(3):
            pltpu.make_async_copy(hotd.at[layer] if p == 2 else hot13.at[layer, p], to[p], sem).start()

    @pl.when(me != unit)
    def _():
        for layer in range(2):
            pltpu.make_async_copy(home13.at[layer], out13.at[layer, 0], sem).start()
            pltpu.make_async_copy(homed.at[layer], outd.at[layer, 0], sem).start()

    @pl.when(me == unit)
    def _():
        for layer in range(2):
            place_hot(layer, 0)

    fetch.wait()
    for layer in range(2):
        for t in range(2):
            filled = slots[t, me] >= 0

            @pl.when(filled)
            def _():
                place_hot(layer, t + 1)

            @pl.when(jnp.logical_not(filled))
            def _():
                for h in range(4):
                    pltpu.make_async_copy(zero, out13.at[layer, t + 1, pl.ds(h * 512, 512)], sem).start()
                for h in range(2):
                    pltpu.make_async_copy(zero, outd.at[layer, t + 1, :, pl.ds(h * 1024, 1024)], sem).start()

    for layer in range(2):
        for t in range(3):
            pltpu.make_async_copy(home13.at[layer], out13.at[layer, t], sem).wait()
            pltpu.make_async_copy(homed.at[layer], outd.at[layer, t], sem).wait()


def solution(mesh):
    DMA = pltpu.SemaphoreType.DMA

    VMEM = pl.BlockSpec(memory_space=pltpu.VMEM)

    def local(gate, up, down, hot_units, slot_map):
        def branch(unit, gate, up, down, slot_map):
            moved = pl.pallas_call(
                functools.partial(move_kernel, unit),
                out_shape=(
                    pltpu.VMEM((2, 2048, 1024), BF16),
                    pltpu.VMEM((2, 512, 2048), BF16),
                    pltpu.VMEM((2, 2, 2048, 512), BF16),
                    pltpu.VMEM((2, 512, 2048), BF16),
                ),
                in_specs=[ANY] * 3,
                out_specs=(VMEM,) * 4,
                scratch_shapes=[
                    pltpu.VMEM((2, 2, 2048, 512), BF16),
                    pltpu.VMEM((2, 512, 2048), BF16),
                    DMA((3,)),
                    DMA((2, 3)),
                    DMA((2, 3, N)),
                    DMA((2, 3, 2)),
                    DMA((2, 3)),
                    DMA((2, 3)),
                    DMA((2, 3)),
                ],
                compiler_params=pltpu.CompilerParams(has_side_effects=True, collective_id=0, vmem_limit_bytes=14 << 20),
                name=f"move{unit}",
            )(gate, up, down)
            return pl.pallas_call(
                functools.partial(place_kernel, unit),
                out_shape=(
                    jax.ShapeDtypeStruct((2, 3, 2048, 1024), BF16),
                    jax.ShapeDtypeStruct((2, 3, 512, 2048), BF16),
                ),
                in_specs=[pl.BlockSpec(memory_space=pltpu.HBM)] + [VMEM] * 4,
                out_specs=(ANY, ANY),
                scratch_shapes=[pltpu.SMEM((2, 16), jnp.int32), pltpu.VMEM((512, 1024), BF16), DMA, DMA],
                compiler_params=pltpu.CompilerParams(vmem_limit_bytes=4 << 20),
                name="place",
            )(slot_map.T, *moved)

        return lax.switch(hot_units[0], [functools.partial(branch, u) for u in range(16)], gate, up, down, slot_map)

    spec = P("stage", "expert")
    out = P(None, ("stage", "expert"))
    return jax.shard_map(local, mesh=mesh, in_specs=(spec, spec, spec, P(), P()), out_specs=(out, out), check_vma=False)
```
